32 devices in a mesh: dp: 32 (over z, y, x, core).
Axes of the slice: x: 2, y: 2, z: 4, core: 2. Of those that a mesh axis runs over, the one named last changes fastest.
Arguments:
- g_mat: bfloat16 [32, 9830400], P('dp')
- g_vec: bfloat16 [32, 16640], P('dp')
- p_mat: float32 [9830400], P('dp')
- m_mat: float32 [9830400], P('dp')
- v_mat: float32 [9830400], P('dp')
- p_vec: float32 [16640], replicated
- m_vec: float32 [16640], replicated
- v_vec: float32 [16640], replicated
- learn_rate: float32 [], replicated
Outputs:
- output 1: float32 [9830400], P('dp')
- output 2: float32 [9830400], P('dp')
- output 3: float32 [9830400], P('dp')
- output 4: float32 [16640], replicated
- output 5: float32 [16640], replicated
- output 6: float32 [16640], replicated
- output 7: bfloat16 [9830400], replicated
All inputs are finite; a program needn't handle non-finite values.
Results may differ from the reference program's by a relative error of at most 0.001.
Values are sent between devices in bfloat16 or wider.
A program may use at most 1 GiB of HBM per device.

```python
import jax
import jax.numpy as jnp
from jax import lax

D = 640
FF = 2560
TP = 1
DP = 32
STEP = 10

N_MAT = (8 * D * D + 4 * D * FF) // TP
N_VEC = 2 * ((3 * D + FF) // TP) + 12 * D
N_ALL = N_MAT + N_VEC
ELEM_SCALE = N_ALL ** -0.5
NOISE_GAIN = 6.0 * DP ** 0.5
ADAM_BETA1 = 0.9
ADAM_BETA2 = 0.98
ADAM_EPS = 1e-8
WEIGHT_DECAY = 0.01
MAX_NORM = 1.0
NORM_EPS = 1e-6
BIAS_ONE = 1.0 - ADAM_BETA1 ** STEP
BIAS_TWO = 1.0 - ADAM_BETA2 ** STEP


def draw_local_grads(draw_key, elem_count):
    key_base, key_dev = jax.random.split(draw_key)
    base_part = 2.0 * jax.random.normal(key_base, (elem_count,), jnp.float32)
    dev_keys = jax.random.split(key_dev, DP)

    def one_device(dev_key):
        noise_part = jax.random.normal(dev_key, (elem_count,), jnp.float32)
        return ((base_part + NOISE_GAIN * noise_part) * ELEM_SCALE).astype(jnp.bfloat16)

    return lax.map(one_device, dev_keys)


def setup_inputs(seed: int = 0) -> dict:
    key_list = jax.random.split(jax.random.key(seed), 9)
    return dict(
        g_mat=draw_local_grads(key_list[0], N_MAT),
        g_vec=draw_local_grads(key_list[1], N_VEC),
        p_mat=0.02 * jax.random.normal(key_list[2], (N_MAT,), jnp.float32),
        m_mat=0.1 * ELEM_SCALE * jax.random.normal(key_list[3], (N_MAT,), jnp.float32),
        v_mat=0.05 * ELEM_SCALE * ELEM_SCALE * jax.random.uniform(key_list[4], (N_MAT,), jnp.float32, minval=0.25, maxval=1.75),
        p_vec=0.05 * jax.random.normal(key_list[5], (N_VEC,), jnp.float32),
        m_vec=0.1 * ELEM_SCALE * jax.random.normal(key_list[6], (N_VEC,), jnp.float32),
        v_vec=0.05 * ELEM_SCALE * ELEM_SCALE * jax.random.uniform(key_list[7], (N_VEC,), jnp.float32, minval=0.25, maxval=1.75),
        learn_rate=jax.random.uniform(key_list[8], (), jnp.float32, minval=0.002, maxval=0.008),
    )


def mean_over_devices(local_grads):
    def add_row(acc_sum, grad_row):
        return acc_sum + grad_row.astype(jnp.float32), None

    total_sum, _ = lax.scan(add_row, jnp.zeros(local_grads.shape[1:], jnp.float32), local_grads)
    return total_sum / local_grads.shape[0]


def adam_update(grad_vals, param_vals, moment_one, moment_two, learn_rate, decay_rate):
    new_one = ADAM_BETA1 * moment_one + (1.0 - ADAM_BETA1) * grad_vals
    new_two = ADAM_BETA2 * moment_two + (1.0 - ADAM_BETA2) * grad_vals * grad_vals
    direction = (new_one / BIAS_ONE) / (jnp.sqrt(new_two / BIAS_TWO) + ADAM_EPS)
    return param_vals - learn_rate * (direction + decay_rate * param_vals), new_one, new_two


def reference(g_mat, g_vec, p_mat, m_mat, v_mat, p_vec, m_vec, v_vec, learn_rate):
    grad_mat = mean_over_devices(g_mat)
    grad_vec = mean_over_devices(g_vec)
    norm_sq = jnp.sum(grad_mat * grad_mat) + jnp.sum(grad_vec * grad_vec)
    clip_scale = jnp.minimum(1.0, MAX_NORM / (jnp.sqrt(norm_sq) + NORM_EPS))
    new_p_mat, new_m_mat, new_v_mat = adam_update(grad_mat * clip_scale, p_mat, m_mat, v_mat, learn_rate, WEIGHT_DECAY)
    new_p_vec, new_m_vec, new_v_vec = adam_update(grad_vec * clip_scale, p_vec, m_vec, v_vec, learn_rate, 0.0)
    return (new_p_mat, new_m_mat, new_v_mat, new_p_vec, new_m_vec, new_v_vec, new_p_mat.astype(jnp.bfloat16))
```

```python
import jax
import jax.numpy as jnp
from jax import lax
from jax.experimental import pallas as pl
from jax.experimental.pallas import tpu as pltpu
from jax.sharding import PartitionSpec as P

STEP = 10
ADAM_BETA1 = 0.9
ADAM_BETA2 = 0.98
ADAM_EPS = 1e-8
WEIGHT_DECAY = 0.01
MAX_NORM = 1.0
NORM_EPS = 1e-6
BIAS_ONE = 1.0 - ADAM_BETA1 ** STEP
BIAS_TWO = 1.0 - ADAM_BETA2 ** STEP

DP = 32
PIECE = 2400
CHUNKS = 15
ROWS = PIECE // CHUNKS
HALF = ROWS // 2
RAB = 32
RCD = HALF - RAB
VEC = 130
VPAD = 136
MESH = pl.DeviceIdType.MESH
F32 = jnp.float32
BF16 = jnp.bfloat16


def adam_update(grad_vals, param_vals, moment_one, moment_two, learn_rate, decay_rate):
    new_one = ADAM_BETA1 * moment_one + (1.0 - ADAM_BETA1) * grad_vals
    new_two = ADAM_BETA2 * moment_two + (1.0 - ADAM_BETA2) * grad_vals * grad_vals
    direction = (new_one / BIAS_ONE) / (jnp.sqrt(new_two / BIAS_TWO) + ADAM_EPS)
    return param_vals - learn_rate * (direction + decay_rate * param_vals), new_one, new_two


def kernel(g, gv, p, m, v, pv, mv, vv, lr,
           po, mo, vo, pvo, mvo, vvo, pb,
           stage, dense, pab, pcd, abz, er, cdr, abr, fr, gsum, ssq, clip, vs, vr, ns, nr,
           in_sem, pmv_sem, s0_send, s0_recv, rs_send, er_recv, cd_recv, ab_recv, f_recv,
           vec_send, vec_recv, norm_send, norm_recv,
           ag_send, ag_ab, ag_cd, ag_cd1, ag_ab2, ag_ab3, ag_cd3, ag_d2d):
    me = lax.axis_index("dp")
    c = me % 2
    x = (me // 2) % 2
    y = (me // 4) % 2
    z = me // 8

    def dev(zz, yy, xx, cc):
        return ((zz * 2 + yy) * 2 + xx) * 2 + cc

    partner = dev(z, y, x, 1 - c)
    xs = dev(z, y, 1 - x, c)
    xo = dev(z, y, 1 - x, 1 - c)
    ys = dev(z, 1 - y, x, c)
    yo = dev(z, 1 - y, x, 1 - c)
    up = dev((z + 1) % 4, y, x, c)
    down = dev((z + 3) % 4, y, x, c)
    z1 = dev(z + 1 - 2 * (z % 2), y, x, c)
    z2 = dev((z + 2) % 4, y, x, c)
    nlow = z >= 1
    nhigh = z <= 2

    def send(src, dst, ssem, rsem, to):
        pltpu.make_async_remote_copy(
            src_ref=src, dst_ref=dst, send_sem=ssem, recv_sem=rsem, device_id=(to,), device_id_type=MESH
        ).start()

    def wait(ref, sem):
        pltpu.make_async_copy(ref, ref, sem).wait()

    def fetch(k, slot):
        def one(d, carry):
            off = pl.multiple_of((d * PIECE + k * ROWS) * 128, 1024)
            pltpu.make_async_copy(g.at[0:1, pl.ds(off, ROWS * 128)], stage.at[slot, d], in_sem.at[slot]).start()
            return carry
        lax.fori_loop(0, DP, one, 0)

    fetch(0, 0)
    pltpu.make_async_copy(p, po, pmv_sem.at[0]).start()
    pltpu.make_async_copy(m, mo, pmv_sem.at[1]).start()
    pltpu.make_async_copy(v, vo, pmv_sem.at[2]).start()

    barrier = pltpu.get_barrier_semaphore()
    for nb in (partner, xs, xo, ys, yo, z2):
        pl.semaphore_signal(barrier, inc=1, device_id=(nb,), device_id_type=MESH)

    @pl.when(nhigh)
    def _():
        pl.semaphore_signal(barrier, inc=1, device_id=(up,), device_id_type=MESH)

    @pl.when(nlow)
    def _():
        pl.semaphore_signal(barrier, inc=1, device_id=(down,), device_id_type=MESH)

    vs[0, 0:128] = gv[0:1, 0:16384].astype(F32).reshape(128, 128)
    vs[0, 128:VPAD] = jnp.zeros((VPAD - 128, 128), F32)
    vs[0, 128:VEC] = gv[0:1, 16384:16640].astype(F32).reshape(2, 128)
    ssq[...] = jnp.zeros((8, 128), F32)

    mid = (z >= 1) & (z <= 2)

    @pl.when(mid)
    def _():
        pl.semaphore_wait(barrier, 8)

    @pl.when(jnp.logical_not(mid))
    def _():
        pl.semaphore_wait(barrier, 7)

    partners = (partner, xs, ys, z1, z2)

    def vec_step(j):
        if j > 0:
            wait(vr.at[j - 1], vec_recv.at[j - 1])
            vs[j] = vs[j - 1] + vr[j - 1]
        if j < 5:
            send(vs.at[j], vr.at[j], vec_send.at[j], vec_recv.at[j], partners[j])

    def rbuf(k, d, j):
        return pb.at[k // 4, (k // 2) % 2, k % 2, d, pl.ds(j * 8 * HALF, 8 * HALF)]

    def stage0(k):
        slot = k % 2
        dslot = k % 3

        @pl.when(k + 1 < CHUNKS)
        def _():
            fetch(k + 1, 1 - slot)

        @pl.when(k >= 3)
        def _():
            wait(dense.at[dslot, :, pl.ds(1, 3)], s0_send.at[dslot])

        wait(stage.at[slot], in_sem.at[slot])

        for d in range(2):
            for q in (3, 2, 1, 0):
                cc = (c, 1 - c, c, 1 - c)[q]
                far = q >= 2

                def conv(b, carry, d=d, q=q, cc=cc, far=far):
                    if d == 0:
                        piece = dev(b // 2, b % 2, 1 - x if far else x, cc)
                    else:
                        piece = dev(b // 2, 1 - y if far else y, b % 2, cc)
                    vals = stage[slot, piece, 0:1, d * HALF * 128:(d + 1) * HALF * 128].astype(F32)
                    row = pl.multiple_of(b * HALF, 16)
                    dense[dslot, d, q, pl.ds(row, HALF)] = vals.reshape(HALF, 128).astype(BF16)
                    return carry

                lax.fori_loop(0, 8, conv, 0)
                if q > 0:
                    to = ((partner, xs, xo), (partner, ys, yo))[d][q - 1]
                    send(dense.at[dslot, d, q], rbuf(k, d, q - 1), s0_send.at[dslot], s0_recv.at[k], to)

    def z_sends(k, t, bufs, recv, rsem):
        @pl.when(z <= t)
        def _():
            dest = 3 + z - t
            if t > 0:
                @pl.when(nlow)
                def _():
                    wait(recv.at[k, t - 1], rsem.at[k, t - 1])
                    bufs[k, dest] += recv[k, t - 1]
            send(bufs.at[k, dest], recv.at[k, t], rs_send.at[k], rsem.at[k, t], up)

        @pl.when(3 - z <= t)
        def _():
            dest = t - (3 - z)
            if t > 0:
                @pl.when(nhigh)
                def _():
                    old = 0 if t == 1 else t + 1
                    wait(recv.at[k, old], rsem.at[k, old])
                    bufs[k, dest] += recv[k, old]
            new = 0 if t == 0 else t + 2
            send(bufs.at[k, dest], recv.at[k, new], rs_send.at[k], rsem.at[k, new], down)

    def z_final(k, bufs, recv, rsem):
        @pl.when(nlow)
        def _():
            wait(recv.at[k, 2], rsem.at[k, 2])
            bufs[k, z] += recv[k, 2]

        @pl.when(nhigh)
        def _():
            wait(recv.at[k, 4], rsem.at[k, 4])
            bufs[k, z] += recv[k, 4]

    def stage1(k):
        dslot = k % 3
        wait(dense.at[dslot, :, pl.ds(1, 3)], s0_recv.at[k])
        for d in range(2):
            def add(b, carry, d=d):
                row = pl.multiple_of(b * HALF, 16)
                tot = dense[dslot, d, 0, pl.ds(row, HALF)].astype(F32)
                for j in range(3):
                    off = pl.multiple_of(j * 8 * HALF + b * HALF, 16)
                    tot = tot + pb[k // 4, (k // 2) % 2, k % 2, d, pl.ds(off, HALF)].astype(F32)
                pab[k, d, b % 2, b // 2] = tot[0:RAB]
                pcd[k, b // 2, d, b % 2] = tot[RAB:HALF]
                return carry
            lax.fori_loop(0, 8, add, 0)
        send(pab.at[k, 0, 1 - y], er.at[k, 0], rs_send.at[k], er_recv.at[k], ys)
        send(pab.at[k, 1, 1 - x], er.at[k, 1], rs_send.at[k], er_recv.at[k], xs)
        z_sends(k, 0, pcd, cdr, cd_recv)

    def stage2(k):
        z_sends(k, 1, pcd, cdr, cd_recv)
        wait(er.at[k], er_recv.at[k])
        for zz in range(4):
            abz[k, zz, 0] = pab[k, 0, y, zz] + er[k, 0, zz]
            abz[k, zz, 1] = pab[k, 1, x, zz] + er[k, 1, zz]
        z_sends(k, 0, abz, abr, ab_recv)

    def stage3(k):
        z_sends(k, 2, pcd, cdr, cd_recv)
        z_sends(k, 1, abz, abr, ab_recv)

    def stage4(k):
        z_final(k, pcd, cdr, cd_recv)
        send(pcd.at[k, z, 0, 1 - y], fr.at[k, 0], rs_send.at[k], f_recv.at[k], ys)
        send(pcd.at[k, z, 1, 1 - x], fr.at[k, 1], rs_send.at[k], f_recv.at[k], xs)
        z_sends(k, 2, abz, abr, ab_recv)

    def stage5(k):
        z_final(k, abz, abr, ab_recv)
        wait(fr.at[k], f_recv.at[k])
        base = pl.multiple_of(k * ROWS, 16)
        parts = (
            (0, RAB, abz[k, z, 0]),
            (RAB, RCD, pcd[k, z, 0, y] + fr[k, 0]),
            (HALF, RAB, abz[k, z, 1]),
            (HALF + RAB, RCD, pcd[k, z, 1, x] + fr[k, 1]),
        )
        acc = ssq[...]
        for off, num, val in parts:
            val = val * (1.0 / DP)
            gsum[pl.ds(base + off, num)] = val
            acc = acc + jnp.sum((val * val).reshape(num // 8, 8, 128), axis=0)
        ssq[...] = acc

    def rs_iter(i, carry):
        for s, fn in enumerate((stage0, stage1, stage2, stage3, stage4, stage5)):
            k = i - s

            @pl.when((k >= 0) & (k < CHUNKS))
            def _(fn=fn, k=k):
                fn(k)
        for j in range(6):
            @pl.when(i == 1 + 2 * j)
            def _(j=j):
                vec_step(j)
        return carry

    lax.fori_loop(0, CHUNKS + 5, rs_iter, 0)

    ns[0] = ssq[...]
    for j in range(5):
        send(ns.at[j], nr.at[j], norm_send.at[j], norm_recv.at[j], partners[j])
        wait(nr.at[j], norm_recv.at[j])
        ns[j + 1] = ns[j] + nr[j]
    gvec = vs[5, 0:VEC] * (1.0 / DP)
    norm_sq = jnp.full((8, 128), jnp.sum(ns[5]) + jnp.sum(gvec * gvec))
    clip[...] = jnp.minimum(1.0, MAX_NORM / (jnp.sqrt(norm_sq) + NORM_EPS))
    rate = lr[0, 0]

    wait(po, pmv_sem.at[0])
    wait(mo, pmv_sem.at[1])
    wait(vo, pmv_sem.at[2])

    def ag_rows(k, off, num):
        return pl.ds(pl.multiple_of(k * ROWS + off, 16), num)

    full = slice(None)

    def region(zz, yy, xx, rows):
        return pb.at[zz, yy, xx, c, rows]

    def push(ref, k, rsem, to):
        send(ref, ref, ag_send.at[k], rsem, to)

    def ag0(k):
        def upd(b, carry):
            rows = pl.ds(pl.multiple_of(k * ROWS + b * 32, 16), 32)
            new = adam_update(gsum[rows] * clip[0:1], po[rows], mo[rows], vo[rows], rate, WEIGHT_DECAY)
            po[rows], mo[rows], vo[rows] = new
            pb[z, y, x, c, rows] = new[0].astype(BF16)
            return carry
        lax.fori_loop(0, ROWS // 32, upd, 0)
        ab = ag_rows(k, 0, 2 * RAB)

        @pl.when(nhigh)
        def _():
            push(region(z, y, x, ab), k, ag_ab.at[k, 0, 0], up)

        @pl.when(nlow)
        def _():
            push(region(z, y, x, ab), k, ag_ab.at[k, 1, 0], down)

        push(region(z, y, x, ag_rows(k, 2 * RAB, RCD)), k, ag_cd1.at[k], ys)
        push(region(z, y, x, ag_rows(k, 2 * RAB + RCD, RCD)), k, ag_cd1.at[k], xs)

    def z_ab(k, t):
        ab = ag_rows(k, 0, 2 * RAB)
        one = region(0, 0, 0, ab)

        @pl.when(z - 1 - t >= 0)
        def _():
            wait(one, ag_ab.at[k, 0, t])
            if t < 2:
                @pl.when(nhigh)
                def _():
                    push(region(z - 1 - t, y, x, ab), k, ag_ab.at[k, 0, t + 1], up)

        @pl.when(z + 1 + t <= 3)
        def _():
            wait(one, ag_ab.at[k, 1, t])
            if t < 2:
                @pl.when(nlow)
                def _():
                    push(region(z + 1 + t, y, x, ab), k, ag_ab.at[k, 1, t + 1], down)

    def cd_push(k, zz, d, t, to):
        push(region(zz, full, x, ag_rows(k, 2 * RAB, RCD)), k, ag_cd.at[k, d, t], to)
        push(region(zz, y, full, ag_rows(k, 2 * RAB + RCD, RCD)), k, ag_cd.at[k, d, t], to)

    def z_cd(k, t):
        both = pb.at[0, 0, full, full, ag_rows(k, 2 * RAB, RCD)]

        @pl.when(z - 1 - t >= 0)
        def _():
            wait(both, ag_cd.at[k, 0, t])
            if t < 2:
                @pl.when(nhigh)
                def _():
                    cd_push(k, z - 1 - t, 0, t + 1, up)

        @pl.when(z + 1 + t <= 3)
        def _():
            wait(both, ag_cd.at[k, 1, t])
            if t < 2:
                @pl.when(nlow)
                def _():
                    cd_push(k, z + 1 + t, 1, t + 1, down)

    def ag1(k):
        wait(pb.at[0, 0, 0, full, ag_rows(k, 2 * RAB, RCD)], ag_cd1.at[k])

        @pl.when(nhigh)
        def _():
            cd_push(k, z, 0, 0, up)

        @pl.when(nlow)
        def _():
            cd_push(k, z, 1, 0, down)

        z_ab(k, 0)

    def ag2(k):
        z_ab(k, 1)
        z_cd(k, 0)

    def ag3(k):
        z_ab(k, 2)
        ra = ag_rows(k, 0, RAB)
        rb = ag_rows(k, RAB, RAB)
        push(region(full, y, x, ra), k, ag_ab2.at[k], ys)
        push(region(full, y, x, rb), k, ag_ab2.at[k], xs)
        push(region(full, y, x, ag_rows(k, 0, 2 * RAB)), k, ag_d2d.at[k], partner)
        z_cd(k, 1)

    def ag4(k):
        ra = ag_rows(k, 0, RAB)
        rb = ag_rows(k, RAB, RAB)
        rc = ag_rows(k, 2 * RAB, RCD)
        rd = ag_rows(k, 2 * RAB + RCD, RCD)
        wait(pb.at[0, 0, full, full, ag_rows(k, 0, 2 * RAB)], ag_ab2.at[k])
        push(region(full, full, x, ra), k, ag_ab3.at[k], xs)
        push(region(full, y, full, rb), k, ag_ab3.at[k], ys)
        push(region(full, 1 - y, x, ra), k, ag_d2d.at[k], partner)
        push(region(full, y, 1 - x, rb), k, ag_d2d.at[k], partner)
        z_cd(k, 2)
        push(region(full, full, x, rc), k, ag_cd3.at[k], xs)
        push(region(full, y, full, rd), k, ag_cd3.at[k], ys)
        push(region(full, full, x, rc), k, ag_d2d.at[k], partner)
        push(region(full, y, full, rd), k, ag_d2d.at[k], partner)

    def ag5(k):
        wait(pb.at[0, full, full, full, ag_rows(k, 0, 2 * RAB)], ag_ab3.at[k])
        push(region(full, full, 1 - x, ag_rows(k, 0, RAB)), k, ag_d2d.at[k], partner)
        push(region(full, 1 - y, full, ag_rows(k, RAB, RAB)), k, ag_d2d.at[k], partner)
        wait(pb.at[full, full, full, 0, ag_rows(k, 2 * RAB, RCD)], ag_cd3.at[k])
        push(region(full, full, 1 - x, ag_rows(k, 2 * RAB, RCD)), k, ag_d2d.at[k], partner)
        push(region(full, 1 - y, full, ag_rows(k, 2 * RAB + RCD, RCD)), k, ag_d2d.at[k], partner)

    def ag_iter(i, carry):
        for s, fn in enumerate((ag0, ag1, ag2, ag3, ag4, ag5)):
            k = i - s

            @pl.when((k >= 0) & (k < CHUNKS))
            def _(fn=fn, k=k):
                fn(k)
        return carry

    lax.fori_loop(0, CHUNKS + 5, ag_iter, 0)

    newv = adam_update(gvec * clip[0:1], pv[...], mv[...], vv[...], rate, 0.0)
    pvo[...], mvo[...], vvo[...] = newv

    def drain(k, carry):
        wait(pb.at[full, full, full, 0, ag_rows(k, 0, ROWS)], ag_d2d.at[k])
        @pl.when(mid)
        def _():
            wait(pb.at[0, 0, full, full, pl.ds(0, 1368)], ag_send.at[k])

        @pl.when(jnp.logical_not(mid))
        def _():
            wait(pb.at[0, 0, 0, full, pl.ds(0, 2224)], ag_send.at[k])

        wait(gsum.at[pl.ds(0, 1120)], rs_send.at[k])
        return carry

    lax.fori_loop(0, CHUNKS, drain, 0)
    for s in range(3):
        wait(dense.at[s, :, pl.ds(1, 3)], s0_send.at[s])
    for j in range(5):
        wait(vs.at[j], vec_send.at[j])
        wait(ns.at[j], norm_send.at[j])


def solution(mesh):
    axis_name = mesh.axis_names[0]
    vm = pl.BlockSpec(memory_space=pltpu.VMEM)
    hbm = pl.BlockSpec(memory_space=pl.ANY)
    dma = pltpu.SemaphoreType.DMA
    K = CHUNKS

    call = pl.pallas_call(
        kernel,
        name="adam_step",
        out_shape=(
            [pltpu.VMEM((PIECE, 128), F32)] * 3
            + [pltpu.VMEM((VEC, 128), F32)] * 3
            + [pltpu.VMEM((4, 2, 2, 2, PIECE, 128), BF16)]
        ),
        in_specs=[hbm, vm, hbm, hbm, hbm, vm, vm, vm, pl.BlockSpec(memory_space=pltpu.SMEM)],
        out_specs=[vm] * 7,
        scratch_shapes=[
            pltpu.VMEM((2, DP, 1, ROWS * 128), BF16),
            pltpu.VMEM((3, 2, 4, 8 * HALF, 128), BF16),
            pltpu.VMEM((K, 2, 2, 4, RAB, 128), F32),
            pltpu.VMEM((K, 4, 2, 2, RCD, 128), F32),
            pltpu.VMEM((K, 4, 2, RAB, 128), F32),
            pltpu.VMEM((K, 2, 4, RAB, 128), F32),
            pltpu.VMEM((K, 5, 2, 2, RCD, 128), F32),
            pltpu.VMEM((K, 5, 2, RAB, 128), F32),
            pltpu.VMEM((K, 2, RCD, 128), F32),
            pltpu.VMEM((PIECE, 128), F32),
            pltpu.VMEM((8, 128), F32),
            pltpu.VMEM((8, 128), F32),
            pltpu.VMEM((6, VPAD, 128), F32),
            pltpu.VMEM((5, VPAD, 128), F32),
            pltpu.VMEM((6, 8, 128), F32),
            pltpu.VMEM((5, 8, 128), F32),
            dma((2,)), dma((3,)), dma((3,)), dma((K,)), dma((K,)), dma((K,)), dma((K, 5)), dma((K, 5)), dma((K,)),
            dma((5,)), dma((5,)), dma((5,)), dma((5,)),
            dma((K,)), dma((K, 2, 3)), dma((K, 2, 3)), dma((K,)), dma((K,)), dma((K,)), dma((K,)), dma((K,)),
        ],
        compiler_params=pltpu.CompilerParams(
            collective_id=0, has_side_effects=True, vmem_limit_bytes=37 * 2 ** 20
        ),
    )

    def local_step(g_mat, g_vec, p_mat, m_mat, v_mat, p_vec, m_vec, v_vec, learn_rate):
        outs = call(
            g_mat, g_vec,
            p_mat.reshape(PIECE, 128), m_mat.reshape(PIECE, 128), v_mat.reshape(PIECE, 128),
            p_vec.reshape(VEC, 128), m_vec.reshape(VEC, 128), v_vec.reshape(VEC, 128),
            learn_rate.reshape(1, 1),
        )
        return tuple(o.reshape(-1) for o in outs)

    return jax.shard_map(
        local_step,
        mesh=mesh,
        in_specs=(P(axis_name, None), P(axis_name, None), P(axis_name), P(axis_name), P(axis_name), P(), P(), P(), P()),
        out_specs=(P(axis_name), P(axis_name), P(axis_name), P(), P(), P(), P()),
        check_vma=False,
    )
```

```python
import jax
import jax.numpy as jnp
from jax import lax
from jax.experimental import pallas as pl
from jax.experimental.pallas import tpu as pltpu
from jax.sharding import PartitionSpec as P

STEP = 10
ADAM_BETA1 = 0.9
ADAM_BETA2 = 0.98
ADAM_EPS = 1e-8
WEIGHT_DECAY = 0.01
MAX_NORM = 1.0
NORM_EPS = 1e-6
BIAS_ONE = 1.0 - ADAM_BETA1 ** STEP
BIAS_TWO = 1.0 - ADAM_BETA2 ** STEP

DP = 32
PIECE = 2400
CHUNKS = 25
ROWS = PIECE // CHUNKS
HALF = ROWS // 2
RAB = 16
RCD = HALF - RAB
VEC = 130
VPAD = 136
MESH = pl.DeviceIdType.MESH
F32 = jnp.float32
BF16 = jnp.bfloat16


def adam_update(grad_vals, param_vals, moment_one, moment_two, learn_rate, decay_rate):
    new_one = ADAM_BETA1 * moment_one + (1.0 - ADAM_BETA1) * grad_vals
    new_two = ADAM_BETA2 * moment_two + (1.0 - ADAM_BETA2) * grad_vals * grad_vals
    direction = (new_one / BIAS_ONE) / (jnp.sqrt(new_two / BIAS_TWO) + ADAM_EPS)
    return param_vals - learn_rate * (direction + decay_rate * param_vals), new_one, new_two


def kernel(g, gv, p, m, v, pv, mv, vv, lr,
           po, mo, vo, pvo, mvo, vvo, pb,
           stage, dense, pab, pcd, abz, er, cdr, abr, fr, gsum, ssq, clip, vs, vr, ns, nr,
           in_sem, pmv_sem, s0_send, s0_recv, rs_send, er_recv, cd_recv, ab_recv, f_recv,
           vec_send, vec_recv, norm_send, norm_recv,
           ag_send, ag_ab, ag_cd, ag_cd1, ag_ab2, ag_ab3, ag_cd3, ag_d2d):
    me = lax.axis_index("dp")
    c = me % 2
    x = (me // 2) % 2
    y = (me // 4) % 2
    z = me // 8

    def dev(zz, yy, xx, cc):
        return ((zz * 2 + yy) * 2 + xx) * 2 + cc

    partner = dev(z, y, x, 1 - c)
    xs = dev(z, y, 1 - x, c)
    xo = dev(z, y, 1 - x, 1 - c)
    ys = dev(z, 1 - y, x, c)
    yo = dev(z, 1 - y, x, 1 - c)
    up = dev((z + 1) % 4, y, x, c)
    down = dev((z + 3) % 4, y, x, c)
    z1 = dev(z + 1 - 2 * (z % 2), y, x, c)
    z2 = dev((z + 2) % 4, y, x, c)
    nlow = z >= 1
    nhigh = z <= 2

    def send(src, dst, ssem, rsem, to):
        pltpu.make_async_remote_copy(
            src_ref=src, dst_ref=dst, send_sem=ssem, recv_sem=rsem, device_id=(to,), device_id_type=MESH
        ).start()

    def wait(ref, sem):
        pltpu.make_async_copy(ref, ref, sem).wait()

    def fetch(k, slot):
        def one(d, carry):
            off = pl.multiple_of((d * PIECE + k * ROWS) * 128, 1024)
            pltpu.make_async_copy(g.at[0:1, pl.ds(off, ROWS * 128)], stage.at[slot, d], in_sem.at[slot]).start()
            return carry
        lax.fori_loop(0, DP, one, 0)

    fetch(0, 0)
    pltpu.make_async_copy(p, po, pmv_sem.at[0]).start()
    pltpu.make_async_copy(m, mo, pmv_sem.at[1]).start()
    pltpu.make_async_copy(v, vo, pmv_sem.at[2]).start()

    barrier = pltpu.get_barrier_semaphore()
    for nb in (partner, xs, xo, ys, yo, z2):
        pl.semaphore_signal(barrier, inc=1, device_id=(nb,), device_id_type=MESH)

    @pl.when(nhigh)
    def _():
        pl.semaphore_signal(barrier, inc=1, device_id=(up,), device_id_type=MESH)

    @pl.when(nlow)
    def _():
        pl.semaphore_signal(barrier, inc=1, device_id=(down,), device_id_type=MESH)

    vs[0, 0:128] = gv[0:1, 0:16384].astype(F32).reshape(128, 128)
    vs[0, 128:VPAD] = jnp.zeros((VPAD - 128, 128), F32)
    vs[0, 128:VEC] = gv[0:1, 16384:16640].astype(F32).reshape(2, 128)
    ssq[...] = jnp.zeros((8, 128), F32)

    mid = (z >= 1) & (z <= 2)

    def await_neighbours():
        @pl.when(mid)
        def _():
            pl.semaphore_wait(barrier, 8)

        @pl.when(jnp.logical_not(mid))
        def _():
            pl.semaphore_wait(barrier, 7)

    partners = (partner, xs, ys, z1, z2)

    def vec_step(j):
        if j > 0:
            wait(vr.at[j - 1], vec_recv.at[j - 1])
            vs[j] = vs[j - 1] + vr[j - 1]
        if j < 5:
            send(vs.at[j], vr.at[j], vec_send.at[j], vec_recv.at[j], partners[j])

    per = PIECE // (24 * HALF)

    def rpiece(k, d):
        at = (2 * k + d) // per
        return at // 8, (at // 4) % 2, (at // 2) % 2, at % 2

    def roff(k, d):
        return ((2 * k + d) % per) * 24 * HALF

    def rbuf(k, d, j):
        return pb.at[(*rpiece(k, d), pl.ds(roff(k, d) + j * 8 * HALF, 8 * HALF))]

    def convert(k):
        slot = k % 2
        dslot = k % 3

        @pl.when(k + 1 < CHUNKS)
        def _():
            fetch(k + 1, 1 - slot)

        @pl.when(k >= 3)
        def _():
            wait(dense.at[dslot, :, pl.ds(1, 3)], s0_send.at[dslot])

        wait(stage.at[slot], in_sem.at[slot])

        def conv(b, carry):
            row = pl.multiple_of(b * HALF, 16)
            for d in range(2):
                for q in range(4):
                    cc = 1 - c if q % 2 else c
                    if d == 0:
                        piece = dev(b // 2, b % 2, 1 - x if q >= 2 else x, cc)
                    else:
                        piece = dev(b // 2, 1 - y if q >= 2 else y, b % 2, cc)
                    vals = stage[slot, piece, 0:1, d * HALF * 128:(d + 1) * HALF * 128].astype(F32)
                    dense[dslot, d, q, pl.ds(row, HALF)] = vals.reshape(HALF, 128).astype(BF16)
            return carry

        lax.fori_loop(0, 8, conv, 0)

    def stage0(k):
        dslot = k % 3
        for q in (3, 2, 1):
            for d in range(2):
                to = ((partner, xs, xo), (partner, ys, yo))[d][q - 1]
                send(dense.at[dslot, d, q], rbuf(k, d, q - 1), s0_send.at[dslot], s0_recv.at[k], to)

        @pl.when(k + 1 < CHUNKS)
        def _():
            convert(k + 1)

    def z_sends(k, t, bufs, recv, rsem):
        @pl.when(z <= t)
        def _():
            dest = 3 + z - t
            if t > 0:
                @pl.when(nlow)
                def _():
                    wait(recv.at[k, t - 1], rsem.at[k, t - 1])
                    bufs[k, dest] += recv[k, t - 1]
            send(bufs.at[k, dest], recv.at[k, t], rs_send.at[k], rsem.at[k, t], up)

        @pl.when(3 - z <= t)
        def _():
            dest = t - (3 - z)
            if t > 0:
                @pl.when(nhigh)
                def _():
                    old = 0 if t == 1 else t + 1
                    wait(recv.at[k, old], rsem.at[k, old])
                    bufs[k, dest] += recv[k, old]
            new = 0 if t == 0 else t + 2
            send(bufs.at[k, dest], recv.at[k, new], rs_send.at[k], rsem.at[k, new], down)

    def z_final(k, bufs, recv, rsem):
        @pl.when(nlow)
        def _():
            wait(recv.at[k, 2], rsem.at[k, 2])
            bufs[k, z] += recv[k, 2]

        @pl.when(nhigh)
        def _():
            wait(recv.at[k, 4], rsem.at[k, 4])
            bufs[k, z] += recv[k, 4]

    def stage1(k):
        dslot = k % 3
        wait(dense.at[dslot, :, pl.ds(1, 3)], s0_recv.at[k])
        for d in range(2):
            def add(b, carry, d=d):
                row = pl.multiple_of(b * HALF, 16)
                tot = dense[dslot, d, 0, pl.ds(row, HALF)].astype(F32)
                for j in range(3):
                    off = pl.multiple_of(roff(k, d) + j * 8 * HALF + b * HALF, 16)
                    tot = tot + pb[(*rpiece(k, d), pl.ds(off, HALF))].astype(F32)
                pab[k, d, b % 2, b // 2] = tot[0:RAB]
                pcd[k, b // 2, d, b % 2] = tot[RAB:HALF]
                return carry
            lax.fori_loop(0, 8, add, 0)
        send(pab.at[k, 0, 1 - y], er.at[k, 0], rs_send.at[k], er_recv.at[k], ys)
        send(pab.at[k, 1, 1 - x], er.at[k, 1], rs_send.at[k], er_recv.at[k], xs)
        z_sends(k, 0, pcd, cdr, cd_recv)

    def stage2(k):
        z_sends(k, 1, pcd, cdr, cd_recv)
        wait(er.at[k], er_recv.at[k])
        for zz in range(4):
            abz[k, zz, 0] = pab[k, 0, y, zz] + er[k, 0, zz]
            abz[k, zz, 1] = pab[k, 1, x, zz] + er[k, 1, zz]
        z_sends(k, 0, abz, abr, ab_recv)

    def stage3(k):
        z_sends(k, 2, pcd, cdr, cd_recv)
        z_sends(k, 1, abz, abr, ab_recv)

    def stage4(k):
        z_final(k, pcd, cdr, cd_recv)
        send(pcd.at[k, z, 0, 1 - y], fr.at[k, 0], rs_send.at[k], f_recv.at[k], ys)
        send(pcd.at[k, z, 1, 1 - x], fr.at[k, 1], rs_send.at[k], f_recv.at[k], xs)
        z_sends(k, 2, abz, abr, ab_recv)

    def stage5(k):
        z_final(k, abz, abr, ab_recv)
        wait(fr.at[k], f_recv.at[k])
        base = pl.multiple_of(k * ROWS, 16)
        parts = (
            (0, RAB, abz[k, z, 0]),
            (RAB, RCD, pcd[k, z, 0, y] + fr[k, 0]),
            (HALF, RAB, abz[k, z, 1]),
            (HALF + RAB, RCD, pcd[k, z, 1, x] + fr[k, 1]),
        )
        acc = ssq[...]
        for off, num, val in parts:
            val = val * (1.0 / DP)
            gsum[pl.ds(base + off, num)] = val
            acc = acc + jnp.sum((val * val).reshape(num // 8, 8, 128), axis=0)
        ssq[...] = acc

    def rs_iter(i, carry):
        for s, fn in enumerate((stage0, stage1, stage2, stage3, stage4, stage5)):
            k = i - s

            @pl.when((k >= 0) & (k < CHUNKS))
            def _(fn=fn, k=k):
                fn(k)
        for j in range(6):
            @pl.when(i == 1 + 2 * j)
            def _(j=j):
                vec_step(j)
        return carry

    convert(0)
    await_neighbours()
    lax.fori_loop(0, CHUNKS + 5, rs_iter, 0)

    ns[...] = jnp.sum(ssq[...], axis=0, keepdims=True)
    nr[me] = ns[...]

    def tell(j, carry):
        send(ns, nr.at[me], norm_send, norm_recv, (me + j) % DP)
        return carry

    lax.fori_loop(1, DP, tell, 0)
    wait(nr.at[pl.ds(0, DP - 1)], norm_recv)
    gvec = vs[5, 0:VEC] * (1.0 / DP)
    norm_sq = jnp.full((8, 128), jnp.sum(nr[...]) + jnp.sum(gvec * gvec))
    clip[...] = jnp.minimum(1.0, MAX_NORM / (jnp.sqrt(norm_sq) + NORM_EPS))
    rate = lr[0, 0]

    wait(po, pmv_sem.at[0])
    wait(mo, pmv_sem.at[1])
    wait(vo, pmv_sem.at[2])

    def ag_rows(k, off, num):
        return pl.ds(pl.multiple_of(k * ROWS + off, 16), num)

    full = slice(None)

    def region(zz, yy, xx, rows):
        return pb.at[zz, yy, xx, c, rows]

    def push(ref, k, rsem, to):
        send(ref, ref, ag_send.at[k], rsem, to)

    def ag0(k):
        def upd(b, carry):
            rows = pl.ds(pl.multiple_of(k * ROWS + b * 32, 16), 32)
            new = adam_update(gsum[rows] * clip[0:1], po[rows], mo[rows], vo[rows], rate, WEIGHT_DECAY)
            po[rows], mo[rows], vo[rows] = new
            pb[z, y, x, c, rows] = new[0].astype(BF16)
            return carry
        lax.fori_loop(0, ROWS // 32, upd, 0)
        ab = ag_rows(k, 0, 2 * RAB)

        @pl.when(nhigh)
        def _():
            push(region(z, y, x, ab), k, ag_ab.at[k, 0, 0], up)

        @pl.when(nlow)
        def _():
            push(region(z, y, x, ab), k, ag_ab.at[k, 1, 0], down)

        push(region(z, y, x, ag_rows(k, 2 * RAB, RCD)), k, ag_cd1.at[k], ys)
        push(region(z, y, x, ag_rows(k, 2 * RAB + RCD, RCD)), k, ag_cd1.at[k], xs)

    def z_ab(k, t):
        ab = ag_rows(k, 0, 2 * RAB)
        one = region(0, 0, 0, ab)

        @pl.when(z - 1 - t >= 0)
        def _():
            wait(one, ag_ab.at[k, 0, t])
            if t < 2:
                @pl.when(nhigh)
                def _():
                    push(region(z - 1 - t, y, x, ab), k, ag_ab.at[k, 0, t + 1], up)

        @pl.when(z + 1 + t <= 3)
        def _():
            wait(one, ag_ab.at[k, 1, t])
            if t < 2:
                @pl.when(nlow)
                def _():
                    push(region(z + 1 + t, y, x, ab), k, ag_ab.at[k, 1, t + 1], down)

    def cd_push(k, zz, d, t, to):
        push(region(zz, full, x, ag_rows(k, 2 * RAB, RCD)), k, ag_cd.at[k, d, t], to)
        push(region(zz, y, full, ag_rows(k, 2 * RAB + RCD, RCD)), k, ag_cd.at[k, d, t], to)

    def z_cd(k, t):
        both = pb.at[0, 0, full, full, ag_rows(k, 2 * RAB, RCD)]

        @pl.when(z - 1 - t >= 0)
        def _():
            wait(both, ag_cd.at[k, 0, t])
            if t < 2:
                @pl.when(nhigh)
                def _():
                    cd_push(k, z - 1 - t, 0, t + 1, up)

        @pl.when(z + 1 + t <= 3)
        def _():
            wait(both, ag_cd.at[k, 1, t])
            if t < 2:
                @pl.when(nlow)
                def _():
                    cd_push(k, z + 1 + t, 1, t + 1, down)

    def ag1(k):
        wait(pb.at[0, 0, 0, full, ag_rows(k, 2 * RAB, RCD)], ag_cd1.at[k])

        @pl.when(nhigh)
        def _():
            cd_push(k, z, 0, 0, up)

        @pl.when(nlow)
        def _():
            cd_push(k, z, 1, 0, down)

        z_ab(k, 0)

    def ag2(k):
        z_ab(k, 1)
        z_cd(k, 0)

    def ag3(k):
        z_ab(k, 2)
        ra = ag_rows(k, 0, RAB)
        rb = ag_rows(k, RAB, RAB)
        push(region(full, y, x, ra), k, ag_ab2.at[k], ys)
        push(region(full, y, x, rb), k, ag_ab2.at[k], xs)
        push(region(full, y, x, ag_rows(k, 0, 2 * RAB)), k, ag_d2d.at[k], partner)
        z_cd(k, 1)

    def ag4(k):
        ra = ag_rows(k, 0, RAB)
        rb = ag_rows(k, RAB, RAB)
        rc = ag_rows(k, 2 * RAB, RCD)
        rd = ag_rows(k, 2 * RAB + RCD, RCD)
        wait(pb.at[0, 0, full, full, ag_rows(k, 0, 2 * RAB)], ag_ab2.at[k])
        push(region(full, full, x, ra), k, ag_ab3.at[k], xs)
        push(region(full, y, full, rb), k, ag_ab3.at[k], ys)
        push(region(full, 1 - y, x, ra), k, ag_d2d.at[k], partner)
        push(region(full, y, 1 - x, rb), k, ag_d2d.at[k], partner)
        z_cd(k, 2)
        push(region(full, full, x, rc), k, ag_cd3.at[k], xs)
        push(region(full, y, full, rd), k, ag_cd3.at[k], ys)
        push(region(full, full, x, rc), k, ag_d2d.at[k], partner)
        push(region(full, y, full, rd), k, ag_d2d.at[k], partner)

    def ag5(k):
        wait(pb.at[0, full, full, full, ag_rows(k, 0, 2 * RAB)], ag_ab3.at[k])
        push(region(full, full, 1 - x, ag_rows(k, 0, RAB)), k, ag_d2d.at[k], partner)
        push(region(full, 1 - y, full, ag_rows(k, RAB, RAB)), k, ag_d2d.at[k], partner)
        wait(pb.at[full, full, full, 0, ag_rows(k, 2 * RAB, RCD)], ag_cd3.at[k])
        push(region(full, full, 1 - x, ag_rows(k, 2 * RAB, RCD)), k, ag_d2d.at[k], partner)
        push(region(full, 1 - y, full, ag_rows(k, 2 * RAB + RCD, RCD)), k, ag_d2d.at[k], partner)

    def ag_iter(i, carry):
        for s, fn in enumerate((ag0, ag1, ag2, ag3, ag4, ag5)):
            k = i - s

            @pl.when((k >= 0) & (k < CHUNKS))
            def _(fn=fn, k=k):
                fn(k)
        return carry

    lax.fori_loop(0, CHUNKS + 5, ag_iter, 0)

    newv = adam_update(gvec * clip[0:1], pv[...], mv[...], vv[...], rate, 0.0)
    pvo[...], mvo[...], vvo[...] = newv

    def drain(k, carry):
        wait(pb.at[full, full, full, 0, ag_rows(k, 0, ROWS)], ag_d2d.at[k])
        base, along = 24 * RAB + 18 * RCD + 16 * ROWS, 2 * RAB + 4 * RCD

        @pl.when(mid)
        def _():
            wait(pb.at[0, 0, full, full, pl.ds(0, (base + 5 * along) // 4)], ag_send.at[k])

        @pl.when(jnp.logical_not(mid))
        def _():
            wait(pb.at[0, 0, 0, full, pl.ds(0, (base + along) // 2)], ag_send.at[k])

        wait(gsum.at[pl.ds(0, 14 * HALF)], rs_send.at[k])
        return carry

    lax.fori_loop(0, CHUNKS, drain, 0)
    for s in range(3):
        wait(dense.at[s, :, pl.ds(1, 3)], s0_send.at[s])
    for j in range(5):
        wait(vs.at[j], vec_send.at[j])
    wait(nr.at[pl.ds(0, DP - 1)], norm_send)


def finish(*refs):
    srcs, dsts, sem = refs[:7], refs[7:14], refs[14]
    copies = [pltpu.make_async_copy(srcs[6].at[zz, yy], dsts[6].at[zz, yy], sem.at[6 + zz * 2 + yy]) for zz in range(4) for yy in range(2)]
    copies += [pltpu.make_async_copy(srcs[i], dsts[i], sem.at[i]) for i in range(6)]
    for copy in copies:
        copy.start()
    for copy in copies:
        copy.wait()


def solution(mesh):
    axis_name = mesh.axis_names[0]
    vm = pl.BlockSpec(memory_space=pltpu.VMEM)
    hbm = pl.BlockSpec(memory_space=pl.ANY)
    dma = pltpu.SemaphoreType.DMA
    K = CHUNKS

    call = pl.pallas_call(
        kernel,
        name="adam_step",
        out_shape=(
            [pltpu.VMEM((PIECE, 128), F32)] * 3
            + [pltpu.VMEM((VEC, 128), F32)] * 3
            + [pltpu.VMEM((4, 2, 2, 2, PIECE, 128), BF16)]
        ),
        in_specs=[hbm, vm, hbm, hbm, hbm, vm, vm, vm, pl.BlockSpec(memory_space=pltpu.SMEM)],
        out_specs=[vm] * 7,
        scratch_shapes=[
            pltpu.VMEM((2, DP, 1, ROWS * 128), BF16),
            pltpu.VMEM((3, 2, 4, 8 * HALF, 128), BF16),
            pltpu.VMEM((K, 2, 2, 4, RAB, 128), F32),
            pltpu.VMEM((K, 4, 2, 2, RCD, 128), F32),
            pltpu.VMEM((K, 4, 2, RAB, 128), F32),
            pltpu.VMEM((K, 2, 4, RAB, 128), F32),
            pltpu.VMEM((K, 5, 2, 2, RCD, 128), F32),
            pltpu.VMEM((K, 5, 2, RAB, 128), F32),
            pltpu.VMEM((K, 2, RCD, 128), F32),
            pltpu.VMEM((PIECE, 128), F32),
            pltpu.VMEM((8, 128), F32),
            pltpu.VMEM((8, 128), F32),
            pltpu.VMEM((6, VPAD, 128), F32),
            pltpu.VMEM((5, VPAD, 128), F32),
            pltpu.VMEM((1, 128), F32),
            pltpu.VMEM((DP, 1, 128), F32),
            dma((2,)), dma((3,)), dma((3,)), dma((K,)), dma((K,)), dma((K,)), dma((K, 5)), dma((K, 5)), dma((K,)),
            dma((5,)), dma((5,)), dma, dma,
            dma((K,)), dma((K, 2, 3)), dma((K, 2, 3)), dma((K,)), dma((K,)), dma((K,)), dma((K,)), dma((K,)),
        ],
        compiler_params=pltpu.CompilerParams(
            collective_id=0, has_side_effects=True, vmem_limit_bytes=37 * 2 ** 20
        ),
    )

    shapes = [(PIECE, 128)] * 3 + [(VEC, 128)] * 3
    copy_out = pl.pallas_call(
        finish,
        name="copy_out",
        out_shape=[jax.ShapeDtypeStruct(s, F32) for s in shapes] + [jax.ShapeDtypeStruct((4, 2, 2, 2, PIECE, 128), BF16)],
        in_specs=[vm] * 7,
        out_specs=[hbm] * 7,
        scratch_shapes=[dma((14,))],
        compiler_params=pltpu.CompilerParams(vmem_limit_bytes=2 ** 20),
    )

    def local_step(g_mat, g_vec, p_mat, m_mat, v_mat, p_vec, m_vec, v_vec, learn_rate):
        outs = call(
            g_mat, g_vec,
            p_mat.reshape(PIECE, 128), m_mat.reshape(PIECE, 128), v_mat.reshape(PIECE, 128),
            p_vec.reshape(VEC, 128), m_vec.reshape(VEC, 128), v_vec.reshape(VEC, 128),
            learn_rate.reshape(1, 1),
        )
        return tuple(o.reshape(-1) for o in copy_out(*outs))

    return jax.shard_map(
        local_step,
        mesh=mesh,
        in_specs=(P(axis_name, None), P(axis_name, None), P(axis_name), P(axis_name), P(axis_name), P(), P(), P(), P()),
        out_specs=(P(axis_name), P(axis_name), P(axis_name), P(), P(), P(), P()),
        check_vma=False,
    )
```

```python
import jax
import jax.numpy as jnp
from jax import lax
from jax.experimental import pallas as pl
from jax.experimental.pallas import tpu as pltpu
from jax.sharding import PartitionSpec as P

STEP = 10
ADAM_BETA1 = 0.9
ADAM_BETA2 = 0.98
ADAM_EPS = 1e-8
WEIGHT_DECAY = 0.01
MAX_NORM = 1.0
NORM_EPS = 1e-6
BIAS_ONE = 1.0 - ADAM_BETA1 ** STEP
BIAS_TWO = 1.0 - ADAM_BETA2 ** STEP

DP = 32
PIECE = 2400
CHUNKS = 25
ROWS = PIECE // CHUNKS
HALF = ROWS // 2
RAB = 16
RCD = HALF - RAB
SKEW_RS = 2
SKEW_AG = 2
VEC = 130
VPAD = 136
MESH = pl.DeviceIdType.MESH
F32 = jnp.float32
BF16 = jnp.bfloat16


def adam_update(grad_vals, param_vals, moment_one, moment_two, learn_rate, decay_rate):
    new_one = ADAM_BETA1 * moment_one + (1.0 - ADAM_BETA1) * grad_vals
    new_two = ADAM_BETA2 * moment_two + (1.0 - ADAM_BETA2) * grad_vals * grad_vals
    direction = (new_one / BIAS_ONE) / (jnp.sqrt(new_two / BIAS_TWO) + ADAM_EPS)
    return param_vals - learn_rate * (direction + decay_rate * param_vals), new_one, new_two


def kernel(g, gv, p, m, v, pv, mv, vv, lr,
           po, mo, vo, pvo, mvo, vvo, pb,
           stage, dense, pab, pcd, abz, er, cdr, abr, fr, gsum, ssq, clip, vs, vr, ns, nr,
           in_sem, pmv_sem, s0_send, s0_recv, rs_send, er_recv, cd_recv, ab_recv, f_recv,
           vec_send, vec_recv, norm_send, norm_recv,
           ag_send, ag_ab, ag_cd, ag_cd1, ag_ab2, ag_ab3, ag_cd3, ag_d2d):
    me = lax.axis_index("dp")
    c = me % 2
    x = (me // 2) % 2
    y = (me // 4) % 2
    z = me // 8

    def dev(zz, yy, xx, cc):
        return ((zz * 2 + yy) * 2 + xx) * 2 + cc

    partner = dev(z, y, x, 1 - c)
    xs = dev(z, y, 1 - x, c)
    xo = dev(z, y, 1 - x, 1 - c)
    ys = dev(z, 1 - y, x, c)
    yo = dev(z, 1 - y, x, 1 - c)
    up = dev((z + 1) % 4, y, x, c)
    down = dev((z + 3) % 4, y, x, c)
    z1 = dev(z + 1 - 2 * (z % 2), y, x, c)
    z2 = dev((z + 2) % 4, y, x, c)
    nlow = z >= 1
    nhigh = z <= 2

    def send(src, dst, ssem, rsem, to):
        pltpu.make_async_remote_copy(
            src_ref=src, dst_ref=dst, send_sem=ssem, recv_sem=rsem, device_id=(to,), device_id_type=MESH
        ).start()

    def wait(ref, sem):
        pltpu.make_async_copy(ref, ref, sem).wait()

    def fetch(k, slot):
        def one(d, carry):
            off = pl.multiple_of((d * PIECE + k * ROWS) * 128, 1024)
            pltpu.make_async_copy(g.at[0:1, pl.ds(off, ROWS * 128)], stage.at[slot, d], in_sem.at[slot]).start()
            return carry
        lax.fori_loop(0, DP, one, 0)

    fetch(0, 0)
    pltpu.make_async_copy(p, po, pmv_sem.at[0]).start()
    pltpu.make_async_copy(m, mo, pmv_sem.at[1]).start()
    pltpu.make_async_copy(v, vo, pmv_sem.at[2]).start()

    barrier = pltpu.get_barrier_semaphore()
    for nb in (partner, xs, xo, ys, yo, z2):
        pl.semaphore_signal(barrier, inc=1, device_id=(nb,), device_id_type=MESH)

    @pl.when(nhigh)
    def _():
        pl.semaphore_signal(barrier, inc=1, device_id=(up,), device_id_type=MESH)

    @pl.when(nlow)
    def _():
        pl.semaphore_signal(barrier, inc=1, device_id=(down,), device_id_type=MESH)

    vs[0, 0:128] = gv[0:1, 0:16384].astype(F32).reshape(128, 128)
    vs[0, 128:VPAD] = jnp.zeros((VPAD - 128, 128), F32)
    vs[0, 128:VEC] = gv[0:1, 16384:16640].astype(F32).reshape(2, 128)
    ssq[...] = jnp.zeros((8, 128), F32)

    mid = (z >= 1) & (z <= 2)

    def await_neighbours():
        @pl.when(mid)
        def _():
            pl.semaphore_wait(barrier, 8)

        @pl.when(jnp.logical_not(mid))
        def _():
            pl.semaphore_wait(barrier, 7)

    partners = (partner, xs, ys, z1, z2)

    def vec_step(j):
        if j > 0:
            wait(vr.at[j - 1], vec_recv.at[j - 1])
            vs[j] = vs[j - 1] + vr[j - 1]
        if j < 5:
            send(vs.at[j], vr.at[j], vec_send.at[j], vec_recv.at[j], partners[j])

    per = PIECE // (24 * HALF)

    def rpiece(k, d):
        at = (2 * k + d) // per
        return at // 8, (at // 4) % 2, (at // 2) % 2, at % 2

    def roff(k, d):
        return ((2 * k + d) % per) * 24 * HALF

    def rbuf(k, d, j):
        return pb.at[(*rpiece(k, d), pl.ds(roff(k, d) + j * 8 * HALF, 8 * HALF))]

    def convert(k):
        slot = k % 2
        dslot = k % 4

        @pl.when(k + 1 < CHUNKS)
        def _():
            fetch(k + 1, 1 - slot)

        @pl.when(k >= 4)
        def _():
            wait(dense.at[dslot, :, pl.ds(1, 3)], s0_send.at[dslot])

        wait(stage.at[slot], in_sem.at[slot])

        def conv(b, carry):
            row = pl.multiple_of(b * HALF, 16)
            for d in range(2):
                for q in range(4):
                    cc = 1 - c if q % 2 else c
                    if d == 0:
                        piece = dev(b // 2, b % 2, 1 - x if q >= 2 else x, cc)
                    else:
                        piece = dev(b // 2, 1 - y if q >= 2 else y, b % 2, cc)
                    vals = stage[slot, piece, 0:1, d * HALF * 128:(d + 1) * HALF * 128].astype(F32)
                    dense[dslot, d, q, pl.ds(row, HALF)] = vals.reshape(HALF, 128).astype(BF16)
            return carry

        lax.fori_loop(0, 8, conv, 0)

    def stage0(k):
        dslot = k % 4
        for q in (3, 2, 1):
            for d in range(2):
                to = ((partner, xs, xo), (partner, ys, yo))[d][q - 1]
                send(dense.at[dslot, d, q], rbuf(k, d, q - 1), s0_send.at[dslot], s0_recv.at[k], to)

        @pl.when(k + 1 < CHUNKS)
        def _():
            convert(k + 1)

    def z_sends(k, t, bufs, recv, rsem):
        @pl.when(z <= t)
        def _():
            dest = 3 + z - t
            if t > 0:
                @pl.when(nlow)
                def _():
                    wait(recv.at[k, t - 1], rsem.at[k, t - 1])
                    bufs[k, dest] += recv[k, t - 1]
            send(bufs.at[k, dest], recv.at[k, t], rs_send.at[k], rsem.at[k, t], up)

        @pl.when(3 - z <= t)
        def _():
            dest = t - (3 - z)
            if t > 0:
                @pl.when(nhigh)
                def _():
                    old = 0 if t == 1 else t + 1
                    wait(recv.at[k, old], rsem.at[k, old])
                    bufs[k, dest] += recv[k, old]
            new = 0 if t == 0 else t + 2
            send(bufs.at[k, dest], recv.at[k, new], rs_send.at[k], rsem.at[k, new], down)

    def z_final(k, bufs, recv, rsem):
        @pl.when(nlow)
        def _():
            wait(recv.at[k, 2], rsem.at[k, 2])
            bufs[k, z] += recv[k, 2]

        @pl.when(nhigh)
        def _():
            wait(recv.at[k, 4], rsem.at[k, 4])
            bufs[k, z] += recv[k, 4]

    def stage1(k):
        dslot = k % 4
        wait(dense.at[dslot, :, pl.ds(1, 3)], s0_recv.at[k])
        for d in range(2):
            def add(b, carry, d=d):
                row = pl.multiple_of(b * HALF, 16)
                tot = dense[dslot, d, 0, pl.ds(row, HALF)].astype(F32)
                for j in range(3):
                    off = pl.multiple_of(roff(k, d) + j * 8 * HALF + b * HALF, 16)
                    tot = tot + pb[(*rpiece(k, d), pl.ds(off, HALF))].astype(F32)
                pab[k, d, b % 2, b // 2] = tot[0:RAB]
                pcd[k, b // 2, d, b % 2] = tot[RAB:HALF]
                return carry
            lax.fori_loop(0, 8, add, 0)
        send(pab.at[k, 0, 1 - y], er.at[k, 0], rs_send.at[k], er_recv.at[k], ys)
        send(pab.at[k, 1, 1 - x], er.at[k, 1], rs_send.at[k], er_recv.at[k], xs)
        z_sends(k, 0, pcd, cdr, cd_recv)

    def stage2(k):
        z_sends(k, 1, pcd, cdr, cd_recv)
        wait(er.at[k], er_recv.at[k])
        for zz in range(4):
            abz[k, zz, 0] = pab[k, 0, y, zz] + er[k, 0, zz]
            abz[k, zz, 1] = pab[k, 1, x, zz] + er[k, 1, zz]
        z_sends(k, 0, abz, abr, ab_recv)

    def stage3(k):
        z_sends(k, 2, pcd, cdr, cd_recv)
        z_sends(k, 1, abz, abr, ab_recv)

    def stage4(k):
        z_final(k, pcd, cdr, cd_recv)
        send(pcd.at[k, z, 0, 1 - y], fr.at[k, 0], rs_send.at[k], f_recv.at[k], ys)
        send(pcd.at[k, z, 1, 1 - x], fr.at[k, 1], rs_send.at[k], f_recv.at[k], xs)
        z_sends(k, 2, abz, abr, ab_recv)

    def stage5(k):
        z_final(k, abz, abr, ab_recv)
        wait(fr.at[k], f_recv.at[k])
        base = pl.multiple_of(k * ROWS, 16)
        parts = (
            (0, RAB, abz[k, z, 0]),
            (RAB, RCD, pcd[k, z, 0, y] + fr[k, 0]),
            (HALF, RAB, abz[k, z, 1]),
            (HALF + RAB, RCD, pcd[k, z, 1, x] + fr[k, 1]),
        )
        acc = ssq[...]
        for off, num, val in parts:
            val = val * (1.0 / DP)
            gsum[pl.ds(base + off, num)] = val
            acc = acc + jnp.sum((val * val).reshape(num // 8, 8, 128), axis=0)
        ssq[...] = acc

    def rs_iter(i, carry):
        for s, fn in enumerate((stage0, stage1, stage2, stage3, stage4, stage5)):
            k = i - SKEW_RS * s

            @pl.when((k >= 0) & (k < CHUNKS))
            def _(fn=fn, k=k):
                fn(k)
        for j in range(6):
            @pl.when(i == 1 + 2 * j)
            def _(j=j):
                vec_step(j)
        return carry

    convert(0)
    await_neighbours()
    lax.fori_loop(0, CHUNKS + 5 * SKEW_RS, rs_iter, 0)

    ns[...] = jnp.sum(ssq[...], axis=0, keepdims=True)
    nr[me] = ns[...]

    def tell(j, carry):
        send(ns, nr.at[me], norm_send, norm_recv, (me + j) % DP)
        return carry

    lax.fori_loop(1, DP, tell, 0)
    wait(nr.at[pl.ds(0, DP - 1)], norm_recv)
    gvec = vs[5, 0:VEC] * (1.0 / DP)
    norm_sq = jnp.full((8, 128), jnp.sum(nr[...]) + jnp.sum(gvec * gvec))
    clip[...] = jnp.minimum(1.0, MAX_NORM / (jnp.sqrt(norm_sq) + NORM_EPS))
    rate = lr[0, 0]

    wait(po, pmv_sem.at[0])
    wait(mo, pmv_sem.at[1])
    wait(vo, pmv_sem.at[2])

    def ag_rows(k, off, num):
        return pl.ds(pl.multiple_of(k * ROWS + off, 16), num)

    full = slice(None)

    def region(zz, yy, xx, rows):
        return pb.at[zz, yy, xx, c, rows]

    def push(ref, k, rsem, to):
        send(ref, ref, ag_send.at[k], rsem, to)

    def ag0(k):
        def upd(b, carry):
            rows = pl.ds(pl.multiple_of(k * ROWS + b * 32, 16), 32)
            new = adam_update(gsum[rows] * clip[0:1], po[rows], mo[rows], vo[rows], rate, WEIGHT_DECAY)
            po[rows], mo[rows], vo[rows] = new
            pb[z, y, x, c, rows] = new[0].astype(BF16)
            return carry
        lax.fori_loop(0, ROWS // 32, upd, 0)
        ab = ag_rows(k, 0, 2 * RAB)

        @pl.when(nhigh)
        def _():
            push(region(z, y, x, ab), k, ag_ab.at[k, 0, 0], up)

        @pl.when(nlow)
        def _():
            push(region(z, y, x, ab), k, ag_ab.at[k, 1, 0], down)

        push(region(z, y, x, ag_rows(k, 2 * RAB, RCD)), k, ag_cd1.at[k], ys)
        push(region(z, y, x, ag_rows(k, 2 * RAB + RCD, RCD)), k, ag_cd1.at[k], xs)

    def z_ab(k, t):
        ab = ag_rows(k, 0, 2 * RAB)
        one = region(0, 0, 0, ab)

        @pl.when(z - 1 - t >= 0)
        def _():
            wait(one, ag_ab.at[k, 0, t])
            if t < 2:
                @pl.when(nhigh)
                def _():
                    push(region(z - 1 - t, y, x, ab), k, ag_ab.at[k, 0, t + 1], up)

        @pl.when(z + 1 + t <= 3)
        def _():
            wait(one, ag_ab.at[k, 1, t])
            if t < 2:
                @pl.when(nlow)
                def _():
                    push(region(z + 1 + t, y, x, ab), k, ag_ab.at[k, 1, t + 1], down)

    def cd_push(k, zz, d, t, to):
        push(region(zz, full, x, ag_rows(k, 2 * RAB, RCD)), k, ag_cd.at[k, d, t], to)
        push(region(zz, y, full, ag_rows(k, 2 * RAB + RCD, RCD)), k, ag_cd.at[k, d, t], to)

    def z_cd(k, t):
        both = pb.at[0, 0, full, full, ag_rows(k, 2 * RAB, RCD)]

        @pl.when(z - 1 - t >= 0)
        def _():
            wait(both, ag_cd.at[k, 0, t])
            if t < 2:
                @pl.when(nhigh)
                def _():
                    cd_push(k, z - 1 - t, 0, t + 1, up)

        @pl.when(z + 1 + t <= 3)
        def _():
            wait(both, ag_cd.at[k, 1, t])
            if t < 2:
                @pl.when(nlow)
                def _():
                    cd_push(k, z + 1 + t, 1, t + 1, down)

    def ag1(k):
        wait(pb.at[0, 0, 0, full, ag_rows(k, 2 * RAB, RCD)], ag_cd1.at[k])

        @pl.when(nhigh)
        def _():
            cd_push(k, z, 0, 0, up)

        @pl.when(nlow)
        def _():
            cd_push(k, z, 1, 0, down)

        z_ab(k, 0)

    def ag2(k):
        z_ab(k, 1)
        z_cd(k, 0)

    def ag3(k):
        z_ab(k, 2)
        ra = ag_rows(k, 0, RAB)
        rb = ag_rows(k, RAB, RAB)
        push(region(full, y, x, ra), k, ag_ab2.at[k], ys)
        push(region(full, y, x, rb), k, ag_ab2.at[k], xs)
        push(region(full, y, x, ag_rows(k, 0, 2 * RAB)), k, ag_d2d.at[k], partner)
        z_cd(k, 1)

    def ag4(k):
        ra = ag_rows(k, 0, RAB)
        rb = ag_rows(k, RAB, RAB)
        rc = ag_rows(k, 2 * RAB, RCD)
        rd = ag_rows(k, 2 * RAB + RCD, RCD)
        wait(pb.at[0, 0, full, full, ag_rows(k, 0, 2 * RAB)], ag_ab2.at[k])
        push(region(full, full, x, ra), k, ag_ab3.at[k], xs)
        push(region(full, y, full, rb), k, ag_ab3.at[k], ys)
        push(region(full, 1 - y, x, ra), k, ag_d2d.at[k], partner)
        push(region(full, y, 1 - x, rb), k, ag_d2d.at[k], partner)
        z_cd(k, 2)
        push(region(full, full, x, rc), k, ag_cd3.at[k], xs)
        push(region(full, y, full, rd), k, ag_cd3.at[k], ys)
        push(region(full, full, x, rc), k, ag_d2d.at[k], partner)
        push(region(full, y, full, rd), k, ag_d2d.at[k], partner)

    def ag5(k):
        wait(pb.at[0, full, full, full, ag_rows(k, 0, 2 * RAB)], ag_ab3.at[k])
        push(region(full, full, 1 - x, ag_rows(k, 0, RAB)), k, ag_d2d.at[k], partner)
        push(region(full, 1 - y, full, ag_rows(k, RAB, RAB)), k, ag_d2d.at[k], partner)
        wait(pb.at[full, full, full, 0, ag_rows(k, 2 * RAB, RCD)], ag_cd3.at[k])
        push(region(full, full, 1 - x, ag_rows(k, 2 * RAB, RCD)), k, ag_d2d.at[k], partner)
        push(region(full, 1 - y, full, ag_rows(k, 2 * RAB + RCD, RCD)), k, ag_d2d.at[k], partner)

    def ag_iter(i, carry):
        for s, fn in enumerate((ag0, ag1, ag2, ag3, ag4, ag5)):
            k = i - SKEW_AG * s

            @pl.when((k >= 0) & (k < CHUNKS))
            def _(fn=fn, k=k):
                fn(k)
        return carry

    lax.fori_loop(0, CHUNKS + 5 * SKEW_AG, ag_iter, 0)

    newv = adam_update(gvec * clip[0:1], pv[...], mv[...], vv[...], rate, 0.0)
    pvo[...], mvo[...], vvo[...] = newv

    def drain(k, carry):
        wait(pb.at[full, full, full, 0, ag_rows(k, 0, ROWS)], ag_d2d.at[k])
        base, along = 24 * RAB + 18 * RCD + 16 * ROWS, 2 * RAB + 4 * RCD

        @pl.when(mid)
        def _():
            wait(pb.at[0, 0, full, full, pl.ds(0, (base + 5 * along) // 4)], ag_send.at[k])

        @pl.when(jnp.logical_not(mid))
        def _():
            wait(pb.at[0, 0, 0, full, pl.ds(0, (base + along) // 2)], ag_send.at[k])

        wait(gsum.at[pl.ds(0, 14 * HALF)], rs_send.at[k])
        return carry

    lax.fori_loop(0, CHUNKS, drain, 0)
    for s in range(4):
        wait(dense.at[s, :, pl.ds(1, 3)], s0_send.at[s])
    for j in range(5):
        wait(vs.at[j], vec_send.at[j])
    wait(nr.at[pl.ds(0, DP - 1)], norm_send)


def finish(*refs):
    srcs, dsts, sem = refs[:7], refs[7:14], refs[14]
    copies = [pltpu.make_async_copy(srcs[6].at[zz, yy], dsts[6].at[zz, yy], sem.at[6 + zz * 2 + yy]) for zz in range(4) for yy in range(2)]
    copies += [pltpu.make_async_copy(srcs[i], dsts[i], sem.at[i]) for i in range(6)]
    for copy in copies:
        copy.start()
    for copy in copies:
        copy.wait()


def solution(mesh):
    axis_name = mesh.axis_names[0]
    vm = pl.BlockSpec(memory_space=pltpu.VMEM)
    hbm = pl.BlockSpec(memory_space=pl.ANY)
    dma = pltpu.SemaphoreType.DMA
    K = CHUNKS

    call = pl.pallas_call(
        kernel,
        name="adam_step",
        out_shape=(
            [pltpu.VMEM((PIECE, 128), F32)] * 3
            + [pltpu.VMEM((VEC, 128), F32)] * 3
            + [pltpu.VMEM((4, 2, 2, 2, PIECE, 128), BF16)]
        ),
        in_specs=[hbm, vm, hbm, hbm, hbm, vm, vm, vm, pl.BlockSpec(memory_space=pltpu.SMEM)],
        out_specs=[vm] * 7,
        scratch_shapes=[
            pltpu.VMEM((2, DP, 1, ROWS * 128), BF16),
            pltpu.VMEM((4, 2, 4, 8 * HALF, 128), BF16),
            pltpu.VMEM((K, 2, 2, 4, RAB, 128), F32),
            pltpu.VMEM((K, 4, 2, 2, RCD, 128), F32),
            pltpu.VMEM((K, 4, 2, RAB, 128), F32),
            pltpu.VMEM((K, 2, 4, RAB, 128), F32),
            pltpu.VMEM((K, 5, 2, 2, RCD, 128), F32),
            pltpu.VMEM((K, 5, 2, RAB, 128), F32),
            pltpu.VMEM((K, 2, RCD, 128), F32),
            pltpu.VMEM((PIECE, 128), F32),
            pltpu.VMEM((8, 128), F32),
            pltpu.VMEM((8, 128), F32),
            pltpu.VMEM((6, VPAD, 128), F32),
            pltpu.VMEM((5, VPAD, 128), F32),
            pltpu.VMEM((1, 128), F32),
            pltpu.VMEM((DP, 1, 128), F32),
            dma((2,)), dma((3,)), dma((4,)), dma((K,)), dma((K,)), dma((K,)), dma((K, 5)), dma((K, 5)), dma((K,)),
            dma((5,)), dma((5,)), dma, dma,
            dma((K,)), dma((K, 2, 3)), dma((K, 2, 3)), dma((K,)), dma((K,)), dma((K,)), dma((K,)), dma((K,)),
        ],
        compiler_params=pltpu.CompilerParams(
            collective_id=0, has_side_effects=True, vmem_limit_bytes=37 * 2 ** 20
        ),
    )

    shapes = [(PIECE, 128)] * 3 + [(VEC, 128)] * 3
    copy_out = pl.pallas_call(
        finish,
        name="copy_out",
        out_shape=[jax.ShapeDtypeStruct(s, F32) for s in shapes] + [jax.ShapeDtypeStruct((4, 2, 2, 2, PIECE, 128), BF16)],
        in_specs=[vm] * 7,
        out_specs=[hbm] * 7,
        scratch_shapes=[dma((14,))],
        compiler_params=pltpu.CompilerParams(vmem_limit_bytes=2 ** 20),
    )

    def local_step(g_mat, g_vec, p_mat, m_mat, v_mat, p_vec, m_vec, v_vec, learn_rate):
        outs = call(
            g_mat, g_vec,
            p_mat.reshape(PIECE, 128), m_mat.reshape(PIECE, 128), v_mat.reshape(PIECE, 128),
            p_vec.reshape(VEC, 128), m_vec.reshape(VEC, 128), v_vec.reshape(VEC, 128),
            learn_rate.reshape(1, 1),
        )
        return tuple(o.reshape(-1) for o in copy_out(*outs))

    return jax.shard_map(
        local_step,
        mesh=mesh,
        in_specs=(P(axis_name, None), P(axis_name, None), P(axis_name), P(axis_name), P(axis_name), P(), P(), P(), P()),
        out_specs=(P(axis_name), P(axis_name), P(axis_name), P(), P(), P(), P()),
        check_vma=False,
    )
```

```python
import jax
import jax.numpy as jnp
from jax import lax
from jax.experimental import pallas as pl
from jax.experimental.pallas import tpu as pltpu
from jax.sharding import PartitionSpec as P

STEP = 10
ADAM_BETA1 = 0.9
ADAM_BETA2 = 0.98
ADAM_EPS = 1e-8
WEIGHT_DECAY = 0.01
MAX_NORM = 1.0
NORM_EPS = 1e-6
BIAS_ONE = 1.0 - ADAM_BETA1 ** STEP
BIAS_TWO = 1.0 - ADAM_BETA2 ** STEP

DP = 32
AG_CHUNKS = 15
AG_ROWS = 160
AG_AB = 32
AG_CD = 48
PIECE = 2400
CHUNKS = 25
ROWS = PIECE // CHUNKS
HALF = ROWS // 2
RAB = 16
RCD = HALF - RAB
SKEW_RS = 2
SKEW_AG = 1
VEC = 130
VPAD = 136
MESH = pl.DeviceIdType.MESH
F32 = jnp.float32
BF16 = jnp.bfloat16


def adam_update(grad_vals, param_vals, moment_one, moment_two, learn_rate, decay_rate):
    new_one = ADAM_BETA1 * moment_one + (1.0 - ADAM_BETA1) * grad_vals
    new_two = ADAM_BETA2 * moment_two + (1.0 - ADAM_BETA2) * grad_vals * grad_vals
    direction = (new_one / BIAS_ONE) / (jnp.sqrt(new_two / BIAS_TWO) + ADAM_EPS)
    return param_vals - learn_rate * (direction + decay_rate * param_vals), new_one, new_two


def kernel(g, gv, p, m, v, pv, mv, vv, lr,
           po, mo, vo, pvo, mvo, vvo, pb,
           stage, dense, pab, pcd, abz, er, cdr, abr, fr, gsum, ssq, clip, vs, vr, ns, nr,
           in_sem, pmv_sem, s0_send, s0_recv, rs_send, er_recv, cd_recv, ab_recv, f_recv,
           vec_send, vec_recv, norm_send, norm_recv,
           ag_send, ag_ab, ag_cd, ag_cd1, ag_h2, ag_h3, ag_d2d):
    me = lax.axis_index("dp")
    c = me % 2
    x = (me // 2) % 2
    y = (me // 4) % 2
    z = me // 8

    def dev(zz, yy, xx, cc):
        return ((zz * 2 + yy) * 2 + xx) * 2 + cc

    partner = dev(z, y, x, 1 - c)
    xs = dev(z, y, 1 - x, c)
    xo = dev(z, y, 1 - x, 1 - c)
    ys = dev(z, 1 - y, x, c)
    yo = dev(z, 1 - y, x, 1 - c)
    up = dev((z + 1) % 4, y, x, c)
    down = dev((z + 3) % 4, y, x, c)
    z1 = dev(z + 1 - 2 * (z % 2), y, x, c)
    z2 = dev((z + 2) % 4, y, x, c)
    nlow = z >= 1
    nhigh = z <= 2

    def send(src, dst, ssem, rsem, to):
        pltpu.make_async_remote_copy(
            src_ref=src, dst_ref=dst, send_sem=ssem, recv_sem=rsem, device_id=(to,), device_id_type=MESH
        ).start()

    def wait(ref, sem):
        pltpu.make_async_copy(ref, ref, sem).wait()

    def fetch(k, slot):
        def one(d, carry):
            off = pl.multiple_of((d * PIECE + k * ROWS) * 128, 1024)
            pltpu.make_async_copy(g.at[0:1, pl.ds(off, ROWS * 128)], stage.at[slot, d], in_sem.at[slot]).start()
            return carry
        lax.fori_loop(0, DP, one, 0)

    fetch(0, 0)
    pltpu.make_async_copy(p, po, pmv_sem.at[0]).start()
    pltpu.make_async_copy(m, mo, pmv_sem.at[1]).start()
    pltpu.make_async_copy(v, vo, pmv_sem.at[2]).start()

    barrier = pltpu.get_barrier_semaphore()
    for nb in (partner, xs, xo, ys, yo, z2):
        pl.semaphore_signal(barrier, inc=1, device_id=(nb,), device_id_type=MESH)

    @pl.when(nhigh)
    def _():
        pl.semaphore_signal(barrier, inc=1, device_id=(up,), device_id_type=MESH)

    @pl.when(nlow)
    def _():
        pl.semaphore_signal(barrier, inc=1, device_id=(down,), device_id_type=MESH)

    vs[0, 0:128] = gv[0:1, 0:16384].astype(F32).reshape(128, 128)
    vs[0, 128:VPAD] = jnp.zeros((VPAD - 128, 128), F32)
    vs[0, 128:VEC] = gv[0:1, 16384:16640].astype(F32).reshape(2, 128)
    ssq[...] = jnp.zeros((8, 128), F32)

    mid = (z >= 1) & (z <= 2)

    def await_neighbours():
        @pl.when(mid)
        def _():
            pl.semaphore_wait(barrier, 8)

        @pl.when(jnp.logical_not(mid))
        def _():
            pl.semaphore_wait(barrier, 7)

    partners = (partner, xs, ys, z1, z2)

    def vec_step(j):
        if j > 0:
            wait(vr.at[j - 1], vec_recv.at[j - 1])
            vs[j] = vs[j - 1] + vr[j - 1]
        if j < 5:
            send(vs.at[j], vr.at[j], vec_send.at[j], vec_recv.at[j], partners[j])

    per = PIECE // (24 * HALF)

    def rpiece(k, d):
        at = (2 * k + d) // per
        return at // 8, (at // 4) % 2, (at // 2) % 2, at % 2

    def roff(k, d):
        return ((2 * k + d) % per) * 24 * HALF

    def rbuf(k, d, j):
        return pb.at[(*rpiece(k, d), pl.ds(roff(k, d) + j * 8 * HALF, 8 * HALF))]

    def convert(k):
        slot = k % 2
        dslot = k % 4

        @pl.when(k + 1 < CHUNKS)
        def _():
            fetch(k + 1, 1 - slot)

        @pl.when(k >= 4)
        def _():
            wait(dense.at[dslot, :, pl.ds(1, 3)], s0_send.at[dslot])

        wait(stage.at[slot], in_sem.at[slot])

        def conv(b, carry):
            row = pl.multiple_of(b * HALF, 16)
            for d in range(2):
                for q in range(4):
                    cc = 1 - c if q % 2 else c
                    if d == 0:
                        piece = dev(b // 2, b % 2, 1 - x if q >= 2 else x, cc)
                    else:
                        piece = dev(b // 2, 1 - y if q >= 2 else y, b % 2, cc)
                    vals = stage[slot, piece, 0:1, d * HALF * 128:(d + 1) * HALF * 128].astype(F32)
                    dense[dslot, d, q, pl.ds(row, HALF)] = vals.reshape(HALF, 128).astype(BF16)
            return carry

        lax.fori_loop(0, 8, conv, 0)

    def stage0(k):
        dslot = k % 4
        for q in (3, 2, 1):
            for d in range(2):
                to = ((partner, xs, xo), (partner, ys, yo))[d][q - 1]
                send(dense.at[dslot, d, q], rbuf(k, d, q - 1), s0_send.at[dslot], s0_recv.at[k], to)

        @pl.when(k + 1 < CHUNKS)
        def _():
            convert(k + 1)

    def z_first(k, bufs, recv, rsem):
        @pl.when(z == 0)
        def _():
            send(bufs.at[k, pl.ds(1, 3)], recv.at[k, pl.ds(0, 3)], rs_send.at[k], rsem.at[k, 0], up)

        @pl.when(z == 3)
        def _():
            send(bufs.at[k, pl.ds(0, 3)], recv.at[k, pl.ds(0, 3)], rs_send.at[k], rsem.at[k, 0], down)

    def z_second(k, bufs, recv, rsem):
        @pl.when(z == 1)
        def _():
            wait(recv.at[k, pl.ds(0, 3)], rsem.at[k, 0])
            bufs[k, 1:4] += recv[k, 0:3]
            send(bufs.at[k, pl.ds(2, 2)], recv.at[k, pl.ds(3, 2)], rs_send.at[k], rsem.at[k, 1], up)

        @pl.when(z == 2)
        def _():
            wait(recv.at[k, pl.ds(0, 3)], rsem.at[k, 0])
            bufs[k, 0:3] += recv[k, 0:3]
            send(bufs.at[k, pl.ds(0, 2)], recv.at[k, pl.ds(3, 2)], rs_send.at[k], rsem.at[k, 1], down)

    def z_third(k, bufs, recv, rsem):
        @pl.when(z == 1)
        def _():
            wait(recv.at[k, pl.ds(3, 2)], rsem.at[k, 1])
            bufs[k, 0:2] += recv[k, 3:5]
            send(bufs.at[k, 0], recv.at[k, 0], rs_send.at[k], rsem.at[k, 0], down)

        @pl.when(z == 2)
        def _():
            wait(recv.at[k, pl.ds(3, 2)], rsem.at[k, 1])
            bufs[k, 2:4] += recv[k, 3:5]
            send(bufs.at[k, 3], recv.at[k, 0], rs_send.at[k], rsem.at[k, 0], up)

    def z_final(k, bufs, recv, rsem):
        @pl.when(jnp.logical_not(mid))
        def _():
            wait(recv.at[k, 0], rsem.at[k, 0])
            bufs[k, z] += recv[k, 0]

    def stage1(k):
        dslot = k % 4
        wait(dense.at[dslot, :, pl.ds(1, 3)], s0_recv.at[k])
        for d in range(2):
            def add(b, carry, d=d):
                row = pl.multiple_of(b * HALF, 16)
                tot = dense[dslot, d, 0, pl.ds(row, HALF)].astype(F32)
                for j in range(3):
                    off = pl.multiple_of(roff(k, d) + j * 8 * HALF + b * HALF, 16)
                    tot = tot + pb[(*rpiece(k, d), pl.ds(off, HALF))].astype(F32)
                pab[k, d, b % 2, b // 2] = tot[0:RAB]
                pcd[k, b // 2, d, b % 2] = tot[RAB:HALF]
                return carry
            lax.fori_loop(0, 8, add, 0)
        send(pab.at[k, 0, 1 - y], er.at[k, 0], rs_send.at[k], er_recv.at[k], ys)
        send(pab.at[k, 1, 1 - x], er.at[k, 1], rs_send.at[k], er_recv.at[k], xs)
        z_first(k, pcd, cdr, cd_recv)

    def stage2(k):
        z_second(k, pcd, cdr, cd_recv)
        wait(er.at[k], er_recv.at[k])
        for zz in range(4):
            abz[k, zz, 0] = pab[k, 0, y, zz] + er[k, 0, zz]
            abz[k, zz, 1] = pab[k, 1, x, zz] + er[k, 1, zz]
        z_first(k, abz, abr, ab_recv)

    def stage3(k):
        z_third(k, pcd, cdr, cd_recv)
        z_second(k, abz, abr, ab_recv)

    def stage4(k):
        z_final(k, pcd, cdr, cd_recv)
        send(pcd.at[k, z, 0, 1 - y], fr.at[k, 0], rs_send.at[k], f_recv.at[k], ys)
        send(pcd.at[k, z, 1, 1 - x], fr.at[k, 1], rs_send.at[k], f_recv.at[k], xs)
        z_third(k, abz, abr, ab_recv)

    def stage5(k):
        z_final(k, abz, abr, ab_recv)
        wait(fr.at[k], f_recv.at[k])
        base = pl.multiple_of(k * ROWS, 16)
        parts = (
            (0, RAB, abz[k, z, 0]),
            (RAB, RCD, pcd[k, z, 0, y] + fr[k, 0]),
            (HALF, RAB, abz[k, z, 1]),
            (HALF + RAB, RCD, pcd[k, z, 1, x] + fr[k, 1]),
        )
        acc = ssq[...]
        for off, num, val in parts:
            val = val * (1.0 / DP)
            gsum[pl.ds(base + off, num)] = val
            acc = acc + jnp.sum((val * val).reshape(num // 8, 8, 128), axis=0)
        ssq[...] = acc

    def rs_iter(i, carry):
        for s, fn in enumerate((stage0, stage1, stage2, stage3, stage4, stage5)):
            k = i - SKEW_RS * s

            @pl.when((k >= 0) & (k < CHUNKS))
            def _(fn=fn, k=k):
                fn(k)
        for j in range(6):
            @pl.when(i == 1 + 2 * j)
            def _(j=j):
                vec_step(j)
        return carry

    convert(0)
    await_neighbours()
    lax.fori_loop(0, CHUNKS + 5 * SKEW_RS, rs_iter, 0)

    ns[...] = jnp.sum(ssq[...], axis=0, keepdims=True)
    nr[me] = ns[...]

    def tell(j, carry):
        send(ns, nr.at[me], norm_send, norm_recv, (me + j) % DP)
        return carry

    lax.fori_loop(1, DP, tell, 0)
    wait(nr.at[pl.ds(0, DP - 1)], norm_recv)
    gvec = vs[5, 0:VEC] * (1.0 / DP)
    norm_sq = jnp.full((8, 128), jnp.sum(nr[...]) + jnp.sum(gvec * gvec))
    clip[...] = jnp.minimum(1.0, MAX_NORM / (jnp.sqrt(norm_sq) + NORM_EPS))
    rate = lr[0, 0]

    wait(po, pmv_sem.at[0])
    wait(mo, pmv_sem.at[1])
    wait(vo, pmv_sem.at[2])

    def cut(k, off, num):
        return pl.ds(pl.multiple_of(k * AG_ROWS + off, 16), num)

    def rows_of(k):
        return (cut(k, 0, AG_AB), cut(k, AG_AB, AG_AB), cut(k, 2 * AG_AB, AG_CD), cut(k, 2 * AG_AB + AG_CD, AG_CD))

    full = slice(None)

    def region(zz, yy, xx, rows):
        return pb.at[zz, yy, xx, c, rows]

    def push(ref, k, rsem, to):
        send(ref, ref, ag_send.at[k], rsem, to)

    def sides(dist, fn):
        if dist == 0:
            fn(z, None)
            return

        @pl.when(z - dist >= 0)
        def _():
            fn(z - dist, 0)

        @pl.when(z + dist <= 3)
        def _():
            fn(z + dist, 1)

    def along_z(fn):
        @pl.when(nhigh)
        def _():
            fn(0, up)

        @pl.when(nlow)
        def _():
            fn(1, down)

    def onward_z(side, dist, fn):
        if dist == 0:
            along_z(fn)
        elif dist < 3 and side == 0:
            @pl.when(nhigh)
            def _():
                fn(0, up)
        elif dist < 3:
            @pl.when(nlow)
            def _():
                fn(1, down)

    def ab_arrived(k, dist):
        ra, rb = rows_of(k)[:2]
        ab = cut(k, 0, 2 * AG_AB)

        def fn(zz, side):
            if dist:
                wait(region(0, 0, 0, ab), ag_ab.at[k, side, dist - 1])
            onward_z(side, dist, lambda way, to: push(region(zz, y, x, ab), k, ag_ab.at[k, way, dist], to))
            push(region(zz, y, x, ra), k, ag_h2.at[k, zz], ys)
            push(region(zz, y, x, rb), k, ag_h2.at[k, zz], xs)

        sides(dist, fn)

    def ab_second(k, dist):
        ra, rb = rows_of(k)[:2]

        def fn(zz, side):
            wait(region(0, 0, 0, cut(k, 0, 2 * AG_AB)), ag_h2.at[k, zz])
            push(region(zz, full, x, ra), k, ag_h3.at[k], xs)
            push(region(zz, y, full, rb), k, ag_h3.at[k], ys)

        sides(dist, fn)

    def cd_arrived(k, dist):
        rc, rd = rows_of(k)[2:]

        def fn(zz, side):
            if dist == 0:
                wait(region(0, 0, 0, cut(k, 0, 2 * AG_CD)), ag_cd1.at[k])
            else:
                wait(pb.at[0, 0, full, full, rc], ag_cd.at[k, side, dist - 1])

            def on(way, to):
                push(region(zz, full, x, rc), k, ag_cd.at[k, way, dist], to)
                push(region(zz, y, full, rd), k, ag_cd.at[k, way, dist], to)

            onward_z(side, dist, on)
            push(region(zz, full, x, rc), k, ag_h3.at[k], xs)
            push(region(zz, y, full, rd), k, ag_h3.at[k], ys)

        sides(dist, fn)

    def ag0(k):
        def upd(b, carry):
            rows = pl.ds(pl.multiple_of(k * AG_ROWS + b * 32, 16), 32)
            new = adam_update(gsum[rows] * clip[0:1], po[rows], mo[rows], vo[rows], rate, WEIGHT_DECAY)
            po[rows], mo[rows], vo[rows] = new
            pb[z, y, x, c, rows] = new[0].astype(BF16)
            return carry
        lax.fori_loop(0, AG_ROWS // 32, upd, 0)
        rc, rd = rows_of(k)[2:]
        push(region(z, y, x, rc), k, ag_cd1.at[k], ys)
        push(region(z, y, x, rd), k, ag_cd1.at[k], xs)
        ab_arrived(k, 0)

    def middle(s):
        def fn(k):
            cd_arrived(k, s - 1)
            if s <= 3:
                ab_arrived(k, s)
            ab_second(k, s - 1)
        return fn

    def ag5(k):
        wait(pb.at[0, full, full, full, cut(k, 0, AG_ROWS)], ag_h3.at[k])
        push(region(full, full, full, cut(k, 0, AG_ROWS)), k, ag_d2d.at[k], partner)

    def ag_iter(i, carry):
        for s, fn in enumerate((ag0, middle(1), middle(2), middle(3), middle(4), ag5)):
            k = i - SKEW_AG * s

            @pl.when((k >= 0) & (k < AG_CHUNKS))
            def _(fn=fn, k=k):
                fn(k)
        return carry

    lax.fori_loop(0, AG_CHUNKS + 5 * SKEW_AG, ag_iter, 0)

    newv = adam_update(gvec * clip[0:1], pv[...], mv[...], vv[...], rate, 0.0)
    pvo[...], mvo[...], vvo[...] = newv

    def drain_rs(k, carry):
        wait(gsum.at[pl.ds(0, 14 * HALF)], rs_send.at[k])
        return carry

    def drain_ag(k, carry):
        wait(pb.at[full, full, full, 0, cut(k, 0, AG_ROWS)], ag_d2d.at[k])
        base, along = 24 * AG_AB + 18 * AG_CD + 16 * AG_ROWS, 2 * AG_AB + 4 * AG_CD

        @pl.when(mid)
        def _():
            wait(pb.at[0, 0, full, full, pl.ds(0, (base + 5 * along) // 4)], ag_send.at[k])

        @pl.when(jnp.logical_not(mid))
        def _():
            wait(pb.at[0, 0, 0, full, pl.ds(0, (base + along) // 2)], ag_send.at[k])

        return carry

    lax.fori_loop(0, CHUNKS, drain_rs, 0)
    lax.fori_loop(0, AG_CHUNKS, drain_ag, 0)
    for s in range(4):
        wait(dense.at[s, :, pl.ds(1, 3)], s0_send.at[s])
    for j in range(5):
        wait(vs.at[j], vec_send.at[j])
    wait(nr.at[pl.ds(0, DP - 1)], norm_send)


def finish(*refs):
    srcs, dsts, sem = refs[:7], refs[7:14], refs[14]
    copies = [pltpu.make_async_copy(srcs[6].at[zz, yy], dsts[6].at[zz, yy], sem.at[6 + zz * 2 + yy]) for zz in range(4) for yy in range(2)]
    copies += [pltpu.make_async_copy(srcs[i], dsts[i], sem.at[i]) for i in range(6)]
    for copy in copies:
        copy.start()
    for copy in copies:
        copy.wait()


def solution(mesh):
    axis_name = mesh.axis_names[0]
    vm = pl.BlockSpec(memory_space=pltpu.VMEM)
    hbm = pl.BlockSpec(memory_space=pl.ANY)
    dma = pltpu.SemaphoreType.DMA
    K, G = CHUNKS, AG_CHUNKS

    call = pl.pallas_call(
        kernel,
        name="adam_step",
        out_shape=(
            [pltpu.VMEM((PIECE, 128), F32)] * 3
            + [pltpu.VMEM((VEC, 128), F32)] * 3
            + [pltpu.VMEM((4, 2, 2, 2, PIECE, 128), BF16)]
        ),
        in_specs=[hbm, vm, hbm, hbm, hbm, vm, vm, vm, pl.BlockSpec(memory_space=pltpu.SMEM)],
        out_specs=[vm] * 7,
        scratch_shapes=[
            pltpu.VMEM((2, DP, 1, ROWS * 128), BF16),
            pltpu.VMEM((4, 2, 4, 8 * HALF, 128), BF16),
            pltpu.VMEM((K, 2, 2, 4, RAB, 128), F32),
            pltpu.VMEM((K, 4, 2, 2, RCD, 128), F32),
            pltpu.VMEM((K, 4, 2, RAB, 128), F32),
            pltpu.VMEM((K, 2, 4, RAB, 128), F32),
            pltpu.VMEM((K, 5, 2, 2, RCD, 128), F32),
            pltpu.VMEM((K, 5, 2, RAB, 128), F32),
            pltpu.VMEM((K, 2, RCD, 128), F32),
            pltpu.VMEM((PIECE, 128), F32),
            pltpu.VMEM((8, 128), F32),
            pltpu.VMEM((8, 128), F32),
            pltpu.VMEM((6, VPAD, 128), F32),
            pltpu.VMEM((5, VPAD, 128), F32),
            pltpu.VMEM((1, 128), F32),
            pltpu.VMEM((DP, 1, 128), F32),
            dma((2,)), dma((3,)), dma((4,)), dma((K,)), dma((K,)), dma((K,)), dma((K, 2)), dma((K, 2)), dma((K,)),
            dma((5,)), dma((5,)), dma, dma,
            dma((G,)), dma((G, 2, 3)), dma((G, 2, 3)), dma((G,)), dma((G, 4)), dma((G,)), dma((G,)),
        ],
        compiler_params=pltpu.CompilerParams(
            collective_id=0, has_side_effects=True, vmem_limit_bytes=37 * 2 ** 20
        ),
    )

    shapes = [(PIECE, 128)] * 3 + [(VEC, 128)] * 3
    copy_out = pl.pallas_call(
        finish,
        name="copy_out",
        out_shape=[jax.ShapeDtypeStruct(s, F32) for s in shapes] + [jax.ShapeDtypeStruct((4, 2, 2, 2, PIECE, 128), BF16)],
        in_specs=[vm] * 7,
        out_specs=[hbm] * 7,
        scratch_shapes=[dma((14,))],
        compiler_params=pltpu.CompilerParams(vmem_limit_bytes=2 ** 20),
    )

    def local_step(g_mat, g_vec, p_mat, m_mat, v_mat, p_vec, m_vec, v_vec, learn_rate):
        outs = call(
            g_mat, g_vec,
            p_mat.reshape(PIECE, 128), m_mat.reshape(PIECE, 128), v_mat.reshape(PIECE, 128),
            p_vec.reshape(VEC, 128), m_vec.reshape(VEC, 128), v_vec.reshape(VEC, 128),
            learn_rate.reshape(1, 1),
        )
        return tuple(o.reshape(-1) for o in copy_out(*outs))

    return jax.shard_map(
        local_step,
        mesh=mesh,
        in_specs=(P(axis_name, None), P(axis_name, None), P(axis_name), P(axis_name), P(axis_name), P(), P(), P(), P()),
        out_specs=(P(axis_name), P(axis_name), P(axis_name), P(), P(), P(), P()),
        check_vma=False,
    )
```

```python
import jax
import jax.numpy as jnp
from jax import lax
from jax.experimental import pallas as pl
from jax.experimental.pallas import tpu as pltpu
from jax.sharding import PartitionSpec as P

STEP = 10
ADAM_BETA1 = 0.9
ADAM_BETA2 = 0.98
ADAM_EPS = 1e-8
WEIGHT_DECAY = 0.01
MAX_NORM = 1.0
NORM_EPS = 1e-6
BIAS_ONE = 1.0 - ADAM_BETA1 ** STEP
BIAS_TWO = 1.0 - ADAM_BETA2 ** STEP

DP = 32
AG_CHUNKS = 15
AG_ROWS = 160
AG_AB = 16
AG_CD = 64
PIECE = 2400
CHUNKS = 25
ROWS = PIECE // CHUNKS
HALF = ROWS // 2
RAB = 16
RCD = HALF - RAB
SKEW_RS = 2
SKEW_AG = 1
VEC = 130
VPAD = 136
MESH = pl.DeviceIdType.MESH
F32 = jnp.float32
BF16 = jnp.bfloat16


def adam_update(grad_vals, param_vals, moment_one, moment_two, learn_rate, decay_rate):
    new_one = ADAM_BETA1 * moment_one + (1.0 - ADAM_BETA1) * grad_vals
    new_two = ADAM_BETA2 * moment_two + (1.0 - ADAM_BETA2) * grad_vals * grad_vals
    direction = (new_one / BIAS_ONE) / (jnp.sqrt(new_two / BIAS_TWO) + ADAM_EPS)
    return param_vals - learn_rate * (direction + decay_rate * param_vals), new_one, new_two


def kernel(g, gv, p, m, v, pv, mv, vv, lr,
           po, mo, vo, pvo, mvo, vvo, pb,
           stage, dense, pab, pcd, abz, er, cdr, abr, fr, gsum, ssq, clip, vs, vr, ns, nr,
           in_sem, pmv_sem, s0_send, s0_recv, rs_send, er_recv, cd_recv, ab_recv, f_recv,
           vec_send, vec_recv, norm_send, norm_recv,
           ag_send, ag_ab, ag_cd, ag_cd1, ag_h2, ag_h3, ag_d2d):
    me = lax.axis_index("dp")
    c = me % 2
    x = (me // 2) % 2
    y = (me // 4) % 2
    z = me // 8

    def dev(zz, yy, xx, cc):
        return ((zz * 2 + yy) * 2 + xx) * 2 + cc

    partner = dev(z, y, x, 1 - c)
    xs = dev(z, y, 1 - x, c)
    xo = dev(z, y, 1 - x, 1 - c)
    ys = dev(z, 1 - y, x, c)
    yo = dev(z, 1 - y, x, 1 - c)
    up = dev((z + 1) % 4, y, x, c)
    down = dev((z + 3) % 4, y, x, c)
    z1 = dev(z + 1 - 2 * (z % 2), y, x, c)
    z2 = dev((z + 2) % 4, y, x, c)
    nlow = z >= 1
    nhigh = z <= 2

    def send(src, dst, ssem, rsem, to):
        pltpu.make_async_remote_copy(
            src_ref=src, dst_ref=dst, send_sem=ssem, recv_sem=rsem, device_id=(to,), device_id_type=MESH
        ).start()

    def wait(ref, sem):
        pltpu.make_async_copy(ref, ref, sem).wait()

    def fetch(k, slot):
        def one(d, carry):
            off = pl.multiple_of((d * PIECE + k * ROWS) * 128, 1024)
            pltpu.make_async_copy(g.at[0:1, pl.ds(off, ROWS * 128)], stage.at[slot, d], in_sem.at[slot]).start()
            return carry
        lax.fori_loop(0, DP, one, 0)

    fetch(0, 0)
    pltpu.make_async_copy(p, po, pmv_sem.at[0]).start()
    pltpu.make_async_copy(m, mo, pmv_sem.at[1]).start()
    pltpu.make_async_copy(v, vo, pmv_sem.at[2]).start()

    barrier = pltpu.get_barrier_semaphore()
    for nb in (partner, xs, xo, ys, yo, z2):
        pl.semaphore_signal(barrier, inc=1, device_id=(nb,), device_id_type=MESH)

    @pl.when(nhigh)
    def _():
        pl.semaphore_signal(barrier, inc=1, device_id=(up,), device_id_type=MESH)

    @pl.when(nlow)
    def _():
        pl.semaphore_signal(barrier, inc=1, device_id=(down,), device_id_type=MESH)

    vs[0, 0:128] = gv[0:1, 0:16384].astype(F32).reshape(128, 128)
    vs[0, 128:VPAD] = jnp.zeros((VPAD - 128, 128), F32)
    vs[0, 128:VEC] = gv[0:1, 16384:16640].astype(F32).reshape(2, 128)
    ssq[...] = jnp.zeros((8, 128), F32)

    mid = (z >= 1) & (z <= 2)

    def await_neighbours():
        @pl.when(mid)
        def _():
            pl.semaphore_wait(barrier, 8)

        @pl.when(jnp.logical_not(mid))
        def _():
            pl.semaphore_wait(barrier, 7)

    partners = (partner, xs, ys, z1, z2)

    def vec_step(j):
        if j > 0:
            wait(vr.at[j - 1], vec_recv.at[j - 1])
            vs[j] = vs[j - 1] + vr[j - 1]
        if j < 5:
            send(vs.at[j], vr.at[j], vec_send.at[j], vec_recv.at[j], partners[j])

    per = PIECE // (24 * HALF)

    def rpiece(k, d):
        at = (2 * k + d) // per
        return at // 8, (at // 4) % 2, (at // 2) % 2, at % 2

    def roff(k, d):
        return ((2 * k + d) % per) * 24 * HALF

    def rbuf(k, d, j):
        return pb.at[(*rpiece(k, d), pl.ds(roff(k, d) + j * 8 * HALF, 8 * HALF))]

    def convert(k):
        slot = k % 2
        dslot = k % 4

        @pl.when(k + 1 < CHUNKS)
        def _():
            fetch(k + 1, 1 - slot)

        @pl.when(k >= 4)
        def _():
            wait(dense.at[dslot, :, pl.ds(1, 3)], s0_send.at[dslot])

        wait(stage.at[slot], in_sem.at[slot])

        def conv(b, carry):
            row = pl.multiple_of(b * HALF, 16)
            for d in range(2):
                for q in range(4):
                    cc = 1 - c if q % 2 else c
                    if d == 0:
                        piece = dev(b // 2, b % 2, 1 - x if q >= 2 else x, cc)
                    else:
                        piece = dev(b // 2, 1 - y if q >= 2 else y, b % 2, cc)
                    vals = stage[slot, piece, 0:1, d * HALF * 128:(d + 1) * HALF * 128].astype(F32)
                    dense[dslot, d, q, pl.ds(row, HALF)] = vals.reshape(HALF, 128).astype(BF16)
            return carry

        lax.fori_loop(0, 8, conv, 0)

    def stage0(k):
        dslot = k % 4
        for q in (3, 2, 1):
            for d in range(2):
                to = ((partner, xs, xo), (partner, ys, yo))[d][q - 1]
                send(dense.at[dslot, d, q], rbuf(k, d, q - 1), s0_send.at[dslot], s0_recv.at[k], to)

        @pl.when(k + 1 < CHUNKS)
        def _():
            convert(k + 1)

    def z_first(k, bufs, recv, rsem):
        @pl.when(z == 0)
        def _():
            send(bufs.at[pl.ds(1, 3)], recv.at[pl.ds(0, 3)], rs_send.at[k], rsem.at[0], up)

        @pl.when(z == 3)
        def _():
            send(bufs.at[pl.ds(0, 3)], recv.at[pl.ds(0, 3)], rs_send.at[k], rsem.at[0], down)

    def z_second(k, bufs, recv, rsem):
        @pl.when(z == 1)
        def _():
            wait(recv.at[pl.ds(0, 3)], rsem.at[0])
            bufs[1:4] += recv[0:3]
            send(bufs.at[pl.ds(2, 2)], recv.at[pl.ds(3, 2)], rs_send.at[k], rsem.at[1], up)

        @pl.when(z == 2)
        def _():
            wait(recv.at[pl.ds(0, 3)], rsem.at[0])
            bufs[0:3] += recv[0:3]
            send(bufs.at[pl.ds(0, 2)], recv.at[pl.ds(3, 2)], rs_send.at[k], rsem.at[1], down)

    def z_third(k, bufs, recv, rsem):
        @pl.when(z == 1)
        def _():
            wait(recv.at[pl.ds(3, 2)], rsem.at[1])
            bufs[0:2] += recv[3:5]
            send(bufs.at[0], recv.at[0], rs_send.at[k], rsem.at[0], down)

        @pl.when(z == 2)
        def _():
            wait(recv.at[pl.ds(3, 2)], rsem.at[1])
            bufs[2:4] += recv[3:5]
            send(bufs.at[3], recv.at[0], rs_send.at[k], rsem.at[0], up)

    def z_final(k, bufs, recv, rsem):
        @pl.when(jnp.logical_not(mid))
        def _():
            wait(recv.at[0], rsem.at[0])
            bufs[z] += recv[0]

    def stage1(k):
        dslot = k % 4
        wait(dense.at[dslot, :, pl.ds(1, 3)], s0_recv.at[k])
        for d in range(2):
            def add(b, carry, d=d):
                row = pl.multiple_of(b * HALF, 16)
                tot = dense[dslot, d, 0, pl.ds(row, HALF)].astype(F32)
                for j in range(3):
                    off = pl.multiple_of(roff(k, d) + j * 8 * HALF + b * HALF, 16)
                    tot = tot + pb[(*rpiece(k, d), pl.ds(off, HALF))].astype(F32)
                pab[k, d, b % 2, b // 2] = tot[0:RAB]
                pcd[k, d, b // 2, b % 2] = tot[RAB:HALF]
                return carry
            lax.fori_loop(0, 8, add, 0)
        send(pab.at[k, 0, 1 - y], er.at[k, 0], rs_send.at[k], er_recv.at[k], ys)
        send(pab.at[k, 1, 1 - x], er.at[k, 1], rs_send.at[k], er_recv.at[k], xs)
        for d in range(2):
            z_first(k, pcd.at[k, d], cdr.at[k, d], cd_recv.at[k, d])

    def stage2(k):
        for d in range(2):
            z_second(k, pcd.at[k, d], cdr.at[k, d], cd_recv.at[k, d])
        wait(er.at[k], er_recv.at[k])
        for zz in range(4):
            abz[k, zz, 0] = pab[k, 0, y, zz] + er[k, 0, zz]
            abz[k, zz, 1] = pab[k, 1, x, zz] + er[k, 1, zz]
        z_first(k, abz.at[k], abr.at[k], ab_recv.at[k])

    def stage3(k):
        for d in range(2):
            z_third(k, pcd.at[k, d], cdr.at[k, d], cd_recv.at[k, d])
        z_second(k, abz.at[k], abr.at[k], ab_recv.at[k])

    def stage4(k):
        for d in range(2):
            z_final(k, pcd.at[k, d], cdr.at[k, d], cd_recv.at[k, d])
        send(pcd.at[k, 0, z, 1 - y], fr.at[k, 0], rs_send.at[k], f_recv.at[k], ys)
        send(pcd.at[k, 1, z, 1 - x], fr.at[k, 1], rs_send.at[k], f_recv.at[k], xs)
        z_third(k, abz.at[k], abr.at[k], ab_recv.at[k])

    def stage5(k):
        z_final(k, abz.at[k], abr.at[k], ab_recv.at[k])
        wait(fr.at[k], f_recv.at[k])
        base = pl.multiple_of(k * ROWS, 16)
        parts = (
            (0, RAB, abz[k, z, 0]),
            (RAB, RCD, pcd[k, 0, z, y] + fr[k, 0]),
            (HALF, RAB, abz[k, z, 1]),
            (HALF + RAB, RCD, pcd[k, 1, z, x] + fr[k, 1]),
        )
        acc = ssq[...]
        for off, num, val in parts:
            val = val * (1.0 / DP)
            gsum[pl.ds(base + off, num)] = val
            acc = acc + jnp.sum((val * val).reshape(num // 8, 8, 128), axis=0)
        ssq[...] = acc

    def rs_iter(i, carry):
        for s, fn in enumerate((stage0, stage1, stage2, stage3, stage4, stage5)):
            k = i - SKEW_RS * s

            @pl.when((k >= 0) & (k < CHUNKS))
            def _(fn=fn, k=k):
                fn(k)
        for j in range(6):
            @pl.when(i == 1 + 2 * j)
            def _(j=j):
                vec_step(j)
        return carry

    convert(0)
    await_neighbours()
    lax.fori_loop(0, CHUNKS + 5 * SKEW_RS, rs_iter, 0)

    ns[...] = jnp.sum(ssq[...], axis=0, keepdims=True)
    nr[me] = ns[...]

    def tell(j, carry):
        send(ns, nr.at[me], norm_send, norm_recv, (me + j) % DP)
        return carry

    lax.fori_loop(1, DP, tell, 0)
    wait(nr.at[pl.ds(0, DP - 1)], norm_recv)
    gvec = vs[5, 0:VEC] * (1.0 / DP)
    norm_sq = jnp.full((8, 128), jnp.sum(nr[...]) + jnp.sum(gvec * gvec))
    clip[...] = jnp.minimum(1.0, MAX_NORM / (jnp.sqrt(norm_sq) + NORM_EPS))
    rate = lr[0, 0]

    wait(po, pmv_sem.at[0])
    wait(mo, pmv_sem.at[1])
    wait(vo, pmv_sem.at[2])

    def cut(k, off, num):
        return pl.ds(pl.multiple_of(k * AG_ROWS + off, 16), num)

    def rows_of(k):
        return (cut(k, 0, AG_AB), cut(k, AG_AB, AG_AB), cut(k, 2 * AG_AB, AG_CD), cut(k, 2 * AG_AB + AG_CD, AG_CD))

    full = slice(None)

    def region(zz, yy, xx, rows):
        return pb.at[zz, yy, xx, c, rows]

    def push(ref, k, rsem, to):
        send(ref, ref, ag_send.at[k], rsem, to)

    def sides(dist, fn):
        if dist == 0:
            fn(z, None)
            return

        @pl.when(z - dist >= 0)
        def _():
            fn(z - dist, 0)

        @pl.when(z + dist <= 3)
        def _():
            fn(z + dist, 1)

    def along_z(fn):
        @pl.when(nhigh)
        def _():
            fn(0, up)

        @pl.when(nlow)
        def _():
            fn(1, down)

    def onward_z(side, dist, fn):
        if dist == 0:
            along_z(fn)
        elif dist < 3 and side == 0:
            @pl.when(nhigh)
            def _():
                fn(0, up)
        elif dist < 3:
            @pl.when(nlow)
            def _():
                fn(1, down)

    def ab_arrived(k, dist):
        ra, rb = rows_of(k)[:2]
        ab = cut(k, 0, 2 * AG_AB)

        def fn(zz, side):
            if dist:
                wait(region(0, 0, 0, ab), ag_ab.at[k, side, dist - 1])
            onward_z(side, dist, lambda way, to: push(region(zz, y, x, ab), k, ag_ab.at[k, way, dist], to))
            push(region(zz, y, x, ra), k, ag_h2.at[k, zz], ys)
            push(region(zz, y, x, rb), k, ag_h2.at[k, zz], xs)

        sides(dist, fn)

    def ab_second(k, dist):
        ra, rb = rows_of(k)[:2]

        def fn(zz, side):
            wait(region(0, 0, 0, cut(k, 0, 2 * AG_AB)), ag_h2.at[k, zz])
            push(region(zz, full, x, ra), k, ag_h3.at[k], xs)
            push(region(zz, y, full, rb), k, ag_h3.at[k], ys)

        sides(dist, fn)

    def cd_arrived(k, dist):
        rc, rd = rows_of(k)[2:]

        def fn(zz, side):
            if dist == 0:
                wait(region(0, 0, 0, cut(k, 0, 2 * AG_CD)), ag_cd1.at[k])
            else:
                wait(pb.at[0, 0, full, full, rc], ag_cd.at[k, side, dist - 1])

            def on(way, to):
                push(region(zz, full, x, rc), k, ag_cd.at[k, way, dist], to)
                push(region(zz, y, full, rd), k, ag_cd.at[k, way, dist], to)

            onward_z(side, dist, on)
            push(region(zz, full, x, rc), k, ag_h3.at[k], xs)
            push(region(zz, y, full, rd), k, ag_h3.at[k], ys)

        sides(dist, fn)

    def ag0(k):
        def upd(b, carry):
            rows = pl.ds(pl.multiple_of(k * AG_ROWS + b * 32, 16), 32)
            new = adam_update(gsum[rows] * clip[0:1], po[rows], mo[rows], vo[rows], rate, WEIGHT_DECAY)
            po[rows], mo[rows], vo[rows] = new
            pb[z, y, x, c, rows] = new[0].astype(BF16)
            return carry
        lax.fori_loop(0, AG_ROWS // 32, upd, 0)
        rc, rd = rows_of(k)[2:]
        push(region(z, y, x, rc), k, ag_cd1.at[k], ys)
        push(region(z, y, x, rd), k, ag_cd1.at[k], xs)
        ab_arrived(k, 0)

    def middle(s):
        def fn(k):
            cd_arrived(k, s - 1)
            if s <= 3:
                ab_arrived(k, s)
            ab_second(k, s - 1)
        return fn

    def ag5(k):
        wait(pb.at[0, full, full, full, cut(k, 0, AG_ROWS)], ag_h3.at[k])
        push(region(full, full, full, cut(k, 0, AG_ROWS)), k, ag_d2d.at[k], partner)

    def ag_iter(i, carry):
        for s, fn in enumerate((ag0, middle(1), middle(2), middle(3), middle(4), ag5)):
            k = i - SKEW_AG * s

            @pl.when((k >= 0) & (k < AG_CHUNKS))
            def _(fn=fn, k=k):
                fn(k)
        return carry

    lax.fori_loop(0, AG_CHUNKS + 5 * SKEW_AG, ag_iter, 0)

    newv = adam_update(gvec * clip[0:1], pv[...], mv[...], vv[...], rate, 0.0)
    pvo[...], mvo[...], vvo[...] = newv

    def drain_rs(k, carry):
        wait(gsum.at[pl.ds(0, 14 * HALF)], rs_send.at[k])
        return carry

    def drain_ag(k, carry):
        wait(pb.at[full, full, full, 0, cut(k, 0, AG_ROWS)], ag_d2d.at[k])
        base, along = 24 * AG_AB + 18 * AG_CD + 16 * AG_ROWS, 2 * AG_AB + 4 * AG_CD

        @pl.when(mid)
        def _():
            wait(pb.at[0, 0, full, full, pl.ds(0, (base + 5 * along) // 4)], ag_send.at[k])

        @pl.when(jnp.logical_not(mid))
        def _():
            wait(pb.at[0, 0, 0, full, pl.ds(0, (base + along) // 2)], ag_send.at[k])

        return carry

    lax.fori_loop(0, CHUNKS, drain_rs, 0)
    lax.fori_loop(0, AG_CHUNKS, drain_ag, 0)
    for s in range(4):
        wait(dense.at[s, :, pl.ds(1, 3)], s0_send.at[s])
    for j in range(5):
        wait(vs.at[j], vec_send.at[j])
    wait(nr.at[pl.ds(0, DP - 1)], norm_send)


def finish(*refs):
    srcs, dsts, sem = refs[:7], refs[7:14], refs[14]
    copies = [pltpu.make_async_copy(srcs[6].at[zz, yy], dsts[6].at[zz, yy], sem.at[6 + zz * 2 + yy]) for zz in range(4) for yy in range(2)]
    copies += [pltpu.make_async_copy(srcs[i], dsts[i], sem.at[i]) for i in range(6)]
    for copy in copies:
        copy.start()
    for copy in copies:
        copy.wait()


def solution(mesh):
    axis_name = mesh.axis_names[0]
    vm = pl.BlockSpec(memory_space=pltpu.VMEM)
    hbm = pl.BlockSpec(memory_space=pl.ANY)
    dma = pltpu.SemaphoreType.DMA
    K, G = CHUNKS, AG_CHUNKS

    call = pl.pallas_call(
        kernel,
        name="adam_step",
        out_shape=(
            [pltpu.VMEM((PIECE, 128), F32)] * 3
            + [pltpu.VMEM((VEC, 128), F32)] * 3
            + [pltpu.VMEM((4, 2, 2, 2, PIECE, 128), BF16)]
        ),
        in_specs=[hbm, vm, hbm, hbm, hbm, vm, vm, vm, pl.BlockSpec(memory_space=pltpu.SMEM)],
        out_specs=[vm] * 7,
        scratch_shapes=[
            pltpu.VMEM((2, DP, 1, ROWS * 128), BF16),
            pltpu.VMEM((4, 2, 4, 8 * HALF, 128), BF16),
            pltpu.VMEM((K, 2, 2, 4, RAB, 128), F32),
            pltpu.VMEM((K, 2, 4, 2, RCD, 128), F32),
            pltpu.VMEM((K, 4, 2, RAB, 128), F32),
            pltpu.VMEM((K, 2, 4, RAB, 128), F32),
            pltpu.VMEM((K, 2, 5, 2, RCD, 128), F32),
            pltpu.VMEM((K, 5, 2, RAB, 128), F32),
            pltpu.VMEM((K, 2, RCD, 128), F32),
            pltpu.VMEM((PIECE, 128), F32),
            pltpu.VMEM((8, 128), F32),
            pltpu.VMEM((8, 128), F32),
            pltpu.VMEM((6, VPAD, 128), F32),
            pltpu.VMEM((5, VPAD, 128), F32),
            pltpu.VMEM((1, 128), F32),
            pltpu.VMEM((DP, 1, 128), F32),
            dma((2,)), dma((3,)), dma((4,)), dma((K,)), dma((K,)), dma((K,)), dma((K, 2, 2)), dma((K, 2)), dma((K,)),
            dma((5,)), dma((5,)), dma, dma,
            dma((G,)), dma((G, 2, 3)), dma((G, 2, 3)), dma((G,)), dma((G, 4)), dma((G,)), dma((G,)),
        ],
        compiler_params=pltpu.CompilerParams(
            collective_id=0, has_side_effects=True, vmem_limit_bytes=37 * 2 ** 20
        ),
    )

    shapes = [(PIECE, 128)] * 3 + [(VEC, 128)] * 3
    copy_out = pl.pallas_call(
        finish,
        name="copy_out",
        out_shape=[jax.ShapeDtypeStruct(s, F32) for s in shapes] + [jax.ShapeDtypeStruct((4, 2, 2, 2, PIECE, 128), BF16)],
        in_specs=[vm] * 7,
        out_specs=[hbm] * 7,
        scratch_shapes=[dma((14,))],
        compiler_params=pltpu.CompilerParams(vmem_limit_bytes=2 ** 20),
    )

    def local_step(g_mat, g_vec, p_mat, m_mat, v_mat, p_vec, m_vec, v_vec, learn_rate):
        outs = call(
            g_mat, g_vec,
            p_mat.reshape(PIECE, 128), m_mat.reshape(PIECE, 128), v_mat.reshape(PIECE, 128),
            p_vec.reshape(VEC, 128), m_vec.reshape(VEC, 128), v_vec.reshape(VEC, 128),
            learn_rate.reshape(1, 1),
        )
        return tuple(o.reshape(-1) for o in copy_out(*outs))

    return jax.shard_map(
        local_step,
        mesh=mesh,
        in_specs=(P(axis_name, None), P(axis_name, None), P(axis_name), P(axis_name), P(axis_name), P(), P(), P(), P()),
        out_specs=(P(axis_name), P(axis_name), P(axis_name), P(), P(), P(), P()),
        check_vma=False,
    )
```

```python
import jax
import jax.numpy as jnp
from jax import lax
from jax.experimental import pallas as pl
from jax.experimental.pallas import tpu as pltpu
from jax.sharding import PartitionSpec as P

STEP = 10
ADAM_BETA1 = 0.9
ADAM_BETA2 = 0.98
ADAM_EPS = 1e-8
WEIGHT_DECAY = 0.01
MAX_NORM = 1.0
NORM_EPS = 1e-6
BIAS_ONE = 1.0 - ADAM_BETA1 ** STEP
BIAS_TWO = 1.0 - ADAM_BETA2 ** STEP

DP = 32
AG_CHUNKS = 15
AG_ROWS = 160
AG_AB = 40
AG_CD = 40
PIECE = 2400
CHUNKS = 25
ROWS = PIECE // CHUNKS
HALF = ROWS // 2
RAB = 24
RCD = HALF - RAB
SKEW_RS = 2
SKEW_AG = 1
VEC = 130
VPAD = 136
MESH = pl.DeviceIdType.MESH
F32 = jnp.float32
BF16 = jnp.bfloat16


def adam_update(grad_vals, param_vals, moment_one, moment_two, learn_rate, decay_rate):
    new_one = ADAM_BETA1 * moment_one + (1.0 - ADAM_BETA1) * grad_vals
    new_two = ADAM_BETA2 * moment_two + (1.0 - ADAM_BETA2) * grad_vals * grad_vals
    direction = (new_one / BIAS_ONE) / (jnp.sqrt(new_two / BIAS_TWO) + ADAM_EPS)
    return param_vals - learn_rate * (direction + decay_rate * param_vals), new_one, new_two


def kernel(g, gv, p, m, v, pv, mv, vv, lr,
           po, mo, vo, pvo, mvo, vvo, pb,
           stage, dense, pab, pcd, abz, er, cdr, abr, fr, gsum, ssq, clip, vs, vr, ns, nr,
           in_sem, pmv_sem, s0_send, s0_recv, rs_send, er_recv, cd_recv, ab_recv, f_recv,
           vec_send, vec_recv, norm_send, norm_recv,
           ag_send, ag_ab, ag_cd, ag_cd1, ag_h2, ag_h3, ag_d2d):
    me = lax.axis_index("dp")
    c = me % 2
    x = (me // 2) % 2
    y = (me // 4) % 2
    z = me // 8

    def dev(zz, yy, xx, cc):
        return ((zz * 2 + yy) * 2 + xx) * 2 + cc

    partner = dev(z, y, x, 1 - c)
    xs = dev(z, y, 1 - x, c)
    xo = dev(z, y, 1 - x, 1 - c)
    ys = dev(z, 1 - y, x, c)
    yo = dev(z, 1 - y, x, 1 - c)
    up = dev((z + 1) % 4, y, x, c)
    down = dev((z + 3) % 4, y, x, c)
    z1 = dev(z + 1 - 2 * (z % 2), y, x, c)
    z2 = dev((z + 2) % 4, y, x, c)
    nlow = z >= 1
    nhigh = z <= 2

    def send(src, dst, ssem, rsem, to):
        pltpu.make_async_remote_copy(
            src_ref=src, dst_ref=dst, send_sem=ssem, recv_sem=rsem, device_id=(to,), device_id_type=MESH
        ).start()

    def wait(ref, sem):
        pltpu.make_async_copy(ref, ref, sem).wait()

    def fetch(k, slot):
        def one(d, carry):
            off = pl.multiple_of((d * PIECE + k * ROWS) * 128, 1024)
            pltpu.make_async_copy(g.at[0:1, pl.ds(off, ROWS * 128)], stage.at[slot, d], in_sem.at[slot]).start()
            return carry
        lax.fori_loop(0, DP, one, 0)

    fetch(0, 0)
    pltpu.make_async_copy(p, po, pmv_sem.at[0]).start()
    pltpu.make_async_copy(m, mo, pmv_sem.at[1]).start()
    pltpu.make_async_copy(v, vo, pmv_sem.at[2]).start()

    barrier = pltpu.get_barrier_semaphore()
    for nb in (partner, xs, xo, ys, yo, z2):
        pl.semaphore_signal(barrier, inc=1, device_id=(nb,), device_id_type=MESH)

    @pl.when(nhigh)
    def _():
        pl.semaphore_signal(barrier, inc=1, device_id=(up,), device_id_type=MESH)

    @pl.when(nlow)
    def _():
        pl.semaphore_signal(barrier, inc=1, device_id=(down,), device_id_type=MESH)

    vs[0, 0:128] = gv[0:1, 0:16384].astype(F32).reshape(128, 128)
    vs[0, 128:VPAD] = jnp.zeros((VPAD - 128, 128), F32)
    vs[0, 128:VEC] = gv[0:1, 16384:16640].astype(F32).reshape(2, 128)
    ssq[...] = jnp.zeros((8, 128), F32)

    mid = (z >= 1) & (z <= 2)

    def await_neighbours():
        @pl.when(mid)
        def _():
            pl.semaphore_wait(barrier, 8)

        @pl.when(jnp.logical_not(mid))
        def _():
            pl.semaphore_wait(barrier, 7)

    partners = (partner, xs, ys, z1, z2)

    def vec_step(j):
        if j > 0:
            wait(vr.at[j - 1], vec_recv.at[j - 1])
            vs[j] = vs[j - 1] + vr[j - 1]
        if j < 5:
            send(vs.at[j], vr.at[j], vec_send.at[j], vec_recv.at[j], partners[j])

    per = PIECE // (24 * HALF)

    def rpiece(k, d):
        at = (2 * k + d) // per
        return at // 8, (at // 4) % 2, (at // 2) % 2, at % 2

    def roff(k, d):
        return ((2 * k + d) % per) * 24 * HALF

    def rbuf(k, d, j):
        return pb.at[(*rpiece(k, d), pl.ds(roff(k, d) + j * 8 * HALF, 8 * HALF))]

    def convert(k):
        slot = k % 2
        dslot = k % 4

        @pl.when(k + 1 < CHUNKS)
        def _():
            fetch(k + 1, 1 - slot)

        @pl.when(k >= 4)
        def _():
            wait(dense.at[dslot, :, pl.ds(1, 3)], s0_send.at[dslot])

        wait(stage.at[slot], in_sem.at[slot])

        def conv(b, carry):
            row = pl.multiple_of(b * HALF, 16)
            for d in range(2):
                for q in range(4):
                    cc = 1 - c if q % 2 else c
                    if d == 0:
                        piece = dev(b // 2, b % 2, 1 - x if q >= 2 else x, cc)
                    else:
                        piece = dev(b // 2, 1 - y if q >= 2 else y, b % 2, cc)
                    vals = stage[slot, piece, 0:1, d * HALF * 128:(d + 1) * HALF * 128].astype(F32)
                    dense[dslot, d, q, pl.ds(row, HALF)] = vals.reshape(HALF, 128).astype(BF16)
            return carry

        lax.fori_loop(0, 8, conv, 0)

    def stage0(k):
        dslot = k % 4
        for q in (3, 2, 1):
            for d in range(2):
                to = ((partner, xs, xo), (partner, ys, yo))[d][q - 1]
                send(dense.at[dslot, d, q], rbuf(k, d, q - 1), s0_send.at[dslot], s0_recv.at[k], to)

        @pl.when(k + 1 < CHUNKS)
        def _():
            convert(k + 1)

    def z_first(k, bufs, recv, rsem):
        @pl.when(z == 0)
        def _():
            send(bufs.at[pl.ds(1, 3)], recv.at[pl.ds(0, 3)], rs_send.at[k], rsem.at[0], up)

        @pl.when(z == 3)
        def _():
            send(bufs.at[pl.ds(0, 3)], recv.at[pl.ds(0, 3)], rs_send.at[k], rsem.at[0], down)

    def z_second(k, bufs, recv, rsem):
        @pl.when(z == 1)
        def _():
            wait(recv.at[pl.ds(0, 3)], rsem.at[0])
            bufs[1:4] += recv[0:3]
            send(bufs.at[pl.ds(2, 2)], recv.at[pl.ds(3, 2)], rs_send.at[k], rsem.at[1], up)

        @pl.when(z == 2)
        def _():
            wait(recv.at[pl.ds(0, 3)], rsem.at[0])
            bufs[0:3] += recv[0:3]
            send(bufs.at[pl.ds(0, 2)], recv.at[pl.ds(3, 2)], rs_send.at[k], rsem.at[1], down)

    def z_third(k, bufs, recv, rsem):
        @pl.when(z == 1)
        def _():
            wait(recv.at[pl.ds(3, 2)], rsem.at[1])
            bufs[0:2] += recv[3:5]
            send(bufs.at[0], recv.at[0], rs_send.at[k], rsem.at[0], down)

        @pl.when(z == 2)
        def _():
            wait(recv.at[pl.ds(3, 2)], rsem.at[1])
            bufs[2:4] += recv[3:5]
            send(bufs.at[3], recv.at[0], rs_send.at[k], rsem.at[0], up)

    def z_final(k, bufs, recv, rsem):
        @pl.when(jnp.logical_not(mid))
        def _():
            wait(recv.at[0], rsem.at[0])
            bufs[z] += recv[0]

    def stage1(k):
        dslot = k % 4
        wait(dense.at[dslot, :, pl.ds(1, 3)], s0_recv.at[k])
        for d in range(2):
            def add(b, carry, d=d):
                row = pl.multiple_of(b * HALF, 16)
                tot = dense[dslot, d, 0, pl.ds(row, HALF)].astype(F32)
                for j in range(3):
                    off = pl.multiple_of(roff(k, d) + j * 8 * HALF + b * HALF, 16)
                    tot = tot + pb[(*rpiece(k, d), pl.ds(off, HALF))].astype(F32)
                pab[k, d, b % 2, b // 2] = tot[0:RAB]
                pcd[k, d, b // 2, b % 2] = tot[RAB:HALF]
                return carry
            lax.fori_loop(0, 8, add, 0)
        send(pab.at[k, 0, 1 - y], er.at[k, 0], rs_send.at[k], er_recv.at[k], ys)
        send(pab.at[k, 1, 1 - x], er.at[k, 1], rs_send.at[k], er_recv.at[k], xs)
        for d in range(2):
            z_first(k, pcd.at[k, d], cdr.at[k, d], cd_recv.at[k, d])

    def stage2(k):
        for d in range(2):
            z_second(k, pcd.at[k, d], cdr.at[k, d], cd_recv.at[k, d])
        wait(er.at[k], er_recv.at[k])
        for zz in range(4):
            abz[k, zz, 0] = pab[k, 0, y, zz] + er[k, 0, zz]
            abz[k, zz, 1] = pab[k, 1, x, zz] + er[k, 1, zz]
        z_first(k, abz.at[k], abr.at[k], ab_recv.at[k])

    def stage3(k):
        for d in range(2):
            z_third(k, pcd.at[k, d], cdr.at[k, d], cd_recv.at[k, d])
        z_second(k, abz.at[k], abr.at[k], ab_recv.at[k])

    def stage4(k):
        for d in range(2):
            z_final(k, pcd.at[k, d], cdr.at[k, d], cd_recv.at[k, d])
        send(pcd.at[k, 0, z, 1 - y], fr.at[k, 0], rs_send.at[k], f_recv.at[k], ys)
        send(pcd.at[k, 1, z, 1 - x], fr.at[k, 1], rs_send.at[k], f_recv.at[k], xs)
        z_third(k, abz.at[k], abr.at[k], ab_recv.at[k])

    def stage5(k):
        z_final(k, abz.at[k], abr.at[k], ab_recv.at[k])
        wait(fr.at[k], f_recv.at[k])
        base = pl.multiple_of(k * ROWS, 16)
        parts = (
            (0, RAB, abz[k, z, 0]),
            (RAB, RCD, pcd[k, 0, z, y] + fr[k, 0]),
            (HALF, RAB, abz[k, z, 1]),
            (HALF + RAB, RCD, pcd[k, 1, z, x] + fr[k, 1]),
        )
        acc = ssq[...]
        for off, num, val in parts:
            val = val * (1.0 / DP)
            gsum[pl.ds(base + off, num)] = val
            acc = acc + jnp.sum((val * val).reshape(num // 8, 8, 128), axis=0)
        ssq[...] = acc

    def rs_iter(i, carry):
        for s, fn in enumerate((stage0, stage1, stage2, stage3, stage4, stage5)):
            k = i - SKEW_RS * s

            @pl.when((k >= 0) & (k < CHUNKS))
            def _(fn=fn, k=k):
                fn(k)
        for j in range(6):
            @pl.when(i == 1 + 2 * j)
            def _(j=j):
                vec_step(j)
        return carry

    convert(0)
    await_neighbours()
    lax.fori_loop(0, CHUNKS + 5 * SKEW_RS, rs_iter, 0)

    ns[...] = jnp.sum(ssq[...], axis=0, keepdims=True)
    nr[me] = ns[...]

    def tell(j, carry):
        send(ns, nr.at[me], norm_send, norm_recv, (me + j) % DP)
        return carry

    lax.fori_loop(1, DP, tell, 0)
    wait(nr.at[pl.ds(0, DP - 1)], norm_recv)
    gvec = vs[5, 0:VEC] * (1.0 / DP)
    norm_sq = jnp.full((8, 128), jnp.sum(nr[...]) + jnp.sum(gvec * gvec))
    clip[...] = jnp.minimum(1.0, MAX_NORM / (jnp.sqrt(norm_sq) + NORM_EPS))
    rate = lr[0, 0]

    wait(po, pmv_sem.at[0])
    wait(mo, pmv_sem.at[1])
    wait(vo, pmv_sem.at[2])

    def cut(k, off, num):
        return pl.ds(pl.multiple_of(k * AG_ROWS + off, 8), num)

    def rows_of(k):
        return (cut(k, 0, AG_AB), cut(k, AG_AB, AG_AB), cut(k, 2 * AG_AB, AG_CD), cut(k, 2 * AG_AB + AG_CD, AG_CD))

    full = slice(None)

    def region(zz, yy, xx, rows):
        return pb.at[zz, yy, xx, c, rows]

    def push(ref, k, rsem, to):
        send(ref, ref, ag_send.at[k], rsem, to)

    def sides(dist, fn):
        if dist == 0:
            fn(z, None)
            return

        @pl.when(z - dist >= 0)
        def _():
            fn(z - dist, 0)

        @pl.when(z + dist <= 3)
        def _():
            fn(z + dist, 1)

    def along_z(fn):
        @pl.when(nhigh)
        def _():
            fn(0, up)

        @pl.when(nlow)
        def _():
            fn(1, down)

    def onward_z(side, dist, fn):
        if dist == 0:
            along_z(fn)
        elif dist < 3 and side == 0:
            @pl.when(nhigh)
            def _():
                fn(0, up)
        elif dist < 3:
            @pl.when(nlow)
            def _():
                fn(1, down)

    def ab_arrived(k, dist):
        ra, rb = rows_of(k)[:2]
        ab = cut(k, 0, 2 * AG_AB)

        def fn(zz, side):
            if dist:
                wait(region(0, 0, 0, ab), ag_ab.at[k, side, dist - 1])
            onward_z(side, dist, lambda way, to: push(region(zz, y, x, ab), k, ag_ab.at[k, way, dist], to))
            push(region(zz, y, x, ra), k, ag_h2.at[k, zz], ys)
            push(region(zz, y, x, rb), k, ag_h2.at[k, zz], xs)

        sides(dist, fn)

    def ab_second(k, dist):
        ra, rb = rows_of(k)[:2]

        def fn(zz, side):
            wait(region(0, 0, 0, cut(k, 0, 2 * AG_AB)), ag_h2.at[k, zz])
            push(region(zz, full, x, ra), k, ag_h3.at[k], xs)
            push(region(zz, y, full, rb), k, ag_h3.at[k], ys)

        sides(dist, fn)

    def cd_arrived(k, dist):
        rc, rd = rows_of(k)[2:]

        def fn(zz, side):
            if dist == 0:
                wait(region(0, 0, 0, cut(k, 0, 2 * AG_CD)), ag_cd1.at[k])
            else:
                wait(pb.at[0, 0, full, full, rc], ag_cd.at[k, side, dist - 1])

            def on(way, to):
                push(region(zz, full, x, rc), k, ag_cd.at[k, way, dist], to)
                push(region(zz, y, full, rd), k, ag_cd.at[k, way, dist], to)

            onward_z(side, dist, on)
            push(region(zz, full, x, rc), k, ag_h3.at[k], xs)
            push(region(zz, y, full, rd), k, ag_h3.at[k], ys)

        sides(dist, fn)

    def ag0(k):
        def upd(b, carry):
            rows = pl.ds(pl.multiple_of(k * AG_ROWS + b * 32, 16), 32)
            new = adam_update(gsum[rows] * clip[0:1], po[rows], mo[rows], vo[rows], rate, WEIGHT_DECAY)
            po[rows], mo[rows], vo[rows] = new
            pb[z, y, x, c, rows] = new[0].astype(BF16)
            return carry
        lax.fori_loop(0, AG_ROWS // 32, upd, 0)
        rc, rd = rows_of(k)[2:]
        push(region(z, y, x, rc), k, ag_cd1.at[k], ys)
        push(region(z, y, x, rd), k, ag_cd1.at[k], xs)
        ab_arrived(k, 0)

    def middle(s):
        def fn(k):
            cd_arrived(k, s - 1)
            if s <= 3:
                ab_arrived(k, s)
            ab_second(k, s - 1)
        return fn

    def ag5(k):
        wait(pb.at[0, full, full, full, cut(k, 0, AG_ROWS)], ag_h3.at[k])
        push(region(full, full, full, cut(k, 0, AG_ROWS)), k, ag_d2d.at[k], partner)

    def ag_iter(i, carry):
        for s, fn in enumerate((ag0, middle(1), middle(2), middle(3), middle(4), ag5)):
            k = i - SKEW_AG * s

            @pl.when((k >= 0) & (k < AG_CHUNKS))
            def _(fn=fn, k=k):
                fn(k)
        return carry

    lax.fori_loop(0, AG_CHUNKS + 5 * SKEW_AG, ag_iter, 0)

    newv = adam_update(gvec * clip[0:1], pv[...], mv[...], vv[...], rate, 0.0)
    pvo[...], mvo[...], vvo[...] = newv

    def drain_rs(k, carry):
        wait(gsum.at[pl.ds(0, 14 * HALF)], rs_send.at[k])
        return carry

    def drain_ag(k, carry):
        wait(pb.at[full, full, full, 0, cut(k, 0, AG_ROWS)], ag_d2d.at[k])
        base, along = 24 * AG_AB + 18 * AG_CD + 16 * AG_ROWS, 2 * AG_AB + 4 * AG_CD

        @pl.when(mid)
        def _():
            wait(pb.at[0, 0, full, full, pl.ds(0, (base + 5 * along) // 4)], ag_send.at[k])

        @pl.when(jnp.logical_not(mid))
        def _():
            wait(pb.at[0, 0, 0, full, pl.ds(0, (base + along) // 2)], ag_send.at[k])

        return carry

    lax.fori_loop(0, CHUNKS, drain_rs, 0)
    lax.fori_loop(0, AG_CHUNKS, drain_ag, 0)
    for s in range(4):
        wait(dense.at[s, :, pl.ds(1, 3)], s0_send.at[s])
    for j in range(5):
        wait(vs.at[j], vec_send.at[j])
    wait(nr.at[pl.ds(0, DP - 1)], norm_send)


def finish(*refs):
    srcs, dsts, sem = refs[:7], refs[7:14], refs[14]
    copies = [pltpu.make_async_copy(srcs[6].at[zz, yy], dsts[6].at[zz, yy], sem.at[6 + zz * 2 + yy]) for zz in range(4) for yy in range(2)]
    copies += [pltpu.make_async_copy(srcs[i], dsts[i], sem.at[i]) for i in range(6)]
    for copy in copies:
        copy.start()
    for copy in copies:
        copy.wait()


def solution(mesh):
    axis_name = mesh.axis_names[0]
    vm = pl.BlockSpec(memory_space=pltpu.VMEM)
    hbm = pl.BlockSpec(memory_space=pl.ANY)
    dma = pltpu.SemaphoreType.DMA
    K, G = CHUNKS, AG_CHUNKS

    call = pl.pallas_call(
        kernel,
        name="adam_step",
        out_shape=(
            [pltpu.VMEM((PIECE, 128), F32)] * 3
            + [pltpu.VMEM((VEC, 128), F32)] * 3
            + [pltpu.VMEM((4, 2, 2, 2, PIECE, 128), BF16)]
        ),
        in_specs=[hbm, vm, hbm, hbm, hbm, vm, vm, vm, pl.BlockSpec(memory_space=pltpu.SMEM)],
        out_specs=[vm] * 7,
        scratch_shapes=[
            pltpu.VMEM((2, DP, 1, ROWS * 128), BF16),
            pltpu.VMEM((4, 2, 4, 8 * HALF, 128), BF16),
            pltpu.VMEM((K, 2, 2, 4, RAB, 128), F32),
            pltpu.VMEM((K, 2, 4, 2, RCD, 128), F32),
            pltpu.VMEM((K, 4, 2, RAB, 128), F32),
            pltpu.VMEM((K, 2, 4, RAB, 128), F32),
            pltpu.VMEM((K, 2, 5, 2, RCD, 128), F32),
            pltpu.VMEM((K, 5, 2, RAB, 128), F32),
            pltpu.VMEM((K, 2, RCD, 128), F32),
            pltpu.VMEM((PIECE, 128), F32),
            pltpu.VMEM((8, 128), F32),
            pltpu.VMEM((8, 128), F32),
            pltpu.VMEM((6, VPAD, 128), F32),
            pltpu.VMEM((5, VPAD, 128), F32),
            pltpu.VMEM((1, 128), F32),
            pltpu.VMEM((DP, 1, 128), F32),
            dma((2,)), dma((3,)), dma((4,)), dma((K,)), dma((K,)), dma((K,)), dma((K, 2, 2)), dma((K, 2)), dma((K,)),
            dma((5,)), dma((5,)), dma, dma,
            dma((G,)), dma((G, 2, 3)), dma((G, 2, 3)), dma((G,)), dma((G, 4)), dma((G,)), dma((G,)),
        ],
        compiler_params=pltpu.CompilerParams(
            collective_id=0, has_side_effects=True, vmem_limit_bytes=37 * 2 ** 20
        ),
    )

    shapes = [(PIECE, 128)] * 3 + [(VEC, 128)] * 3
    copy_out = pl.pallas_call(
        finish,
        name="copy_out",
        out_shape=[jax.ShapeDtypeStruct(s, F32) for s in shapes] + [jax.ShapeDtypeStruct((4, 2, 2, 2, PIECE, 128), BF16)],
        in_specs=[vm] * 7,
        out_specs=[hbm] * 7,
        scratch_shapes=[dma((14,))],
        compiler_params=pltpu.CompilerParams(vmem_limit_bytes=2 ** 20),
    )

    def local_step(g_mat, g_vec, p_mat, m_mat, v_mat, p_vec, m_vec, v_vec, learn_rate):
        outs = call(
            g_mat, g_vec,
            p_mat.reshape(PIECE, 128), m_mat.reshape(PIECE, 128), v_mat.reshape(PIECE, 128),
            p_vec.reshape(VEC, 128), m_vec.reshape(VEC, 128), v_vec.reshape(VEC, 128),
            learn_rate.reshape(1, 1),
        )
        return tuple(o.reshape(-1) for o in copy_out(*outs))

    return jax.shard_map(
        local_step,
        mesh=mesh,
        in_specs=(P(axis_name, None), P(axis_name, None), P(axis_name), P(axis_name), P(axis_name), P(), P(), P(), P()),
        out_specs=(P(axis_name), P(axis_name), P(axis_name), P(), P(), P(), P()),
        check_vma=False,
    )
```

```python
import jax
import jax.numpy as jnp
from jax import lax
from jax.experimental import pallas as pl
from jax.experimental.pallas import tpu as pltpu
from jax.sharding import PartitionSpec as P

STEP = 10
ADAM_BETA1 = 0.9
ADAM_BETA2 = 0.98
ADAM_EPS = 1e-8
WEIGHT_DECAY = 0.01
MAX_NORM = 1.0
NORM_EPS = 1e-6
BIAS_ONE = 1.0 - ADAM_BETA1 ** STEP
BIAS_TWO = 1.0 - ADAM_BETA2 ** STEP

DP = 32
AG_CHUNKS = 10
AG_ROWS = 240
AG_AB = 48
AG_CD = 72
PIECE = 2400
CHUNKS = 50
ROWS = PIECE // CHUNKS
HALF = ROWS // 2
RAB = 8
RCD = HALF - RAB
SKEW_RS = 2
AG_STAGES = (0, 2, 3, 4, 5, 6)
SLOTS = 16
VEC = 130
VPAD = 136
MESH = pl.DeviceIdType.MESH
F32 = jnp.float32
BF16 = jnp.bfloat16


def adam_update(grad_vals, param_vals, moment_one, moment_two, learn_rate, decay_rate):
    new_one = ADAM_BETA1 * moment_one + (1.0 - ADAM_BETA1) * grad_vals
    new_two = ADAM_BETA2 * moment_two + (1.0 - ADAM_BETA2) * grad_vals * grad_vals
    direction = (new_one / BIAS_ONE) / (jnp.sqrt(new_two / BIAS_TWO) + ADAM_EPS)
    return param_vals - learn_rate * (direction + decay_rate * param_vals), new_one, new_two


def kernel(g, gv, p, m, v, pv, mv, vv, lr,
           po, mo, vo, pvo, mvo, vvo, pb,
           gvb, stage, dense, pab, pcd, abz, er, cdr, abr, fr, gsum, ssq, clip, vs, vr, ns, nr,
           in_sem, pmv_sem, s0_send, s0_recv, rs_send, er_recv, cd_recv, ab_recv, f_recv,
           vec_send, vec_recv, norm_send, norm_recv,
           ag_send, ag_ab, ag_cd, ag_cd1, ag_h2, ag_h3, ag_d2d):
    me = lax.axis_index("dp")
    c = me % 2
    x = (me // 2) % 2
    y = (me // 4) % 2
    z = me // 8

    def dev(zz, yy, xx, cc):
        return ((zz * 2 + yy) * 2 + xx) * 2 + cc

    partner = dev(z, y, x, 1 - c)
    xs = dev(z, y, 1 - x, c)
    xo = dev(z, y, 1 - x, 1 - c)
    ys = dev(z, 1 - y, x, c)
    yo = dev(z, 1 - y, x, 1 - c)
    up = dev((z + 1) % 4, y, x, c)
    down = dev((z + 3) % 4, y, x, c)
    z1 = dev(z + 1 - 2 * (z % 2), y, x, c)
    z2 = dev((z + 2) % 4, y, x, c)
    nlow = z >= 1
    nhigh = z <= 2

    def send(src, dst, ssem, rsem, to):
        pltpu.make_async_remote_copy(
            src_ref=src, dst_ref=dst, send_sem=ssem, recv_sem=rsem, device_id=(to,), device_id_type=MESH
        ).start()

    def wait(ref, sem):
        pltpu.make_async_copy(ref, ref, sem).wait()

    def fetch(k, slot):
        def one(d, carry):
            off = pl.multiple_of((d * PIECE + k * ROWS) * 128, 1024)
            pltpu.make_async_copy(g.at[0:1, pl.ds(off, ROWS * 128)], stage.at[slot, d], in_sem.at[slot]).start()
            return carry
        lax.fori_loop(0, DP, one, 0)

    fetch(0, 0)

    barrier = pltpu.get_barrier_semaphore()
    for nb in (partner, xs, xo, ys, yo, z2):
        pl.semaphore_signal(barrier, inc=1, device_id=(nb,), device_id_type=MESH)

    @pl.when(nhigh)
    def _():
        pl.semaphore_signal(barrier, inc=1, device_id=(up,), device_id_type=MESH)

    @pl.when(nlow)
    def _():
        pl.semaphore_signal(barrier, inc=1, device_id=(down,), device_id_type=MESH)

    ssq[...] = jnp.zeros((8, 128), F32)

    mid = (z >= 1) & (z <= 2)

    def await_neighbours():
        @pl.when(mid)
        def _():
            pl.semaphore_wait(barrier, 8)

        @pl.when(jnp.logical_not(mid))
        def _():
            pl.semaphore_wait(barrier, 7)

    partners = (partner, xs, ys, z1, z2)

    loads = ((gv, gvb), (p, po), (m, mo), (v, vo), (pv, pvo), (mv, mvo), (vv, vvo))

    def vec_step(j):
        if j == 0:
            for i, (src, dst) in enumerate(loads):
                pltpu.make_async_copy(src, dst, pmv_sem.at[i]).start()
            wait(gvb, pmv_sem.at[0])
            vs[0, 0:128] = gvb[0:1, 0:16384].astype(F32).reshape(128, 128)
            vs[0, 128:VPAD] = jnp.zeros((VPAD - 128, 128), F32)
            vs[0, 128:VEC] = gvb[0:1, 16384:16640].astype(F32).reshape(2, 128)
        else:
            wait(vr.at[j - 1], vec_recv.at[j - 1])
            vs[j] = vs[j - 1] + vr[j - 1]
        if j < 5:
            send(vs.at[j], vr.at[j], vec_send.at[j], vec_recv.at[j], partners[j])

    per = PIECE // (24 * HALF)

    def rpiece(k, d):
        at = (2 * k + d) // per
        return at // 8, (at // 4) % 2, (at // 2) % 2, at % 2

    def roff(k, d):
        return ((2 * k + d) % per) * 24 * HALF

    def rbuf(k, d, j):
        return pb.at[(*rpiece(k, d), pl.ds(roff(k, d) + j * 8 * HALF, 8 * HALF))]

    def convert(k):
        slot = k % 2
        dslot = k % 4

        @pl.when(k + 1 < CHUNKS)
        def _():
            fetch(k + 1, 1 - slot)

        @pl.when(k >= 4)
        def _():
            wait(dense.at[dslot, :, pl.ds(1, 3)], s0_send.at[dslot])

        wait(stage.at[slot], in_sem.at[slot])

        def conv(b, carry):
            row = pl.multiple_of(b * 2 * HALF, 16)
            for d in range(2):
                for q in range(4):
                    cc = 1 - c if q % 2 else c
                    vals = []
                    for o in range(2):
                        if d == 0:
                            piece = dev(b, o, 1 - x if q >= 2 else x, cc)
                        else:
                            piece = dev(b, 1 - y if q >= 2 else y, o, cc)
                        flat = stage[slot, piece, 0:1, d * HALF * 128:(d + 1) * HALF * 128].astype(F32)
                        vals.append(flat.reshape(HALF, 128))
                    dense[dslot, d, q, pl.ds(row, 2 * HALF)] = jnp.concatenate(vals, axis=0).astype(BF16)
            return carry

        lax.fori_loop(0, 4, conv, 0)

    def stage0(k):
        dslot = k % 4
        for q in (3, 2, 1):
            for d in range(2):
                to = ((partner, xs, xo), (partner, ys, yo))[d][q - 1]
                send(dense.at[dslot, d, q], rbuf(k, d, q - 1), s0_send.at[dslot], s0_recv.at[k % SLOTS], to)

        @pl.when(k + 1 < CHUNKS)
        def _():
            convert(k + 1)

    def z_first(k, bufs, recv, rsem):
        @pl.when(z == 0)
        def _():
            send(bufs.at[pl.ds(1, 3)], recv.at[pl.ds(0, 3)], rs_send.at[k], rsem.at[0], up)

        @pl.when(z == 3)
        def _():
            send(bufs.at[pl.ds(0, 3)], recv.at[pl.ds(0, 3)], rs_send.at[k], rsem.at[0], down)

    def z_second(k, bufs, recv, rsem):
        @pl.when(z == 1)
        def _():
            wait(recv.at[pl.ds(0, 3)], rsem.at[0])
            bufs[1:4] += recv[0:3]
            send(bufs.at[pl.ds(2, 2)], recv.at[pl.ds(3, 2)], rs_send.at[k], rsem.at[1], up)

        @pl.when(z == 2)
        def _():
            wait(recv.at[pl.ds(0, 3)], rsem.at[0])
            bufs[0:3] += recv[0:3]
            send(bufs.at[pl.ds(0, 2)], recv.at[pl.ds(3, 2)], rs_send.at[k], rsem.at[1], down)

    def z_third(k, bufs, recv, rsem):
        @pl.when(z == 1)
        def _():
            wait(recv.at[pl.ds(3, 2)], rsem.at[1])
            bufs[0:2] += recv[3:5]
            send(bufs.at[0], recv.at[0], rs_send.at[k], rsem.at[0], down)

        @pl.when(z == 2)
        def _():
            wait(recv.at[pl.ds(3, 2)], rsem.at[1])
            bufs[2:4] += recv[3:5]
            send(bufs.at[3], recv.at[0], rs_send.at[k], rsem.at[0], up)

    def z_final(k, bufs, recv, rsem):
        @pl.when(jnp.logical_not(mid))
        def _():
            wait(recv.at[0], rsem.at[0])
            bufs[z] += recv[0]

    def stage1(k):
        dslot = k % 4
        wait(dense.at[dslot, :, pl.ds(1, 3)], s0_recv.at[k % SLOTS])
        for d in range(2):
            def add(b, carry, d=d):
                row = pl.multiple_of(b * 2 * HALF, 16)
                tot = dense[dslot, d, 0, pl.ds(row, 2 * HALF)].astype(F32)
                for j in range(3):
                    off = pl.multiple_of(roff(k, d) + j * 8 * HALF + b * 2 * HALF, 16)
                    tot = tot + pb[(*rpiece(k, d), pl.ds(off, 2 * HALF))].astype(F32)
                for o in range(2):
                    pab[k, d, o, b] = tot[o * HALF:o * HALF + RAB]
                    pcd[k, d, b, o] = tot[o * HALF + RAB:(o + 1) * HALF]
                return carry
            lax.fori_loop(0, 4, add, 0)
        send(pab.at[k, 0, 1 - y], er.at[k, 0], rs_send.at[k], er_recv.at[k % SLOTS], ys)
        send(pab.at[k, 1, 1 - x], er.at[k, 1], rs_send.at[k], er_recv.at[k % SLOTS], xs)
        for d in range(2):
            z_first(k, pcd.at[k, d], cdr.at[k, d], cd_recv.at[k % SLOTS, d])

    def stage2(k):
        for d in range(2):
            z_second(k, pcd.at[k, d], cdr.at[k, d], cd_recv.at[k % SLOTS, d])
        wait(er.at[k], er_recv.at[k % SLOTS])
        for zz in range(4):
            abz[k, zz, 0] = pab[k, 0, y, zz] + er[k, 0, zz]
            abz[k, zz, 1] = pab[k, 1, x, zz] + er[k, 1, zz]
        z_first(k, abz.at[k], abr.at[k], ab_recv.at[k % SLOTS])

    def stage3(k):
        for d in range(2):
            z_third(k, pcd.at[k, d], cdr.at[k, d], cd_recv.at[k % SLOTS, d])
        z_second(k, abz.at[k], abr.at[k], ab_recv.at[k % SLOTS])

    def stage4(k):
        for d in range(2):
            z_final(k, pcd.at[k, d], cdr.at[k, d], cd_recv.at[k % SLOTS, d])
        send(pcd.at[k, 0, z, 1 - y], fr.at[k, 0], rs_send.at[k], f_recv.at[k % SLOTS], ys)
        send(pcd.at[k, 1, z, 1 - x], fr.at[k, 1], rs_send.at[k], f_recv.at[k % SLOTS], xs)
        z_third(k, abz.at[k], abr.at[k], ab_recv.at[k % SLOTS])

    def stage5(k):
        z_final(k, abz.at[k], abr.at[k], ab_recv.at[k % SLOTS])
        wait(fr.at[k], f_recv.at[k % SLOTS])
        base = pl.multiple_of(k * ROWS, 16)
        parts = (
            (0, RAB, abz[k, z, 0]),
            (RAB, RCD, pcd[k, 0, z, y] + fr[k, 0]),
            (HALF, RAB, abz[k, z, 1]),
            (HALF + RAB, RCD, pcd[k, 1, z, x] + fr[k, 1]),
        )
        acc = ssq[...]
        for off, num, val in parts:
            val = val * (1.0 / DP)
            gsum[pl.ds(base + off, num)] = val
            acc = acc + jnp.sum((val * val).reshape(num // 8, 8, 128), axis=0)
        ssq[...] = acc

    def rs_iter(i, carry):
        for s, fn in enumerate((stage0, stage1, stage2, stage3, stage4, stage5)):
            k = i - SKEW_RS * s

            @pl.when((k >= 0) & (k < CHUNKS))
            def _(fn=fn, k=k):
                fn(k)
        for j in range(6):
            @pl.when(i == 4 + 4 * j)
            def _(j=j):
                vec_step(j)
        return carry

    convert(0)
    await_neighbours()
    lax.fori_loop(0, CHUNKS + 5 * SKEW_RS, rs_iter, 0)

    ns[...] = jnp.sum(ssq[...], axis=0, keepdims=True)
    nr[me] = ns[...]

    def tell(j, carry):
        send(ns, nr.at[me], norm_send, norm_recv, (me + j) % DP)
        return carry

    lax.fori_loop(1, DP, tell, 0)
    wait(nr.at[pl.ds(0, DP - 1)], norm_recv)
    gvec = vs[5, 0:VEC] * (1.0 / DP)
    norm_sq = jnp.full((8, 128), jnp.sum(nr[...]) + jnp.sum(gvec * gvec))
    clip[...] = jnp.minimum(1.0, MAX_NORM / (jnp.sqrt(norm_sq) + NORM_EPS))
    rate = lr[0, 0]

    for i, (_, dst) in enumerate(loads[1:]):
        wait(dst, pmv_sem.at[i + 1])

    def cut(k, off, num):
        return pl.ds(pl.multiple_of(k * AG_ROWS + off, 8), num)

    def rows_of(k):
        return (cut(k, 0, AG_AB), cut(k, AG_AB, AG_AB), cut(k, 2 * AG_AB, AG_CD), cut(k, 2 * AG_AB + AG_CD, AG_CD))

    full = slice(None)

    def region(zz, yy, xx, rows):
        return pb.at[zz, yy, xx, c, rows]

    def push(ref, k, rsem, to):
        send(ref, ref, ag_send.at[k], rsem, to)

    def sides(dist, fn):
        if dist == 0:
            fn(z, None)
            return

        @pl.when(z - dist >= 0)
        def _():
            fn(z - dist, 0)

        @pl.when(z + dist <= 3)
        def _():
            fn(z + dist, 1)

    def along_z(fn):
        @pl.when(nhigh)
        def _():
            fn(0, up)

        @pl.when(nlow)
        def _():
            fn(1, down)

    def onward_z(side, dist, fn):
        if dist == 0:
            along_z(fn)
        elif dist < 3 and side == 0:
            @pl.when(nhigh)
            def _():
                fn(0, up)
        elif dist < 3:
            @pl.when(nlow)
            def _():
                fn(1, down)

    def ab_arrived(k, dist):
        ra, rb = rows_of(k)[:2]
        ab = cut(k, 0, 2 * AG_AB)

        def fn(zz, side):
            if dist:
                wait(region(0, 0, 0, ab), ag_ab.at[k, side, dist - 1])
            onward_z(side, dist, lambda way, to: push(region(zz, y, x, ab), k, ag_ab.at[k, way, dist], to))
            push(region(zz, y, x, ra), k, ag_h2.at[k, zz], ys)
            push(region(zz, y, x, rb), k, ag_h2.at[k, zz], xs)

        sides(dist, fn)

    def ab_second(k, dist):
        ra, rb = rows_of(k)[:2]

        def fn(zz, side):
            wait(region(0, 0, 0, cut(k, 0, 2 * AG_AB)), ag_h2.at[k, zz])
            push(region(zz, full, x, ra), k, ag_h3.at[k], xs)
            push(region(zz, y, full, rb), k, ag_h3.at[k], ys)

        sides(dist, fn)

    def cd_arrived(k, dist):
        rc, rd = rows_of(k)[2:]

        def fn(zz, side):
            if dist == 0:
                wait(region(0, 0, 0, cut(k, 0, 2 * AG_CD)), ag_cd1.at[k])
            else:
                wait(pb.at[0, 0, full, full, rc], ag_cd.at[k, side, dist - 1])

            def on(way, to):
                push(region(zz, full, x, rc), k, ag_cd.at[k, way, dist], to)
                push(region(zz, y, full, rd), k, ag_cd.at[k, way, dist], to)

            onward_z(side, dist, on)
            push(region(zz, full, x, rc), k, ag_h3.at[k], xs)
            push(region(zz, y, full, rd), k, ag_h3.at[k], ys)

        sides(dist, fn)

    def ag0(k):
        def upd(b, carry):
            rows = pl.ds(pl.multiple_of(k * AG_ROWS + b * 48, 16), 48)
            new = adam_update(gsum[rows] * clip[0:1], po[rows], mo[rows], vo[rows], rate, WEIGHT_DECAY)
            po[rows], mo[rows], vo[rows] = new
            pb[z, y, x, c, rows] = new[0].astype(BF16)
            return carry
        lax.fori_loop(0, AG_ROWS // 48, upd, 0)
        rc, rd = rows_of(k)[2:]
        push(region(z, y, x, rc), k, ag_cd1.at[k], ys)
        push(region(z, y, x, rd), k, ag_cd1.at[k], xs)
        ab_arrived(k, 0)

    def middle(s):
        def fn(k):
            cd_arrived(k, s - 1)
            if s <= 3:
                ab_arrived(k, s)
            ab_second(k, s - 1)
        return fn

    def ag5(k):
        wait(pb.at[0, full, full, full, cut(k, 0, AG_ROWS)], ag_h3.at[k])
        push(region(full, full, full, cut(k, 0, AG_ROWS)), k, ag_d2d.at[k], partner)

    def ag_iter(i, carry):
        for s, fn in zip(AG_STAGES, (ag0, middle(1), middle(2), middle(3), middle(4), ag5)):
            k = i - s

            @pl.when((k >= 0) & (k < AG_CHUNKS))
            def _(fn=fn, k=k):
                fn(k)
        return carry

    lax.fori_loop(0, AG_CHUNKS + AG_STAGES[-1], ag_iter, 0)

    newv = adam_update(gvec * clip[0:1], pvo[...], mvo[...], vvo[...], rate, 0.0)
    pvo[...], mvo[...], vvo[...] = newv

    def drain_rs(k, carry):
        wait(gsum.at[pl.ds(0, 14 * HALF)], rs_send.at[k])
        return carry

    def drain_ag(k, carry):
        wait(pb.at[full, full, full, 0, cut(k, 0, AG_ROWS)], ag_d2d.at[k])
        base, along = 24 * AG_AB + 18 * AG_CD + 16 * AG_ROWS, 2 * AG_AB + 4 * AG_CD

        @pl.when(mid)
        def _():
            wait(pb.at[0, 0, full, full, pl.ds(0, (base + 5 * along) // 4)], ag_send.at[k])

        @pl.when(jnp.logical_not(mid))
        def _():
            wait(pb.at[0, 0, full, full, pl.ds(0, (base + along) // 4)], ag_send.at[k])

        return carry

    lax.fori_loop(0, CHUNKS, drain_rs, 0)
    lax.fori_loop(0, AG_CHUNKS, drain_ag, 0)
    for s in range(4):
        wait(dense.at[s, :, pl.ds(1, 3)], s0_send.at[s])
    for j in range(5):
        wait(vs.at[j], vec_send.at[j])
    wait(nr.at[pl.ds(0, DP - 1)], norm_send)


def finish(*refs):
    srcs, dsts, sem = refs[:7], refs[7:14], refs[14]
    copies = [pltpu.make_async_copy(srcs[6].at[zz, yy], dsts[6].at[zz, yy], sem.at[6 + zz * 2 + yy]) for zz in range(4) for yy in range(2)]
    copies += [pltpu.make_async_copy(srcs[i], dsts[i], sem.at[i]) for i in range(6)]
    for copy in copies:
        copy.start()
    for copy in copies:
        copy.wait()


def solution(mesh):
    axis_name = mesh.axis_names[0]
    vm = pl.BlockSpec(memory_space=pltpu.VMEM)
    hbm = pl.BlockSpec(memory_space=pl.ANY)
    dma = pltpu.SemaphoreType.DMA
    K, G = CHUNKS, AG_CHUNKS

    call = pl.pallas_call(
        kernel,
        name="adam_step",
        out_shape=(
            [pltpu.VMEM((PIECE, 128), F32)] * 3
            + [pltpu.VMEM((VEC, 128), F32)] * 3
            + [pltpu.VMEM((4, 2, 2, 2, PIECE, 128), BF16)]
        ),
        in_specs=[hbm] * 8 + [pl.BlockSpec(memory_space=pltpu.SMEM)],
        out_specs=[vm] * 7,
        scratch_shapes=[
            pltpu.VMEM((1, VEC * 128), BF16),
            pltpu.VMEM((2, DP, 1, ROWS * 128), BF16),
            pltpu.VMEM((4, 2, 4, 8 * HALF, 128), BF16),
            pltpu.VMEM((K, 2, 2, 4, RAB, 128), F32),
            pltpu.VMEM((K, 2, 4, 2, RCD, 128), F32),
            pltpu.VMEM((K, 4, 2, RAB, 128), F32),
            pltpu.VMEM((K, 2, 4, RAB, 128), F32),
            pltpu.VMEM((K, 2, 5, 2, RCD, 128), F32),
            pltpu.VMEM((K, 5, 2, RAB, 128), F32),
            pltpu.VMEM((K, 2, RCD, 128), F32),
            pltpu.VMEM((PIECE, 128), F32),
            pltpu.VMEM((8, 128), F32),
            pltpu.VMEM((8, 128), F32),
            pltpu.VMEM((6, VPAD, 128), F32),
            pltpu.VMEM((5, VPAD, 128), F32),
            pltpu.VMEM((1, 128), F32),
            pltpu.VMEM((DP, 1, 128), F32),
            dma((2,)), dma((7,)), dma((4,)), dma((SLOTS,)), dma((K,)), dma((SLOTS,)), dma((SLOTS, 2, 2)), dma((SLOTS, 2)), dma((SLOTS,)),
            dma((5,)), dma((5,)), dma, dma,
            dma((G,)), dma((G, 2, 3)), dma((G, 2, 3)), dma((G,)), dma((G, 4)), dma((G,)), dma((G,)),
        ],
        compiler_params=pltpu.CompilerParams(
            collective_id=0, has_side_effects=True, vmem_limit_bytes=37 * 2 ** 20
        ),
    )

    shapes = [(PIECE, 128)] * 3 + [(VEC, 128)] * 3
    copy_out = pl.pallas_call(
        finish,
        name="copy_out",
        out_shape=[jax.ShapeDtypeStruct(s, F32) for s in shapes] + [jax.ShapeDtypeStruct((4, 2, 2, 2, PIECE, 128), BF16)],
        in_specs=[vm] * 7,
        out_specs=[hbm] * 7,
        scratch_shapes=[dma((14,))],
        compiler_params=pltpu.CompilerParams(vmem_limit_bytes=2 ** 20),
    )

    def local_step(g_mat, g_vec, p_mat, m_mat, v_mat, p_vec, m_vec, v_vec, learn_rate):
        outs = call(
            g_mat, g_vec,
            p_mat.reshape(PIECE, 128), m_mat.reshape(PIECE, 128), v_mat.reshape(PIECE, 128),
            p_vec.reshape(VEC, 128), m_vec.reshape(VEC, 128), v_vec.reshape(VEC, 128),
            learn_rate.reshape(1, 1),
        )
        return tuple(o.reshape(-1) for o in copy_out(*outs))

    return jax.shard_map(
        local_step,
        mesh=mesh,
        in_specs=(P(axis_name, None), P(axis_name, None), P(axis_name), P(axis_name), P(axis_name), P(), P(), P(), P()),
        out_specs=(P(axis_name), P(axis_name), P(axis_name), P(), P(), P(), P()),
        check_vma=False,
    )
```

```python
import jax
import jax.numpy as jnp
from jax import lax
from jax.experimental import pallas as pl
from jax.experimental.pallas import tpu as pltpu
from jax.sharding import PartitionSpec as P

STEP = 10
ADAM_BETA1 = 0.9
ADAM_BETA2 = 0.98
ADAM_EPS = 1e-8
WEIGHT_DECAY = 0.01
MAX_NORM = 1.0
NORM_EPS = 1e-6
BIAS_ONE = 1.0 - ADAM_BETA1 ** STEP
BIAS_TWO = 1.0 - ADAM_BETA2 ** STEP

DP = 32
AG_CHUNKS = 10
AG_ROWS = 240
AG_AB = 48
AG_CD = 72
PIECE = 2400
CHUNKS = 50
ROWS = PIECE // CHUNKS
HALF = ROWS // 2
RAB = 8
RCD = HALF - RAB
SKEW_RS = 2
AG_STAGES = (0, 2, 3, 4, 5, 6)
SLOTS = 16
VEC = 130
VPAD = 136
MESH = pl.DeviceIdType.MESH
F32 = jnp.float32
BF16 = jnp.bfloat16


def adam_update(grad_vals, param_vals, moment_one, moment_two, learn_rate, decay_rate):
    new_one = ADAM_BETA1 * moment_one + (1.0 - ADAM_BETA1) * grad_vals
    new_two = ADAM_BETA2 * moment_two + (1.0 - ADAM_BETA2) * grad_vals * grad_vals
    direction = (new_one / BIAS_ONE) / (jnp.sqrt(new_two / BIAS_TWO) + ADAM_EPS)
    return param_vals - learn_rate * (direction + decay_rate * param_vals), new_one, new_two


def kernel(g, gv, p, m, v, pv, mv, vv, lr,
           po, mo, vo, pvo, mvo, vvo, pb,
           gvb, stage, dense, pab, pcd, abz, er, cdr, abr, fr, gsum, ssq, clip, vs, vr, ns, nr,
           in_sem, pmv_sem, s0_send, s0_recv, rs_send, er_recv, cd_recv, ab_recv, f_recv,
           vec_send, vec_recv, norm_send, norm_recv,
           ag_send, ag_ab, ag_cd, ag_cd1, ag_h2, ag_h3, ag_d2d):
    me = lax.axis_index("dp")
    c = me % 2
    x = (me // 2) % 2
    y = (me // 4) % 2
    z = me // 8

    def dev(zz, yy, xx, cc):
        return ((zz * 2 + yy) * 2 + xx) * 2 + cc

    partner = dev(z, y, x, 1 - c)
    xs = dev(z, y, 1 - x, c)
    xo = dev(z, y, 1 - x, 1 - c)
    ys = dev(z, 1 - y, x, c)
    yo = dev(z, 1 - y, x, 1 - c)
    up = dev((z + 1) % 4, y, x, c)
    down = dev((z + 3) % 4, y, x, c)
    z1 = dev(z + 1 - 2 * (z % 2), y, x, c)
    z2 = dev((z + 2) % 4, y, x, c)
    nlow = z >= 1
    nhigh = z <= 2

    def send(src, dst, ssem, rsem, to):
        pltpu.make_async_remote_copy(
            src_ref=src, dst_ref=dst, send_sem=ssem, recv_sem=rsem, device_id=(to,), device_id_type=MESH
        ).start()

    def wait(ref, sem):
        pltpu.make_async_copy(ref, ref, sem).wait()

    def fetch(k, slot):
        def one(d, carry):
            off = pl.multiple_of((d * PIECE + k * ROWS) * 128, 1024)
            pltpu.make_async_copy(g.at[0:1, pl.ds(off, ROWS * 128)], stage.at[slot, d], in_sem.at[slot]).start()
            return carry
        lax.fori_loop(0, DP, one, 0)

    barrier = pltpu.get_barrier_semaphore()
    for nb in (partner, xs, xo, ys, yo, z2):
        pl.semaphore_signal(barrier, inc=1, device_id=(nb,), device_id_type=MESH)

    @pl.when(nhigh)
    def _():
        pl.semaphore_signal(barrier, inc=1, device_id=(up,), device_id_type=MESH)

    @pl.when(nlow)
    def _():
        pl.semaphore_signal(barrier, inc=1, device_id=(down,), device_id_type=MESH)

    fetch(0, 0)
    ssq[...] = jnp.zeros((8, 128), F32)

    mid = (z >= 1) & (z <= 2)

    def await_neighbours():
        @pl.when(mid)
        def _():
            pl.semaphore_wait(barrier, 8)

        @pl.when(jnp.logical_not(mid))
        def _():
            pl.semaphore_wait(barrier, 7)

    partners = (partner, xs, ys, z1, z2)

    loads = ((gv, gvb), (p, po), (m, mo), (v, vo), (pv, pvo), (mv, mvo), (vv, vvo))

    def vec_step(j):
        if j == 0:
            for i, (src, dst) in enumerate(loads):
                pltpu.make_async_copy(src, dst, pmv_sem.at[i]).start()
            wait(gvb, pmv_sem.at[0])
            vs[0, 0:128] = gvb[0:1, 0:16384].astype(F32).reshape(128, 128)
            vs[0, 128:VPAD] = jnp.zeros((VPAD - 128, 128), F32)
            vs[0, 128:VEC] = gvb[0:1, 16384:16640].astype(F32).reshape(2, 128)
        else:
            wait(vr.at[j - 1], vec_recv.at[j - 1])
            vs[j] = vs[j - 1] + vr[j - 1]
        if j < 5:
            send(vs.at[j], vr.at[j], vec_send.at[j], vec_recv.at[j], partners[j])

    per = PIECE // (24 * HALF)

    def rpiece(k, d):
        at = (2 * k + d) // per
        return at // 8, (at // 4) % 2, (at // 2) % 2, at % 2

    def roff(k, d):
        return ((2 * k + d) % per) * 24 * HALF

    def rbuf(k, d, j):
        return pb.at[(*rpiece(k, d), pl.ds(roff(k, d) + j * 8 * HALF, 8 * HALF))]

    def convert(k):
        slot = k % 2
        dslot = k % 4

        @pl.when(k >= 4)
        def _():
            wait(dense.at[dslot, :, pl.ds(1, 3)], s0_send.at[dslot])

        wait(stage.at[slot], in_sem.at[slot])

        def conv(b, carry):
            row = pl.multiple_of(b * 2 * HALF, 16)
            for d in range(2):
                for q in range(4):
                    cc = 1 - c if q % 2 else c
                    vals = []
                    for o in range(2):
                        if d == 0:
                            piece = dev(b, o, 1 - x if q >= 2 else x, cc)
                        else:
                            piece = dev(b, 1 - y if q >= 2 else y, o, cc)
                        flat = stage[slot, piece, 0:1, d * HALF * 128:(d + 1) * HALF * 128].astype(F32)
                        vals.append(flat.reshape(HALF, 128))
                    dense[dslot, d, q, pl.ds(row, 2 * HALF)] = jnp.concatenate(vals, axis=0).astype(BF16)
            return carry

        lax.fori_loop(0, 4, conv, 0)

        @pl.when(k + 1 < CHUNKS)
        def _():
            fetch(k + 1, 1 - slot)

    def stage0(k):
        dslot = k % 4
        for q in (3, 2, 1):
            for d in range(2):
                to = ((partner, xs, xo), (partner, ys, yo))[d][q - 1]
                send(dense.at[dslot, d, q], rbuf(k, d, q - 1), s0_send.at[dslot], s0_recv.at[k % SLOTS], to)

        @pl.when(k + 1 < CHUNKS)
        def _():
            convert(k + 1)

    def z_first(k, bufs, recv, rsem):
        @pl.when(z == 0)
        def _():
            send(bufs.at[pl.ds(1, 3)], recv.at[pl.ds(0, 3)], rs_send.at[k], rsem.at[0], up)

        @pl.when(z == 3)
        def _():
            send(bufs.at[pl.ds(0, 3)], recv.at[pl.ds(0, 3)], rs_send.at[k], rsem.at[0], down)

    def z_second(k, bufs, recv, rsem):
        @pl.when(z == 1)
        def _():
            wait(recv.at[pl.ds(0, 3)], rsem.at[0])
            bufs[1:4] += recv[0:3]
            send(bufs.at[pl.ds(2, 2)], recv.at[pl.ds(3, 2)], rs_send.at[k], rsem.at[1], up)

        @pl.when(z == 2)
        def _():
            wait(recv.at[pl.ds(0, 3)], rsem.at[0])
            bufs[0:3] += recv[0:3]
            send(bufs.at[pl.ds(0, 2)], recv.at[pl.ds(3, 2)], rs_send.at[k], rsem.at[1], down)

    def z_third(k, bufs, recv, rsem):
        @pl.when(z == 1)
        def _():
            wait(recv.at[pl.ds(3, 2)], rsem.at[1])
            bufs[0:2] += recv[3:5]
            send(bufs.at[0], recv.at[0], rs_send.at[k], rsem.at[0], down)

        @pl.when(z == 2)
        def _():
            wait(recv.at[pl.ds(3, 2)], rsem.at[1])
            bufs[2:4] += recv[3:5]
            send(bufs.at[3], recv.at[0], rs_send.at[k], rsem.at[0], up)

    def z_final(k, bufs, recv, rsem):
        @pl.when(jnp.logical_not(mid))
        def _():
            wait(recv.at[0], rsem.at[0])
            bufs[z] += recv[0]

    def stage1(k):
        dslot = k % 4
        wait(dense.at[dslot, :, pl.ds(1, 3)], s0_recv.at[k % SLOTS])
        for d in range(2):
            def add(b, carry, d=d):
                row = pl.multiple_of(b * 2 * HALF, 16)
                tot = dense[dslot, d, 0, pl.ds(row, 2 * HALF)].astype(F32)
                for j in range(3):
                    off = pl.multiple_of(roff(k, d) + j * 8 * HALF + b * 2 * HALF, 16)
                    tot = tot + pb[(*rpiece(k, d), pl.ds(off, 2 * HALF))].astype(F32)
                for o in range(2):
                    pab[k, d, o, b] = tot[o * HALF:o * HALF + RAB]
                    pcd[k, d, b, o] = tot[o * HALF + RAB:(o + 1) * HALF]
                return carry
            lax.fori_loop(0, 4, add, 0)
        send(pab.at[k, 0, 1 - y], er.at[k, 0], rs_send.at[k], er_recv.at[k % SLOTS], ys)
        send(pab.at[k, 1, 1 - x], er.at[k, 1], rs_send.at[k], er_recv.at[k % SLOTS], xs)
        for d in range(2):
            z_first(k, pcd.at[k, d], cdr.at[k, d], cd_recv.at[k % SLOTS, d])

    def stage2(k):
        for d in range(2):
            z_second(k, pcd.at[k, d], cdr.at[k, d], cd_recv.at[k % SLOTS, d])
        wait(er.at[k], er_recv.at[k % SLOTS])
        for zz in range(4):
            abz[k, zz, 0] = pab[k, 0, y, zz] + er[k, 0, zz]
            abz[k, zz, 1] = pab[k, 1, x, zz] + er[k, 1, zz]
        z_first(k, abz.at[k], abr.at[k], ab_recv.at[k % SLOTS])

    def stage3(k):
        for d in range(2):
            z_third(k, pcd.at[k, d], cdr.at[k, d], cd_recv.at[k % SLOTS, d])
        z_second(k, abz.at[k], abr.at[k], ab_recv.at[k % SLOTS])

    def stage4(k):
        for d in range(2):
            z_final(k, pcd.at[k, d], cdr.at[k, d], cd_recv.at[k % SLOTS, d])
        send(pcd.at[k, 0, z, 1 - y], fr.at[k, 0], rs_send.at[k], f_recv.at[k % SLOTS], ys)
        send(pcd.at[k, 1, z, 1 - x], fr.at[k, 1], rs_send.at[k], f_recv.at[k % SLOTS], xs)
        z_third(k, abz.at[k], abr.at[k], ab_recv.at[k % SLOTS])

    def stage5(k):
        z_final(k, abz.at[k], abr.at[k], ab_recv.at[k % SLOTS])
        wait(fr.at[k], f_recv.at[k % SLOTS])
        base = pl.multiple_of(k * ROWS, 16)
        parts = (
            (0, RAB, abz[k, z, 0]),
            (RAB, RCD, pcd[k, 0, z, y] + fr[k, 0]),
            (HALF, RAB, abz[k, z, 1]),
            (HALF + RAB, RCD, pcd[k, 1, z, x] + fr[k, 1]),
        )
        acc = ssq[...]
        for off, num, val in parts:
            val = val * (1.0 / DP)
            gsum[pl.ds(base + off, num)] = val
            acc = acc + jnp.sum((val * val).reshape(num // 8, 8, 128), axis=0)
        ssq[...] = acc

    def rs_iter(i, carry):
        for s, fn in enumerate((stage0, stage1, stage2, stage3, stage4, stage5)):
            k = i - SKEW_RS * s

            @pl.when((k >= 0) & (k < CHUNKS))
            def _(fn=fn, k=k):
                fn(k)
        for j in range(6):
            @pl.when(i == 4 + 4 * j)
            def _(j=j):
                vec_step(j)
        return carry

    convert(0)
    await_neighbours()
    lax.fori_loop(0, CHUNKS + 5 * SKEW_RS, rs_iter, 0)

    ns[...] = jnp.sum(ssq[...], axis=0, keepdims=True)
    nr[me] = ns[...]

    def tell(j, carry):
        send(ns, nr.at[me], norm_send, norm_recv, (me + j) % DP)
        return carry

    lax.fori_loop(1, DP, tell, 0)
    wait(nr.at[pl.ds(0, DP - 1)], norm_recv)
    gvec = vs[5, 0:VEC] * (1.0 / DP)
    norm_sq = jnp.full((8, 128), jnp.sum(nr[...]) + jnp.sum(gvec * gvec))
    clip[...] = jnp.minimum(1.0, MAX_NORM / (jnp.sqrt(norm_sq) + NORM_EPS))
    rate = lr[0, 0]

    for i, (_, dst) in enumerate(loads[1:]):
        wait(dst, pmv_sem.at[i + 1])

    def cut(k, off, num):
        return pl.ds(pl.multiple_of(k * AG_ROWS + off, 8), num)

    def rows_of(k):
        return (cut(k, 0, AG_AB), cut(k, AG_AB, AG_AB), cut(k, 2 * AG_AB, AG_CD), cut(k, 2 * AG_AB + AG_CD, AG_CD))

    full = slice(None)

    def region(zz, yy, xx, rows):
        return pb.at[zz, yy, xx, c, rows]

    def push(ref, k, rsem, to):
        send(ref, ref, ag_send.at[k], rsem, to)

    def sides(dist, fn):
        if dist == 0:
            fn(z, None)
            return

        @pl.when(z - dist >= 0)
        def _():
            fn(z - dist, 0)

        @pl.when(z + dist <= 3)
        def _():
            fn(z + dist, 1)

    def along_z(fn):
        @pl.when(nhigh)
        def _():
            fn(0, up)

        @pl.when(nlow)
        def _():
            fn(1, down)

    def onward_z(side, dist, fn):
        if dist == 0:
            along_z(fn)
        elif dist < 3 and side == 0:
            @pl.when(nhigh)
            def _():
                fn(0, up)
        elif dist < 3:
            @pl.when(nlow)
            def _():
                fn(1, down)

    def ab_arrived(k, dist):
        ra, rb = rows_of(k)[:2]
        ab = cut(k, 0, 2 * AG_AB)

        def fn(zz, side):
            if dist:
                wait(region(0, 0, 0, ab), ag_ab.at[k, side, dist - 1])
            onward_z(side, dist, lambda way, to: push(region(zz, y, x, ab), k, ag_ab.at[k, way, dist], to))
            push(region(zz, y, x, ra), k, ag_h2.at[k, zz], ys)
            push(region(zz, y, x, rb), k, ag_h2.at[k, zz], xs)

        sides(dist, fn)

    def ab_second(k, dist):
        ra, rb = rows_of(k)[:2]

        def fn(zz, side):
            wait(region(0, 0, 0, cut(k, 0, 2 * AG_AB)), ag_h2.at[k, zz])
            push(region(zz, full, x, ra), k, ag_h3.at[k], xs)
            push(region(zz, y, full, rb), k, ag_h3.at[k], ys)

        sides(dist, fn)

    def cd_arrived(k, dist):
        rc, rd = rows_of(k)[2:]

        def fn(zz, side):
            if dist == 0:
                wait(region(0, 0, 0, cut(k, 0, 2 * AG_CD)), ag_cd1.at[k])
            else:
                wait(pb.at[0, 0, full, full, rc], ag_cd.at[k, side, dist - 1])

            def on(way, to):
                push(region(zz, full, x, rc), k, ag_cd.at[k, way, dist], to)
                push(region(zz, y, full, rd), k, ag_cd.at[k, way, dist], to)

            onward_z(side, dist, on)
            push(region(zz, full, x, rc), k, ag_h3.at[k], xs)
            push(region(zz, y, full, rd), k, ag_h3.at[k], ys)

        sides(dist, fn)

    def ag0(k):
        def upd(b, carry):
            rows = pl.ds(pl.multiple_of(k * AG_ROWS + b * 48, 16), 48)
            new = adam_update(gsum[rows] * clip[0:1], po[rows], mo[rows], vo[rows], rate, WEIGHT_DECAY)
            po[rows], mo[rows], vo[rows] = new
            pb[z, y, x, c, rows] = new[0].astype(BF16)
            return carry
        lax.fori_loop(0, AG_ROWS // 48, upd, 0)
        rc, rd = rows_of(k)[2:]
        push(region(z, y, x, rc), k, ag_cd1.at[k], ys)
        push(region(z, y, x, rd), k, ag_cd1.at[k], xs)
        ab_arrived(k, 0)

    def middle(s):
        def fn(k):
            cd_arrived(k, s - 1)
            if s <= 3:
                ab_arrived(k, s)
            ab_second(k, s - 1)
        return fn

    def ag5(k):
        ra, rb, rc, rd = rows_of(k)
        for xx, yy in ((x, y), (1 - x, 1 - y)):
            if xx is not x:
                wait(pb.at[0, full, full, full, cut(k, 0, AG_ROWS)], ag_h3.at[k])
            push(region(full, full, xx, ra), k, ag_d2d.at[k], partner)
            push(region(full, yy, full, rb), k, ag_d2d.at[k], partner)
            push(region(full, full, xx, rc), k, ag_d2d.at[k], partner)
            push(region(full, yy, full, rd), k, ag_d2d.at[k], partner)

    def ag_iter(i, carry):
        for s, fn in zip(AG_STAGES, (ag0, middle(1), middle(2), middle(3), middle(4), ag5)):
            k = i - s

            @pl.when((k >= 0) & (k < AG_CHUNKS))
            def _(fn=fn, k=k):
                fn(k)
        return carry

    lax.fori_loop(0, AG_CHUNKS + AG_STAGES[-1], ag_iter, 0)

    newv = adam_update(gvec * clip[0:1], pvo[...], mvo[...], vvo[...], rate, 0.0)
    pvo[...], mvo[...], vvo[...] = newv

    def drain_rs(k, carry):
        wait(gsum.at[pl.ds(0, 14 * HALF)], rs_send.at[k])
        return carry

    def drain_ag(k, carry):
        wait(pb.at[full, full, full, 0, cut(k, 0, AG_ROWS)], ag_d2d.at[k])
        base, along = 24 * AG_AB + 18 * AG_CD + 16 * AG_ROWS, 2 * AG_AB + 4 * AG_CD

        @pl.when(mid)
        def _():
            wait(pb.at[0, 0, full, full, pl.ds(0, (base + 5 * along) // 4)], ag_send.at[k])

        @pl.when(jnp.logical_not(mid))
        def _():
            wait(pb.at[0, 0, full, full, pl.ds(0, (base + along) // 4)], ag_send.at[k])

        return carry

    lax.fori_loop(0, CHUNKS, drain_rs, 0)
    lax.fori_loop(0, AG_CHUNKS, drain_ag, 0)
    for s in range(4):
        wait(dense.at[s, :, pl.ds(1, 3)], s0_send.at[s])
    for j in range(5):
        wait(vs.at[j], vec_send.at[j])
    wait(nr.at[pl.ds(0, DP - 1)], norm_send)


def finish(*refs):
    srcs, dsts, sem = refs[:7], refs[7:14], refs[14]
    copies = [
        pltpu.make_async_copy(srcs[6].at[i // 4, i // 2 % 2, i % 2], dsts[6].at[i // 4, i // 2 % 2, i % 2], sem.at[6 + i])
        for i in range(16)
    ]
    copies += [pltpu.make_async_copy(srcs[i], dsts[i], sem.at[i]) for i in range(6)]
    for copy in copies:
        copy.start()
    for copy in copies:
        copy.wait()


def solution(mesh):
    axis_name = mesh.axis_names[0]
    vm = pl.BlockSpec(memory_space=pltpu.VMEM)
    hbm = pl.BlockSpec(memory_space=pl.ANY)
    dma = pltpu.SemaphoreType.DMA
    K, G = CHUNKS, AG_CHUNKS

    call = pl.pallas_call(
        kernel,
        name="adam_step",
        out_shape=(
            [pltpu.VMEM((PIECE, 128), F32)] * 3
            + [pltpu.VMEM((VEC, 128), F32)] * 3
            + [pltpu.VMEM((4, 2, 2, 2, PIECE, 128), BF16)]
        ),
        in_specs=[hbm] * 8 + [pl.BlockSpec(memory_space=pltpu.SMEM)],
        out_specs=[vm] * 7,
        scratch_shapes=[
            pltpu.VMEM((1, VEC * 128), BF16),
            pltpu.VMEM((2, DP, 1, ROWS * 128), BF16),
            pltpu.VMEM((4, 2, 4, 8 * HALF, 128), BF16),
            pltpu.VMEM((K, 2, 2, 4, RAB, 128), F32),
            pltpu.VMEM((K, 2, 4, 2, RCD, 128), F32),
            pltpu.VMEM((K, 4, 2, RAB, 128), F32),
            pltpu.VMEM((K, 2, 4, RAB, 128), F32),
            pltpu.VMEM((K, 2, 5, 2, RCD, 128), F32),
            pltpu.VMEM((K, 5, 2, RAB, 128), F32),
            pltpu.VMEM((K, 2, RCD, 128), F32),
            pltpu.VMEM((PIECE, 128), F32),
            pltpu.VMEM((8, 128), F32),
            pltpu.VMEM((8, 128), F32),
            pltpu.VMEM((6, VPAD, 128), F32),
            pltpu.VMEM((5, VPAD, 128), F32),
            pltpu.VMEM((1, 128), F32),
            pltpu.VMEM((DP, 1, 128), F32),
            dma((2,)), dma((7,)), dma((4,)), dma((SLOTS,)), dma((K,)), dma((SLOTS,)), dma((SLOTS, 2, 2)), dma((SLOTS, 2)), dma((SLOTS,)),
            dma((5,)), dma((5,)), dma, dma,
            dma((G,)), dma((G, 2, 3)), dma((G, 2, 3)), dma((G,)), dma((G, 4)), dma((G,)), dma((G,)),
        ],
        compiler_params=pltpu.CompilerParams(
            collective_id=0, has_side_effects=True, vmem_limit_bytes=37 * 2 ** 20
        ),
    )

    shapes = [(PIECE, 128)] * 3 + [(VEC, 128)] * 3
    copy_out = pl.pallas_call(
        finish,
        name="copy_out",
        out_shape=[jax.ShapeDtypeStruct(s, F32) for s in shapes] + [jax.ShapeDtypeStruct((4, 2, 2, 2, PIECE, 128), BF16)],
        in_specs=[vm] * 7,
        out_specs=[hbm] * 7,
        scratch_shapes=[dma((22,))],
        compiler_params=pltpu.CompilerParams(vmem_limit_bytes=2 ** 20),
    )

    def local_step(g_mat, g_vec, p_mat, m_mat, v_mat, p_vec, m_vec, v_vec, learn_rate):
        outs = call(
            g_mat, g_vec,
            p_mat.reshape(PIECE, 128), m_mat.reshape(PIECE, 128), v_mat.reshape(PIECE, 128),
            p_vec.reshape(VEC, 128), m_vec.reshape(VEC, 128), v_vec.reshape(VEC, 128),
            learn_rate.reshape(1, 1),
        )
        return tuple(o.reshape(-1) for o in copy_out(*outs))

    return jax.shard_map(
        local_step,
        mesh=mesh,
        in_specs=(P(axis_name, None), P(axis_name, None), P(axis_name), P(axis_name), P(axis_name), P(), P(), P(), P()),
        out_specs=(P(axis_name), P(axis_name), P(axis_name), P(), P(), P(), P()),
        check_vma=False,
    )
```

```python
import jax
import jax.numpy as jnp
from jax import lax
from jax.experimental import pallas as pl
from jax.experimental.pallas import tpu as pltpu
from jax.sharding import PartitionSpec as P

STEP = 10
ADAM_BETA1 = 0.9
ADAM_BETA2 = 0.98
ADAM_EPS = 1e-8
WEIGHT_DECAY = 0.01
MAX_NORM = 1.0
NORM_EPS = 1e-6
BIAS_ONE = 1.0 - ADAM_BETA1 ** STEP
BIAS_TWO = 1.0 - ADAM_BETA2 ** STEP

DP = 32
AG_CHUNKS = 10
AG_ROWS = 240
AG_AB = 48
AG_CD = 72
PIECE = 2400
CHUNKS = 50
ROWS = PIECE // CHUNKS
HALF = ROWS // 2
RAB = 8
RCD = HALF - RAB
SKEW_RS = 2
AG_STAGES = (0, 2, 3, 4, 5, 6)
SLOTS = 12
VEC = 130
VPAD = 136
MESH = pl.DeviceIdType.MESH
F32 = jnp.float32
BF16 = jnp.bfloat16


def adam_update(grad_vals, param_vals, moment_one, moment_two, learn_rate, decay_rate):
    new_one = ADAM_BETA1 * moment_one + (1.0 - ADAM_BETA1) * grad_vals
    new_two = ADAM_BETA2 * moment_two + (1.0 - ADAM_BETA2) * grad_vals * grad_vals
    direction = (new_one / BIAS_ONE) / (jnp.sqrt(new_two / BIAS_TWO) + ADAM_EPS)
    return param_vals - learn_rate * (direction + decay_rate * param_vals), new_one, new_two


def kernel(g, gv, p, m, v, pv, mv, vv, lr,
           po, mo, vo, pvo, mvo, vvo, pb,
           lrs, gvb, stage, dense, pab, pcd, abz, er, cdr, abr, fr, gsum, ssq, clip, vs, vr, ns, nr,
           in_sem, pmv_sem, s0_send, s0_recv, rs_send, er_recv, cd_recv, ab_recv, f_recv,
           vec_send, vec_recv, norm_send, norm_recv,
           ag_send, ag_ab, ag_cd, ag_cd1, ag_h2, ag_h3, ag_d2d):
    me = lax.axis_index("dp")
    c = me % 2
    x = (me // 2) % 2
    y = (me // 4) % 2
    z = me // 8

    def dev(zz, yy, xx, cc):
        return ((zz * 2 + yy) * 2 + xx) * 2 + cc

    partner = dev(z, y, x, 1 - c)
    xs = dev(z, y, 1 - x, c)
    xo = dev(z, y, 1 - x, 1 - c)
    ys = dev(z, 1 - y, x, c)
    yo = dev(z, 1 - y, x, 1 - c)
    up = dev((z + 1) % 4, y, x, c)
    down = dev((z + 3) % 4, y, x, c)
    z1 = dev(z + 1 - 2 * (z % 2), y, x, c)
    z2 = dev((z + 2) % 4, y, x, c)
    nlow = z >= 1
    nhigh = z <= 2

    def send(src, dst, ssem, rsem, to):
        pltpu.make_async_remote_copy(
            src_ref=src, dst_ref=dst, send_sem=ssem, recv_sem=rsem, device_id=(to,), device_id_type=MESH
        ).start()

    def wait(ref, sem):
        pltpu.make_async_copy(ref, ref, sem).wait()

    def fetch(k, slot):
        def one(d, carry):
            off = pl.multiple_of((d * PIECE + k * ROWS) * 128, 1024)
            pltpu.make_async_copy(g.at[0:1, pl.ds(off, ROWS * 128)], stage.at[slot, d], in_sem.at[slot]).start()
            return carry
        lax.fori_loop(0, DP, one, 0)

    barrier = pltpu.get_barrier_semaphore()
    for nb in (partner, xs, xo, ys, yo, z2):
        pl.semaphore_signal(barrier, inc=1, device_id=(nb,), device_id_type=MESH)

    @pl.when(nhigh)
    def _():
        pl.semaphore_signal(barrier, inc=1, device_id=(up,), device_id_type=MESH)

    @pl.when(nlow)
    def _():
        pl.semaphore_signal(barrier, inc=1, device_id=(down,), device_id_type=MESH)

    fetch(0, 0)
    ssq[...] = jnp.zeros((8, 128), F32)

    mid = (z >= 1) & (z <= 2)

    def await_neighbours():
        @pl.when(mid)
        def _():
            pl.semaphore_wait(barrier, 8)

        @pl.when(jnp.logical_not(mid))
        def _():
            pl.semaphore_wait(barrier, 7)

    partners = (partner, xs, ys, z1, z2)

    loads = ((gv, gvb), (p, po), (m, mo), (v, vo), (pv, pvo), (mv, mvo), (vv, vvo), (lr, lrs))

    def vec_step(j):
        if j == 0:
            for i, (src, dst) in enumerate(loads):
                pltpu.make_async_copy(src, dst, pmv_sem.at[i]).start()
            wait(gvb, pmv_sem.at[0])
            vs[0, 0:128] = gvb[0:1, 0:16384].astype(F32).reshape(128, 128)
            vs[0, 128:VPAD] = jnp.zeros((VPAD - 128, 128), F32)
            vs[0, 128:VEC] = gvb[0:1, 16384:16640].astype(F32).reshape(2, 128)
        else:
            wait(vr.at[j - 1], vec_recv.at[j - 1])
            vs[j] = vs[j - 1] + vr[j - 1]
        if j < 5:
            send(vs.at[j], vr.at[j], vec_send.at[j], vec_recv.at[j], partners[j])

    per = PIECE // (24 * HALF)

    def rpiece(k, d):
        at = (2 * k + d) // per
        return at // 8, (at // 4) % 2, (at // 2) % 2, at % 2

    def roff(k, d):
        return ((2 * k + d) % per) * 24 * HALF

    def rbuf(k, d, j):
        return pb.at[(*rpiece(k, d), pl.ds(roff(k, d) + j * 8 * HALF, 8 * HALF))]

    def convert(k):
        slot = k % 2
        dslot = k % 4

        @pl.when(k >= 4)
        def _():
            wait(dense.at[dslot, :, pl.ds(1, 3)], s0_send.at[dslot])

        wait(stage.at[slot], in_sem.at[slot])

        def conv(b, carry):
            row = pl.multiple_of(b * 2 * HALF, 16)
            for d in range(2):
                for q in range(4):
                    cc = 1 - c if q % 2 else c
                    vals = []
                    for o in range(2):
                        if d == 0:
                            piece = dev(b, o, 1 - x if q >= 2 else x, cc)
                        else:
                            piece = dev(b, 1 - y if q >= 2 else y, o, cc)
                        flat = stage[slot, piece, 0:1, d * HALF * 128:(d + 1) * HALF * 128].astype(F32)
                        vals.append(flat.reshape(HALF, 128))
                    dense[dslot, d, q, pl.ds(row, 2 * HALF)] = jnp.concatenate(vals, axis=0).astype(BF16)
            return carry

        lax.fori_loop(0, 4, conv, 0)

        @pl.when(k + 1 < CHUNKS)
        def _():
            fetch(k + 1, 1 - slot)

    def stage0(k):
        dslot = k % 4
        for q in (3, 2, 1):
            for d in range(2):
                to = ((partner, xs, xo), (partner, ys, yo))[d][q - 1]
                send(dense.at[dslot, d, q], rbuf(k, d, q - 1), s0_send.at[dslot], s0_recv.at[k % SLOTS], to)

        @pl.when(k + 1 < CHUNKS)
        def _():
            convert(k + 1)

    def z_first(k, bufs, recv, rsem):
        @pl.when(z == 0)
        def _():
            send(bufs.at[pl.ds(1, 3)], recv.at[pl.ds(0, 3)], rs_send.at[k], rsem.at[0], up)

        @pl.when(z == 3)
        def _():
            send(bufs.at[pl.ds(0, 3)], recv.at[pl.ds(0, 3)], rs_send.at[k], rsem.at[0], down)

    def z_second(k, bufs, recv, rsem):
        @pl.when(z == 1)
        def _():
            wait(recv.at[pl.ds(0, 3)], rsem.at[0])
            bufs[1:4] += recv[0:3]
            send(bufs.at[pl.ds(2, 2)], recv.at[pl.ds(3, 2)], rs_send.at[k], rsem.at[1], up)

        @pl.when(z == 2)
        def _():
            wait(recv.at[pl.ds(0, 3)], rsem.at[0])
            bufs[0:3] += recv[0:3]
            send(bufs.at[pl.ds(0, 2)], recv.at[pl.ds(3, 2)], rs_send.at[k], rsem.at[1], down)

    def z_third(k, bufs, recv, rsem):
        @pl.when(z == 1)
        def _():
            wait(recv.at[pl.ds(3, 2)], rsem.at[1])
            bufs[0:2] += recv[3:5]
            send(bufs.at[0], recv.at[0], rs_send.at[k], rsem.at[0], down)

        @pl.when(z == 2)
        def _():
            wait(recv.at[pl.ds(3, 2)], rsem.at[1])
            bufs[2:4] += recv[3:5]
            send(bufs.at[3], recv.at[0], rs_send.at[k], rsem.at[0], up)

    def z_final(k, bufs, recv, rsem):
        @pl.when(jnp.logical_not(mid))
        def _():
            wait(recv.at[0], rsem.at[0])
            bufs[z] += recv[0]

    def stage1(k):
        dslot = k % 4
        wait(dense.at[dslot, :, pl.ds(1, 3)], s0_recv.at[k % SLOTS])
        for d in range(2):
            def add(b, carry, d=d):
                row = pl.multiple_of(b * 2 * HALF, 16)
                tot = dense[dslot, d, 0, pl.ds(row, 2 * HALF)].astype(F32)
                for j in range(3):
                    off = pl.multiple_of(roff(k, d) + j * 8 * HALF + b * 2 * HALF, 16)
                    tot = tot + pb[(*rpiece(k, d), pl.ds(off, 2 * HALF))].astype(F32)
                for o in range(2):
                    pab[k, d, o, b] = tot[o * HALF:o * HALF + RAB]
                    pcd[k, d, b, o] = tot[o * HALF + RAB:(o + 1) * HALF]
                return carry
            lax.fori_loop(0, 4, add, 0)
        send(pab.at[k, 0, 1 - y], er.at[k, 0], rs_send.at[k], er_recv.at[k % SLOTS], ys)
        send(pab.at[k, 1, 1 - x], er.at[k, 1], rs_send.at[k], er_recv.at[k % SLOTS], xs)
        for d in range(2):
            z_first(k, pcd.at[k, d], cdr.at[k, d], cd_recv.at[k % SLOTS, d])

    def stage2(k):
        for d in range(2):
            z_second(k, pcd.at[k, d], cdr.at[k, d], cd_recv.at[k % SLOTS, d])
        wait(er.at[k], er_recv.at[k % SLOTS])
        for zz in range(4):
            abz[k, zz, 0] = pab[k, 0, y, zz] + er[k, 0, zz]
            abz[k, zz, 1] = pab[k, 1, x, zz] + er[k, 1, zz]
        z_first(k, abz.at[k], abr.at[k], ab_recv.at[k % SLOTS])

    def stage3(k):
        for d in range(2):
            z_third(k, pcd.at[k, d], cdr.at[k, d], cd_recv.at[k % SLOTS, d])
        z_second(k, abz.at[k], abr.at[k], ab_recv.at[k % SLOTS])

    def stage4(k):
        for d in range(2):
            z_final(k, pcd.at[k, d], cdr.at[k, d], cd_recv.at[k % SLOTS, d])
        send(pcd.at[k, 0, z, 1 - y], fr.at[k, 0], rs_send.at[k], f_recv.at[k % SLOTS], ys)
        send(pcd.at[k, 1, z, 1 - x], fr.at[k, 1], rs_send.at[k], f_recv.at[k % SLOTS], xs)
        z_third(k, abz.at[k], abr.at[k], ab_recv.at[k % SLOTS])

    def stage5(k):
        z_final(k, abz.at[k], abr.at[k], ab_recv.at[k % SLOTS])
        wait(fr.at[k], f_recv.at[k % SLOTS])
        base = pl.multiple_of(k * ROWS, 16)
        parts = (
            (0, RAB, abz[k, z, 0]),
            (RAB, RCD, pcd[k, 0, z, y] + fr[k, 0]),
            (HALF, RAB, abz[k, z, 1]),
            (HALF + RAB, RCD, pcd[k, 1, z, x] + fr[k, 1]),
        )
        acc = ssq[...]
        for off, num, val in parts:
            val = val * (1.0 / DP)
            gsum[pl.ds(base + off, num)] = val
            acc = acc + jnp.sum((val * val).reshape(num // 8, 8, 128), axis=0)
        ssq[...] = acc

    def rs_iter(i, carry):
        for s, fn in enumerate((stage0, stage1, stage2, stage3, stage4, stage5)):
            k = i - SKEW_RS * s

            @pl.when((k >= 0) & (k < CHUNKS))
            def _(fn=fn, k=k):
                fn(k)
        for j in range(6):
            @pl.when(i == 4 + 4 * j)
            def _(j=j):
                vec_step(j)
        return carry

    convert(0)
    await_neighbours()
    lax.fori_loop(0, CHUNKS + 5 * SKEW_RS, rs_iter, 0)

    for i, (src, dst) in enumerate(loads[1:]):
        pltpu.make_async_copy(src, dst, pmv_sem.at[i + 1]).wait()
    ns[...] = jnp.sum(ssq[...], axis=0, keepdims=True)
    nr[me] = ns[...]

    def tell(j, carry):
        send(ns, nr.at[me], norm_send, norm_recv, (me + j) % DP)
        return carry

    lax.fori_loop(1, DP, tell, 0)
    gvec = vs[5, 0:VEC] * (1.0 / DP)
    ssq[0:1] = jnp.sum(gvec * gvec, axis=0, keepdims=True)
    wait(nr.at[pl.ds(0, DP - 1)], norm_recv)
    norm_sq = jnp.full((8, 128), jnp.sum(jnp.sum(nr[...], axis=0) + ssq[0:1]))
    clip[...] = jnp.minimum(1.0, MAX_NORM / (jnp.sqrt(norm_sq) + NORM_EPS))

    rate = lrs[0, 0]

    def cut(k, off, num):
        return pl.ds(pl.multiple_of(k * AG_ROWS + off, 8), num)

    def rows_of(k):
        return (cut(k, 0, AG_AB), cut(k, AG_AB, AG_AB), cut(k, 2 * AG_AB, AG_CD), cut(k, 2 * AG_AB + AG_CD, AG_CD))

    full = slice(None)

    def region(zz, yy, xx, rows):
        return pb.at[zz, yy, xx, c, rows]

    def push(ref, k, rsem, to):
        send(ref, ref, ag_send.at[k], rsem, to)

    def sides(dist, fn):
        if dist == 0:
            fn(z, None)
            return

        @pl.when(z - dist >= 0)
        def _():
            fn(z - dist, 0)

        @pl.when(z + dist <= 3)
        def _():
            fn(z + dist, 1)

    def along_z(fn):
        @pl.when(nhigh)
        def _():
            fn(0, up)

        @pl.when(nlow)
        def _():
            fn(1, down)

    def onward_z(side, dist, fn):
        if dist == 0:
            along_z(fn)
        elif dist < 3 and side == 0:
            @pl.when(nhigh)
            def _():
                fn(0, up)
        elif dist < 3:
            @pl.when(nlow)
            def _():
                fn(1, down)

    def ab_arrived(k, dist):
        ra, rb = rows_of(k)[:2]
        ab = cut(k, 0, 2 * AG_AB)

        def fn(zz, side):
            if dist:
                wait(region(0, 0, 0, ab), ag_ab.at[k, zz])
            onward_z(side, dist, lambda way, to: push(region(zz, y, x, ab), k, ag_ab.at[k, zz], to))
            push(region(zz, y, x, ra), k, ag_h2.at[k, zz], ys)
            push(region(zz, y, x, rb), k, ag_h2.at[k, zz], xs)

        sides(dist, fn)

    def ab_second(k, dist):
        ra, rb = rows_of(k)[:2]

        def fn(zz, side):
            wait(region(0, 0, 0, cut(k, 0, 2 * AG_AB)), ag_h2.at[k, zz])
            push(region(zz, full, x, ra), k, ag_h3.at[k], xs)
            push(region(zz, y, full, rb), k, ag_h3.at[k], ys)

        sides(dist, fn)

    def cd_arrived(k, dist):
        rc, rd = rows_of(k)[2:]

        def fn(zz, side):
            if dist == 0:
                wait(region(0, 0, 0, cut(k, 0, 2 * AG_CD)), ag_cd1.at[k])
            else:
                wait(pb.at[0, 0, full, full, rc], ag_cd.at[k, zz])

            def on(way, to):
                push(region(zz, full, x, rc), k, ag_cd.at[k, zz], to)
                push(region(zz, y, full, rd), k, ag_cd.at[k, zz], to)

            onward_z(side, dist, on)
            push(region(zz, full, x, rc), k, ag_h3.at[k], xs)
            push(region(zz, y, full, rd), k, ag_h3.at[k], ys)

        sides(dist, fn)

    def ag0(k):
        def upd(b, carry):
            rows = pl.ds(pl.multiple_of(k * AG_ROWS + b * 48, 16), 48)
            new = adam_update(gsum[rows] * clip[0:1], po[rows], mo[rows], vo[rows], rate, WEIGHT_DECAY)
            po[rows], mo[rows], vo[rows] = new
            pb[z, y, x, c, rows] = new[0].astype(BF16)
            return carry
        lax.fori_loop(0, AG_ROWS // 48, upd, 0)
        rc, rd = rows_of(k)[2:]
        push(region(z, y, x, rc), k, ag_cd1.at[k], ys)
        push(region(z, y, x, rd), k, ag_cd1.at[k], xs)
        ab_arrived(k, 0)

    def middle(s):
        def fn(k):
            cd_arrived(k, s - 1)
            if s <= 3:
                ab_arrived(k, s)
            ab_second(k, s - 1)
        return fn

    def ag5(k):
        ra, rb, rc, rd = rows_of(k)
        for xx, yy in ((x, y), (1 - x, 1 - y)):
            if xx is not x:
                wait(pb.at[0, full, full, full, cut(k, 0, AG_ROWS)], ag_h3.at[k])
            push(region(full, full, xx, ra), k, ag_d2d.at[k], partner)
            push(region(full, yy, full, rb), k, ag_d2d.at[k], partner)
            push(region(full, full, xx, rc), k, ag_d2d.at[k], partner)
            push(region(full, yy, full, rd), k, ag_d2d.at[k], partner)

    def ag_iter(i, carry):
        for s, fn in zip(AG_STAGES, (ag0, middle(1), middle(2), middle(3), middle(4), ag5)):
            k = i - s

            @pl.when((k >= 0) & (k < AG_CHUNKS))
            def _(fn=fn, k=k):
                fn(k)
        return carry

    lax.fori_loop(0, AG_CHUNKS + AG_STAGES[-1], ag_iter, 0)

    newv = adam_update(gvec * clip[0:1], pvo[...], mvo[...], vvo[...], rate, 0.0)
    pvo[...], mvo[...], vvo[...] = newv

    def drain_rs(k, carry):
        wait(gsum.at[pl.ds(0, 14 * HALF)], rs_send.at[k])
        return carry

    def drain_ag(k, carry):
        wait(pb.at[full, full, full, 0, cut(k, 0, AG_ROWS)], ag_d2d.at[k])
        base, along = 24 * AG_AB + 18 * AG_CD + 16 * AG_ROWS, 2 * AG_AB + 4 * AG_CD

        @pl.when(mid)
        def _():
            wait(pb.at[0, 0, full, full, pl.ds(0, (base + 5 * along) // 4)], ag_send.at[k])

        @pl.when(jnp.logical_not(mid))
        def _():
            wait(pb.at[0, 0, full, full, pl.ds(0, (base + along) // 4)], ag_send.at[k])

        return carry

    lax.fori_loop(0, CHUNKS, drain_rs, 0)
    lax.fori_loop(0, AG_CHUNKS, drain_ag, 0)
    for s in range(4):
        wait(dense.at[s, :, pl.ds(1, 3)], s0_send.at[s])
    for j in range(5):
        wait(vs.at[j], vec_send.at[j])
    wait(nr.at[pl.ds(0, DP - 1)], norm_send)


def finish(*refs):
    srcs, dsts, sem = refs[:7], refs[7:14], refs[14]
    copies = [
        pltpu.make_async_copy(srcs[6].at[i // 4, i // 2 % 2, i % 2], dsts[6].at[i // 4, i // 2 % 2, i % 2], sem.at[6 + i])
        for i in range(16)
    ]
    copies += [pltpu.make_async_copy(srcs[i], dsts[i], sem.at[i]) for i in range(6)]
    for copy in copies:
        copy.start()
    for copy in copies:
        copy.wait()


def solution(mesh):
    axis_name = mesh.axis_names[0]
    vm = pl.BlockSpec(memory_space=pltpu.VMEM)
    hbm = pl.BlockSpec(memory_space=pl.ANY)
    dma = pltpu.SemaphoreType.DMA
    K, G = CHUNKS, AG_CHUNKS

    call = pl.pallas_call(
        kernel,
        name="adam_step",
        out_shape=(
            [pltpu.VMEM((PIECE, 128), F32)] * 3
            + [pltpu.VMEM((VEC, 128), F32)] * 3
            + [pltpu.VMEM((4, 2, 2, 2, PIECE, 128), BF16)]
        ),
        in_specs=[hbm] * 9,
        out_specs=[vm] * 7,
        scratch_shapes=[
            pltpu.SMEM((1, 1), F32),
            pltpu.VMEM((1, VEC * 128), BF16),
            pltpu.VMEM((2, DP, 1, ROWS * 128), BF16),
            pltpu.VMEM((4, 2, 4, 8 * HALF, 128), BF16),
            pltpu.VMEM((K, 2, 2, 4, RAB, 128), F32),
            pltpu.VMEM((K, 2, 4, 2, RCD, 128), F32),
            pltpu.VMEM((K, 4, 2, RAB, 128), F32),
            pltpu.VMEM((K, 2, 4, RAB, 128), F32),
            pltpu.VMEM((K, 2, 5, 2, RCD, 128), F32),
            pltpu.VMEM((K, 5, 2, RAB, 128), F32),
            pltpu.VMEM((K, 2, RCD, 128), F32),
            pltpu.VMEM((PIECE, 128), F32),
            pltpu.VMEM((8, 128), F32),
            pltpu.VMEM((8, 128), F32),
            pltpu.VMEM((6, VPAD, 128), F32),
            pltpu.VMEM((5, VPAD, 128), F32),
            pltpu.VMEM((1, 128), F32),
            pltpu.VMEM((DP, 1, 128), F32),
            dma((2,)), dma((8,)), dma((4,)), dma((SLOTS,)), dma((K,)), dma((SLOTS,)), dma((SLOTS, 2, 2)), dma((SLOTS, 2)), dma((SLOTS,)),
            dma((5,)), dma((5,)), dma, dma,
            dma((G,)), dma((G, 4)), dma((G, 4)), dma((G,)), dma((G, 4)), dma((G,)), dma((G,)),
        ],
        compiler_params=pltpu.CompilerParams(
            collective_id=0, has_side_effects=True, vmem_limit_bytes=37 * 2 ** 20
        ),
    )

    shapes = [(PIECE, 128)] * 3 + [(VEC, 128)] * 3
    copy_out = pl.pallas_call(
        finish,
        name="copy_out",
        out_shape=[jax.ShapeDtypeStruct(s, F32) for s in shapes] + [jax.ShapeDtypeStruct((4, 2, 2, 2, PIECE, 128), BF16)],
        in_specs=[vm] * 7,
        out_specs=[hbm] * 7,
        scratch_shapes=[dma((22,))],
        compiler_params=pltpu.CompilerParams(vmem_limit_bytes=2 ** 20),
    )

    def local_step(g_mat, g_vec, p_mat, m_mat, v_mat, p_vec, m_vec, v_vec, learn_rate):
        outs = call(
            g_mat, g_vec,
            p_mat.reshape(PIECE, 128), m_mat.reshape(PIECE, 128), v_mat.reshape(PIECE, 128),
            p_vec.reshape(VEC, 128), m_vec.reshape(VEC, 128), v_vec.reshape(VEC, 128),
            learn_rate.reshape(1, 1),
        )
        return tuple(o.reshape(-1) for o in copy_out(*outs))

    return jax.shard_map(
        local_step,
        mesh=mesh,
        in_specs=(P(axis_name, None), P(axis_name, None), P(axis_name), P(axis_name), P(axis_name), P(), P(), P(), P()),
        out_specs=(P(axis_name), P(axis_name), P(axis_name), P(), P(), P(), P()),
        check_vma=False,
    )
```

```python
import jax
import jax.numpy as jnp
from jax import lax
from jax.experimental import pallas as pl
from jax.experimental.pallas import tpu as pltpu
from jax.sharding import PartitionSpec as P

STEP = 10
ADAM_BETA1 = 0.9
ADAM_BETA2 = 0.98
ADAM_EPS = 1e-8
WEIGHT_DECAY = 0.01
MAX_NORM = 1.0
NORM_EPS = 1e-6
BIAS_ONE = 1.0 - ADAM_BETA1 ** STEP
BIAS_TWO = 1.0 - ADAM_BETA2 ** STEP

DP = 32
AG_CHUNKS = 10
AG_ROWS = 240
AG_AB = 48
AG_CD = 72
PIECE = 2400
CHUNKS = 50
ROWS = PIECE // CHUNKS
HALF = ROWS // 2
RAB = 8
RCD = HALF - RAB
SKEW_RS = 2
AG_STAGES = (0, 2, 3, 4, 5, 6)
SLOTS = 12
VEC = 130
VPAD = 136
MESH = pl.DeviceIdType.MESH
F32 = jnp.float32
BF16 = jnp.bfloat16


def adam_update(grad_vals, param_vals, moment_one, moment_two, learn_rate, decay_rate):
    new_one = ADAM_BETA1 * moment_one + (1.0 - ADAM_BETA1) * grad_vals
    new_two = ADAM_BETA2 * moment_two + (1.0 - ADAM_BETA2) * grad_vals * grad_vals
    direction = (new_one / BIAS_ONE) / (jnp.sqrt(new_two / BIAS_TWO) + ADAM_EPS)
    return param_vals - learn_rate * (direction + decay_rate * param_vals), new_one, new_two


def kernel(g, gv, p, m, v, pv, mv, vv, lr,
           po, mo, vo, pvo, mvo, vvo, pb,
           lrs, gvb, stage, dense, pab, pcd, abz, er, cdr, abr, fr, gsum, ssq, clip, vs, vr, ns, nr,
           in_sem, pmv_sem, s0_send, s0_recv, rs_send, er_recv, cd_recv, ab_recv, f_recv,
           vec_send, vec_recv, norm_send, norm_recv,
           ag_send, ag_ab, ag_cd, ag_cd1, ag_h2, ag_h3, ag_d2d):
    me = lax.axis_index("dp")
    c = me % 2
    x = (me // 2) % 2
    y = (me // 4) % 2
    z = me // 8

    def dev(zz, yy, xx, cc):
        return ((zz * 2 + yy) * 2 + xx) * 2 + cc

    partner = dev(z, y, x, 1 - c)
    xs = dev(z, y, 1 - x, c)
    xo = dev(z, y, 1 - x, 1 - c)
    ys = dev(z, 1 - y, x, c)
    yo = dev(z, 1 - y, x, 1 - c)
    up = dev((z + 1) % 4, y, x, c)
    down = dev((z + 3) % 4, y, x, c)
    z1 = dev(z + 1 - 2 * (z % 2), y, x, c)
    z2 = dev((z + 2) % 4, y, x, c)
    nlow = z >= 1
    nhigh = z <= 2

    def send(src, dst, ssem, rsem, to):
        pltpu.make_async_remote_copy(
            src_ref=src, dst_ref=dst, send_sem=ssem, recv_sem=rsem, device_id=(to,), device_id_type=MESH
        ).start()

    def wait(ref, sem):
        pltpu.make_async_copy(ref, ref, sem).wait()

    def fetch(k, slot):
        def one(d, carry):
            off = pl.multiple_of((d * PIECE + k * ROWS) * 128, 1024)
            pltpu.make_async_copy(g.at[0:1, pl.ds(off, ROWS * 128)], stage.at[slot, d], in_sem.at[slot]).start()
            return carry
        lax.fori_loop(0, DP, one, 0)

    barrier = pltpu.get_barrier_semaphore()
    for nb in (partner, xs, xo, ys, yo, z2):
        pl.semaphore_signal(barrier, inc=1, device_id=(nb,), device_id_type=MESH)

    @pl.when(nhigh)
    def _():
        pl.semaphore_signal(barrier, inc=1, device_id=(up,), device_id_type=MESH)

    @pl.when(nlow)
    def _():
        pl.semaphore_signal(barrier, inc=1, device_id=(down,), device_id_type=MESH)

    fetch(0, 0)
    ssq[...] = jnp.zeros((8, 128), F32)

    mid = (z >= 1) & (z <= 2)

    def await_neighbours():
        @pl.when(mid)
        def _():
            pl.semaphore_wait(barrier, 8)

        @pl.when(jnp.logical_not(mid))
        def _():
            pl.semaphore_wait(barrier, 7)

    partners = (partner, xs, ys, z1, z2)

    loads = ((gv, gvb), (p, po), (m, mo), (v, vo), (pv, pvo), (mv, mvo), (vv, vvo), (lr, lrs))

    def vec_step(j):
        if j == 0:
            for i, (src, dst) in enumerate(loads):
                pltpu.make_async_copy(src, dst, pmv_sem.at[i]).start()
            wait(gvb, pmv_sem.at[0])
            vs[0, 0:128] = gvb[0:1, 0:16384].astype(F32).reshape(128, 128)
            vs[0, 128:VPAD] = jnp.zeros((VPAD - 128, 128), F32)
            vs[0, 128:VEC] = gvb[0:1, 16384:16640].astype(F32).reshape(2, 128)
        else:
            wait(vr.at[j - 1], vec_recv.at[j - 1])
            vs[j] = vs[j - 1] + vr[j - 1]
        if j < 5:
            send(vs.at[j], vr.at[j], vec_send.at[j], vec_recv.at[j], partners[j])

    per = PIECE // (24 * HALF)

    def rpiece(k, d):
        at = (2 * k + d) // per
        return at // 8, (at // 4) % 2, (at // 2) % 2, at % 2

    def roff(k, d):
        return ((2 * k + d) % per) * 24 * HALF

    def rbuf(k, d, j):
        return pb.at[(*rpiece(k, d), pl.ds(roff(k, d) + j * 8 * HALF, 8 * HALF))]

    def convert(k):
        slot = k % 2
        dslot = k % 4

        @pl.when(k >= 4)
        def _():
            wait(dense.at[dslot, :, pl.ds(1, 3)], s0_send.at[dslot])

        wait(stage.at[slot], in_sem.at[slot])

        def conv(b, carry):
            row = pl.multiple_of(b * 2 * HALF, 16)
            for d in range(2):
                for q in range(4):
                    cc = 1 - c if q % 2 else c
                    vals = []
                    for o in range(2):
                        if d == 0:
                            piece = dev(b, o, 1 - x if q >= 2 else x, cc)
                        else:
                            piece = dev(b, 1 - y if q >= 2 else y, o, cc)
                        flat = stage[slot, piece, 0:1, d * HALF * 128:(d + 1) * HALF * 128].astype(F32)
                        vals.append(flat.reshape(HALF, 128))
                    dense[dslot, d, q, pl.ds(row, 2 * HALF)] = jnp.concatenate(vals, axis=0).astype(BF16)
            return carry

        lax.fori_loop(0, 4, conv, 0)

        @pl.when(k + 1 < CHUNKS)
        def _():
            fetch(k + 1, 1 - slot)

    def stage0(k):
        dslot = k % 4
        for q in (3, 2, 1):
            for d in range(2):
                to = ((partner, xs, xo), (partner, ys, yo))[d][q - 1]
                send(dense.at[dslot, d, q], rbuf(k, d, q - 1), s0_send.at[dslot], s0_recv.at[k % SLOTS], to)

        @pl.when(k + 1 < CHUNKS)
        def _():
            convert(k + 1)

    def z_first(k, bufs, recv, rsem):
        @pl.when(z == 0)
        def _():
            send(bufs.at[pl.ds(1, 3)], recv.at[pl.ds(0, 3)], rs_send.at[k], rsem.at[0], up)

        @pl.when(z == 3)
        def _():
            send(bufs.at[pl.ds(0, 3)], recv.at[pl.ds(0, 3)], rs_send.at[k], rsem.at[0], down)

    def z_second(k, bufs, recv, rsem):
        @pl.when(z == 1)
        def _():
            wait(recv.at[pl.ds(0, 3)], rsem.at[0])
            bufs[1:4] += recv[0:3]
            send(bufs.at[pl.ds(2, 2)], recv.at[pl.ds(3, 2)], rs_send.at[k], rsem.at[1], up)

        @pl.when(z == 2)
        def _():
            wait(recv.at[pl.ds(0, 3)], rsem.at[0])
            bufs[0:3] += recv[0:3]
            send(bufs.at[pl.ds(0, 2)], recv.at[pl.ds(3, 2)], rs_send.at[k], rsem.at[1], down)

    def z_third(k, bufs, recv, rsem):
        @pl.when(z == 1)
        def _():
            wait(recv.at[pl.ds(3, 2)], rsem.at[1])
            bufs[0:2] += recv[3:5]
            send(bufs.at[0], recv.at[0], rs_send.at[k], rsem.at[0], down)

        @pl.when(z == 2)
        def _():
            wait(recv.at[pl.ds(3, 2)], rsem.at[1])
            bufs[2:4] += recv[3:5]
            send(bufs.at[3], recv.at[0], rs_send.at[k], rsem.at[0], up)

    def z_final(k, bufs, recv, rsem):
        @pl.when(jnp.logical_not(mid))
        def _():
            wait(recv.at[0], rsem.at[0])
            bufs[z] += recv[0]

    def stage1(k):
        dslot = k % 4
        wait(dense.at[dslot, :, pl.ds(1, 3)], s0_recv.at[k % SLOTS])
        for d in range(2):
            def add(b, carry, d=d):
                row = pl.multiple_of(b * 2 * HALF, 16)
                tot = dense[dslot, d, 0, pl.ds(row, 2 * HALF)].astype(F32)
                for j in range(3):
                    off = pl.multiple_of(roff(k, d) + j * 8 * HALF + b * 2 * HALF, 16)
                    tot = tot + pb[(*rpiece(k, d), pl.ds(off, 2 * HALF))].astype(F32)
                for o in range(2):
                    pab[k, d, o, b] = tot[o * HALF:o * HALF + RAB]
                    pcd[k, d, b, o] = tot[o * HALF + RAB:(o + 1) * HALF]
                return carry
            lax.fori_loop(0, 4, add, 0)
        send(pab.at[k, 0, 1 - y], er.at[k, 0], rs_send.at[k], er_recv.at[k % SLOTS], ys)
        send(pab.at[k, 1, 1 - x], er.at[k, 1], rs_send.at[k], er_recv.at[k % SLOTS], xs)
        for d in range(2):
            z_first(k, pcd.at[k, d], cdr.at[k, d], cd_recv.at[k % SLOTS, d])

    def stage2(k):
        for d in range(2):
            z_second(k, pcd.at[k, d], cdr.at[k, d], cd_recv.at[k % SLOTS, d])
        wait(er.at[k], er_recv.at[k % SLOTS])
        for zz in range(4):
            abz[k, zz, 0] = pab[k, 0, y, zz] + er[k, 0, zz]
            abz[k, zz, 1] = pab[k, 1, x, zz] + er[k, 1, zz]
        z_first(k, abz.at[k], abr.at[k], ab_recv.at[k % SLOTS])

    def stage3(k):
        for d in range(2):
            z_third(k, pcd.at[k, d], cdr.at[k, d], cd_recv.at[k % SLOTS, d])
        z_second(k, abz.at[k], abr.at[k], ab_recv.at[k % SLOTS])

    def stage4(k):
        for d in range(2):
            z_final(k, pcd.at[k, d], cdr.at[k, d], cd_recv.at[k % SLOTS, d])
        send(pcd.at[k, 0, z, 1 - y], fr.at[k, 0], rs_send.at[k], f_recv.at[k % SLOTS], ys)
        send(pcd.at[k, 1, z, 1 - x], fr.at[k, 1], rs_send.at[k], f_recv.at[k % SLOTS], xs)
        z_third(k, abz.at[k], abr.at[k], ab_recv.at[k % SLOTS])

    def stage5(k):
        z_final(k, abz.at[k], abr.at[k], ab_recv.at[k % SLOTS])
        wait(fr.at[k], f_recv.at[k % SLOTS])
        base = pl.multiple_of(k * ROWS, 16)
        parts = (
            (0, RAB, abz[k, z, 0]),
            (RAB, RCD, pcd[k, 0, z, y] + fr[k, 0]),
            (HALF, RAB, abz[k, z, 1]),
            (HALF + RAB, RCD, pcd[k, 1, z, x] + fr[k, 1]),
        )
        acc = ssq[...]
        for off, num, val in parts:
            val = val * (1.0 / DP)
            gsum[pl.ds(base + off, num)] = val
            acc = acc + jnp.sum((val * val).reshape(num // 8, 8, 128), axis=0)
        ssq[...] = acc

    def rs_iter(i, carry):
        for s, fn in enumerate((stage0, stage1, stage2, stage3, stage4, stage5)):
            k = i - SKEW_RS * s

            @pl.when((k >= 0) & (k < CHUNKS))
            def _(fn=fn, k=k):
                fn(k)
        for j in range(6):
            @pl.when(i == 4 + 4 * j)
            def _(j=j):
                vec_step(j)
        return carry

    convert(0)
    await_neighbours()
    lax.fori_loop(0, CHUNKS + 5 * SKEW_RS, rs_iter, 0)

    for i, (src, dst) in enumerate(loads[1:]):
        pltpu.make_async_copy(src, dst, pmv_sem.at[i + 1]).wait()
    ns[...] = jnp.sum(ssq[...], axis=0, keepdims=True)
    nr[me] = ns[...]

    def tell(j, carry):
        send(ns, nr.at[me], norm_send, norm_recv, (me + j) % DP)
        return carry

    lax.fori_loop(1, DP, tell, 0)
    gvec = vs[5, 0:VEC] * (1.0 / DP)
    ssq[0:1] = jnp.sum(gvec * gvec, axis=0, keepdims=True)
    wait(nr.at[pl.ds(0, DP - 1)], norm_recv)
    norm_sq = jnp.full((8, 128), jnp.sum(jnp.sum(nr[...], axis=0) + ssq[0:1]))
    clip[...] = jnp.minimum(1.0, MAX_NORM / (jnp.sqrt(norm_sq) + NORM_EPS))

    rate = lrs[0, 0]

    def cut(k, off, num):
        return pl.ds(pl.multiple_of(k * AG_ROWS + off, 8), num)

    def rows_of(k):
        return (cut(k, 0, AG_AB), cut(k, AG_AB, AG_AB), cut(k, 2 * AG_AB, AG_CD), cut(k, 2 * AG_AB + AG_CD, AG_CD))

    full = slice(None)

    def region(zz, yy, xx, rows):
        return pb.at[zz, yy, xx, c, rows]

    def push(ref, k, rsem, to):
        send(ref, ref, ag_send.at[k], rsem, to)

    def sides(dist, fn):
        if dist == 0:
            fn(z, None)
            return

        @pl.when(z - dist >= 0)
        def _():
            fn(z - dist, 0)

        @pl.when(z + dist <= 3)
        def _():
            fn(z + dist, 1)

    def along_z(fn):
        @pl.when(nhigh)
        def _():
            fn(0, up)

        @pl.when(nlow)
        def _():
            fn(1, down)

    def onward_z(side, dist, fn):
        if dist == 0:
            along_z(fn)
        elif dist < 3 and side == 0:
            @pl.when(nhigh)
            def _():
                fn(0, up)
        elif dist < 3:
            @pl.when(nlow)
            def _():
                fn(1, down)

    def ab_arrived(k, dist):
        ra, rb = rows_of(k)[:2]
        ab = cut(k, 0, 2 * AG_AB)

        def fn(zz, side):
            if dist:
                wait(region(0, 0, 0, ab), ag_ab.at[k, zz])
            onward_z(side, dist, lambda way, to: push(region(zz, y, x, ab), k, ag_ab.at[k, zz], to))
            push(region(zz, y, x, ra), k, ag_h2.at[k, zz], ys)
            push(region(zz, y, x, rb), k, ag_h2.at[k, zz], xs)

        sides(dist, fn)

    def ab_second(k, dist):
        ra, rb = rows_of(k)[:2]

        def fn(zz, side):
            wait(region(0, 0, 0, cut(k, 0, 2 * AG_AB)), ag_h2.at[k, zz])
            push(region(zz, full, x, ra), k, ag_h3.at[k, zz], xs)
            push(region(zz, y, full, rb), k, ag_h3.at[k, zz], ys)

        sides(dist, fn)

    def cd_arrived(k, dist):
        rc, rd = rows_of(k)[2:]

        def fn(zz, side):
            if dist == 0:
                wait(region(0, 0, 0, cut(k, 0, 2 * AG_CD)), ag_cd1.at[k])
            else:
                wait(pb.at[0, 0, full, full, rc], ag_cd.at[k, zz])

            def on(way, to):
                push(region(zz, full, x, rc), k, ag_cd.at[k, zz], to)
                push(region(zz, y, full, rd), k, ag_cd.at[k, zz], to)

            onward_z(side, dist, on)
            push(region(zz, full, x, rc), k, ag_h3.at[k, zz], xs)
            push(region(zz, y, full, rd), k, ag_h3.at[k, zz], ys)

        sides(dist, fn)

    def ag0(k):
        def upd(b, carry):
            rows = pl.ds(pl.multiple_of(k * AG_ROWS + b * 48, 16), 48)
            new = adam_update(gsum[rows] * clip[0:1], po[rows], mo[rows], vo[rows], rate, WEIGHT_DECAY)
            po[rows], mo[rows], vo[rows] = new
            pb[z, y, x, c, rows] = new[0].astype(BF16)
            return carry
        lax.fori_loop(2 * AG_AB // 48, AG_ROWS // 48, upd, 0)
        rc, rd = rows_of(k)[2:]
        push(region(z, y, x, rc), k, ag_cd1.at[k], ys)
        push(region(z, y, x, rd), k, ag_cd1.at[k], xs)
        lax.fori_loop(0, 2 * AG_AB // 48, upd, 0)
        ab_arrived(k, 0)

    def middle(s):
        def fn(k):
            cd_arrived(k, s - 1)
            if s <= 3:
                ab_arrived(k, s)
            ab_second(k, s - 1)
        return fn

    def ag5(k):
        ra, rb, rc, rd = rows_of(k)

        def over(zz, xx, yy):
            push(region(zz, full, xx, ra), k, ag_d2d.at[k], partner)
            push(region(zz, yy, full, rb), k, ag_d2d.at[k], partner)
            push(region(zz, full, xx, rc), k, ag_d2d.at[k], partner)
            push(region(zz, yy, full, rd), k, ag_d2d.at[k], partner)

        def fn(zz, side):
            wait(pb.at[0, 0, 0, full, cut(k, 0, AG_ROWS)], ag_h3.at[k, zz])
            over(zz, 1 - x, 1 - y)

        over(full, x, y)
        for dist in range(4):
            sides(dist, fn)

    def ag_iter(i, carry):
        for s, fn in zip(AG_STAGES, (ag0, middle(1), middle(2), middle(3), middle(4), ag5)):
            k = i - s

            @pl.when((k >= 0) & (k < AG_CHUNKS))
            def _(fn=fn, k=k):
                fn(k)
        return carry

    lax.fori_loop(0, AG_CHUNKS + AG_STAGES[-1], ag_iter, 0)

    newv = adam_update(gvec * clip[0:1], pvo[...], mvo[...], vvo[...], rate, 0.0)
    pvo[...], mvo[...], vvo[...] = newv

    def drain_rs(k, carry):
        wait(gsum.at[pl.ds(0, 14 * HALF)], rs_send.at[k])
        return carry

    def drain_ag(k, carry):
        wait(pb.at[full, full, full, 0, cut(k, 0, AG_ROWS)], ag_d2d.at[k])
        base, along = 24 * AG_AB + 18 * AG_CD + 16 * AG_ROWS, 2 * AG_AB + 4 * AG_CD

        @pl.when(mid)
        def _():
            wait(pb.at[0, 0, full, full, pl.ds(0, (base + 5 * along) // 4)], ag_send.at[k])

        @pl.when(jnp.logical_not(mid))
        def _():
            wait(pb.at[0, 0, full, full, pl.ds(0, (base + along) // 4)], ag_send.at[k])

        return carry

    lax.fori_loop(0, CHUNKS, drain_rs, 0)
    lax.fori_loop(0, AG_CHUNKS, drain_ag, 0)
    for s in range(4):
        wait(dense.at[s, :, pl.ds(1, 3)], s0_send.at[s])
    for j in range(5):
        wait(vs.at[j], vec_send.at[j])
    wait(nr.at[pl.ds(0, DP - 1)], norm_send)


def finish(*refs):
    srcs, dsts, sem = refs[:7], refs[7:14], refs[14]
    copies = [
        pltpu.make_async_copy(srcs[6].at[i // 4, i // 2 % 2, i % 2], dsts[6].at[i // 4, i // 2 % 2, i % 2], sem.at[6 + i])
        for i in range(16)
    ]
    copies += [pltpu.make_async_copy(srcs[i], dsts[i], sem.at[i]) for i in range(6)]
    for copy in copies:
        copy.start()
    for copy in copies:
        copy.wait()


def solution(mesh):
    axis_name = mesh.axis_names[0]
    vm = pl.BlockSpec(memory_space=pltpu.VMEM)
    hbm = pl.BlockSpec(memory_space=pl.ANY)
    dma = pltpu.SemaphoreType.DMA
    K, G = CHUNKS, AG_CHUNKS

    call = pl.pallas_call(
        kernel,
        name="adam_step",
        out_shape=(
            [pltpu.VMEM((PIECE, 128), F32)] * 3
            + [pltpu.VMEM((VEC, 128), F32)] * 3
            + [pltpu.VMEM((4, 2, 2, 2, PIECE, 128), BF16)]
        ),
        in_specs=[hbm] * 9,
        out_specs=[vm] * 7,
        scratch_shapes=[
            pltpu.SMEM((1, 1), F32),
            pltpu.VMEM((1, VEC * 128), BF16),
            pltpu.VMEM((2, DP, 1, ROWS * 128), BF16),
            pltpu.VMEM((4, 2, 4, 8 * HALF, 128), BF16),
            pltpu.VMEM((K, 2, 2, 4, RAB, 128), F32),
            pltpu.VMEM((K, 2, 4, 2, RCD, 128), F32),
            pltpu.VMEM((K, 4, 2, RAB, 128), F32),
            pltpu.VMEM((K, 2, 4, RAB, 128), F32),
            pltpu.VMEM((K, 2, 5, 2, RCD, 128), F32),
            pltpu.VMEM((K, 5, 2, RAB, 128), F32),
            pltpu.VMEM((K, 2, RCD, 128), F32),
            pltpu.VMEM((PIECE, 128), F32),
            pltpu.VMEM((8, 128), F32),
            pltpu.VMEM((8, 128), F32),
            pltpu.VMEM((6, VPAD, 128), F32),
            pltpu.VMEM((5, VPAD, 128), F32),
            pltpu.VMEM((1, 128), F32),
            pltpu.VMEM((DP, 1, 128), F32),
            dma((2,)), dma((8,)), dma((4,)), dma((SLOTS,)), dma((K,)), dma((SLOTS,)), dma((SLOTS, 2, 2)), dma((SLOTS, 2)), dma((SLOTS,)),
            dma((5,)), dma((5,)), dma, dma,
            dma((G,)), dma((G, 4)), dma((G, 4)), dma((G,)), dma((G, 4)), dma((G, 4)), dma((G,)),
        ],
        compiler_params=pltpu.CompilerParams(
            collective_id=0, has_side_effects=True, vmem_limit_bytes=37 * 2 ** 20
        ),
    )

    shapes = [(PIECE, 128)] * 3 + [(VEC, 128)] * 3
    copy_out = pl.pallas_call(
        finish,
        name="copy_out",
        out_shape=[jax.ShapeDtypeStruct(s, F32) for s in shapes] + [jax.ShapeDtypeStruct((4, 2, 2, 2, PIECE, 128), BF16)],
        in_specs=[vm] * 7,
        out_specs=[hbm] * 7,
        scratch_shapes=[dma((22,))],
        compiler_params=pltpu.CompilerParams(vmem_limit_bytes=2 ** 20),
    )

    def local_step(g_mat, g_vec, p_mat, m_mat, v_mat, p_vec, m_vec, v_vec, learn_rate):
        outs = call(
            g_mat, g_vec,
            p_mat.reshape(PIECE, 128), m_mat.reshape(PIECE, 128), v_mat.reshape(PIECE, 128),
            p_vec.reshape(VEC, 128), m_vec.reshape(VEC, 128), v_vec.reshape(VEC, 128),
            learn_rate.reshape(1, 1),
        )
        return tuple(o.reshape(-1) for o in copy_out(*outs))

    return jax.shard_map(
        local_step,
        mesh=mesh,
        in_specs=(P(axis_name, None), P(axis_name, None), P(axis_name), P(axis_name), P(axis_name), P(), P(), P(), P()),
        out_specs=(P(axis_name), P(axis_name), P(axis_name), P(), P(), P(), P()),
        check_vma=False,
    )
```

```python
import jax
import jax.numpy as jnp
from jax import lax
from jax.experimental import pallas as pl
from jax.experimental.pallas import tpu as pltpu
from jax.sharding import PartitionSpec as P

STEP = 10
ADAM_BETA1 = 0.9
ADAM_BETA2 = 0.98
ADAM_EPS = 1e-8
WEIGHT_DECAY = 0.01
MAX_NORM = 1.0
NORM_EPS = 1e-6
BIAS_ONE = 1.0 - ADAM_BETA1 ** STEP
BIAS_TWO = 1.0 - ADAM_BETA2 ** STEP

DP = 32
AG_CHUNKS = 10
AG_ROWS = 240
AG_AB = 48
AG_CD = 72
PIECE = 2400
CHUNKS = 50
ROWS = PIECE // CHUNKS
HALF = ROWS // 2
RAB = 8
RCD = HALF - RAB
SKEW_RS = 3
AG_STAGES = (0, 2, 3, 4, 5, 6)
SLOTS = 20
VEC = 130
VPAD = 136
MESH = pl.DeviceIdType.MESH
F32 = jnp.float32
BF16 = jnp.bfloat16


def adam_update(grad_vals, param_vals, moment_one, moment_two, learn_rate, decay_rate):
    new_one = ADAM_BETA1 * moment_one + (1.0 - ADAM_BETA1) * grad_vals
    new_two = ADAM_BETA2 * moment_two + (1.0 - ADAM_BETA2) * grad_vals * grad_vals
    direction = (new_one / BIAS_ONE) / (jnp.sqrt(new_two / BIAS_TWO) + ADAM_EPS)
    return param_vals - learn_rate * (direction + decay_rate * param_vals), new_one, new_two


def kernel(g, gv, p, m, v, pv, mv, vv, lr,
           po, mo, vo, pvo, mvo, vvo, pb,
           lrs, gvb, stage, dense, pab, pcd, abz, er, cdr, abr, fr, gsum, ssq, clip, vs, vr, ns, nr,
           in_sem, pmv_sem, s0_send, s0_recv, rs_send, er_recv, cd_recv, ab_recv, f_recv,
           vec_send, vec_recv, norm_send, norm_recv,
           ag_send, ag_ab, ag_cd, ag_cd1, ag_h2, ag_h3, ag_d2d):
    me = lax.axis_index("dp")
    c = me % 2
    x = (me // 2) % 2
    y = (me // 4) % 2
    z = me // 8

    def dev(zz, yy, xx, cc):
        return ((zz * 2 + yy) * 2 + xx) * 2 + cc

    partner = dev(z, y, x, 1 - c)
    xs = dev(z, y, 1 - x, c)
    xo = dev(z, y, 1 - x, 1 - c)
    ys = dev(z, 1 - y, x, c)
    yo = dev(z, 1 - y, x, 1 - c)
    up = dev((z + 1) % 4, y, x, c)
    down = dev((z + 3) % 4, y, x, c)
    z1 = dev(z + 1 - 2 * (z % 2), y, x, c)
    z2 = dev((z + 2) % 4, y, x, c)
    nlow = z >= 1
    nhigh = z <= 2

    def send(src, dst, ssem, rsem, to):
        pltpu.make_async_remote_copy(
            src_ref=src, dst_ref=dst, send_sem=ssem, recv_sem=rsem, device_id=(to,), device_id_type=MESH
        ).start()

    def wait(ref, sem):
        pltpu.make_async_copy(ref, ref, sem).wait()

    def fetch(k, slot):
        def one(d, carry):
            off = pl.multiple_of((d * PIECE + k * ROWS) * 128, 1024)
            pltpu.make_async_copy(g.at[0:1, pl.ds(off, ROWS * 128)], stage.at[slot, d], in_sem.at[slot]).start()
            return carry
        lax.fori_loop(0, DP, one, 0)

    barrier = pltpu.get_barrier_semaphore()
    for nb in (partner, xs, xo, ys, yo, z2):
        pl.semaphore_signal(barrier, inc=1, device_id=(nb,), device_id_type=MESH)

    @pl.when(nhigh)
    def _():
        pl.semaphore_signal(barrier, inc=1, device_id=(up,), device_id_type=MESH)

    @pl.when(nlow)
    def _():
        pl.semaphore_signal(barrier, inc=1, device_id=(down,), device_id_type=MESH)

    fetch(0, 0)
    ssq[...] = jnp.zeros((8, 128), F32)

    mid = (z >= 1) & (z <= 2)

    def await_neighbours():
        @pl.when(mid)
        def _():
            pl.semaphore_wait(barrier, 8)

        @pl.when(jnp.logical_not(mid))
        def _():
            pl.semaphore_wait(barrier, 7)

    partners = (partner, xs, ys, z1, z2)

    loads = ((gv, gvb), (p, po), (m, mo), (v, vo), (pv, pvo), (mv, mvo), (vv, vvo), (lr, lrs))

    def vec_step(j):
        if j == 0:
            for i, (src, dst) in enumerate(loads):
                pltpu.make_async_copy(src, dst, pmv_sem.at[i]).start()
            wait(gvb, pmv_sem.at[0])
            vs[0, 0:128] = gvb[0:1, 0:16384].astype(F32).reshape(128, 128)
            vs[0, 128:VPAD] = jnp.zeros((VPAD - 128, 128), F32)
            vs[0, 128:VEC] = gvb[0:1, 16384:16640].astype(F32).reshape(2, 128)
        else:
            wait(vr.at[j - 1], vec_recv.at[j - 1])
            vs[j] = vs[j - 1] + vr[j - 1]
        if j < 5:
            send(vs.at[j], vr.at[j], vec_send.at[j], vec_recv.at[j], partners[j])

    per = PIECE // (24 * HALF)

    def rpiece(k, d):
        at = (2 * k + d) // per
        return at // 8, (at // 4) % 2, (at // 2) % 2, at % 2

    def roff(k, d):
        return ((2 * k + d) % per) * 24 * HALF

    def rbuf(k, d, j):
        return pb.at[(*rpiece(k, d), pl.ds(roff(k, d) + j * 8 * HALF, 8 * HALF))]

    def convert(k):
        slot = k % 2
        dslot = k % 5

        @pl.when(k >= 5)
        def _():
            wait(dense.at[dslot, :, pl.ds(1, 3)], s0_send.at[dslot])

        wait(stage.at[slot], in_sem.at[slot])

        def conv(b, carry):
            row = pl.multiple_of(b * 2 * HALF, 16)
            for d in range(2):
                for q in range(4):
                    cc = 1 - c if q % 2 else c
                    vals = []
                    for o in range(2):
                        if d == 0:
                            piece = dev(b, o, 1 - x if q >= 2 else x, cc)
                        else:
                            piece = dev(b, 1 - y if q >= 2 else y, o, cc)
                        flat = stage[slot, piece, 0:1, d * HALF * 128:(d + 1) * HALF * 128].astype(F32)
                        vals.append(flat.reshape(HALF, 128))
                    dense[dslot, d, q, pl.ds(row, 2 * HALF)] = jnp.concatenate(vals, axis=0).astype(BF16)
            return carry

        lax.fori_loop(0, 4, conv, 0)

        @pl.when(k + 1 < CHUNKS)
        def _():
            fetch(k + 1, 1 - slot)

    def stage0(k):
        dslot = k % 5
        for q in (3, 2, 1):
            for d in range(2):
                to = ((partner, xs, xo), (partner, ys, yo))[d][q - 1]
                send(dense.at[dslot, d, q], rbuf(k, d, q - 1), s0_send.at[dslot], s0_recv.at[k % SLOTS], to)

        @pl.when(k + 1 < CHUNKS)
        def _():
            convert(k + 1)

    def z_first(k, bufs, recv, rsem):
        @pl.when(z == 0)
        def _():
            send(bufs.at[pl.ds(1, 3)], recv.at[pl.ds(0, 3)], rs_send.at[k], rsem.at[0], up)

        @pl.when(z == 3)
        def _():
            send(bufs.at[pl.ds(0, 3)], recv.at[pl.ds(0, 3)], rs_send.at[k], rsem.at[0], down)

    def z_second(k, bufs, recv, rsem):
        @pl.when(z == 1)
        def _():
            wait(recv.at[pl.ds(0, 3)], rsem.at[0])
            bufs[1:4] += recv[0:3]
            send(bufs.at[pl.ds(2, 2)], recv.at[pl.ds(3, 2)], rs_send.at[k], rsem.at[1], up)

        @pl.when(z == 2)
        def _():
            wait(recv.at[pl.ds(0, 3)], rsem.at[0])
            bufs[0:3] += recv[0:3]
            send(bufs.at[pl.ds(0, 2)], recv.at[pl.ds(3, 2)], rs_send.at[k], rsem.at[1], down)

    def z_third(k, bufs, recv, rsem):
        @pl.when(z == 1)
        def _():
            wait(recv.at[pl.ds(3, 2)], rsem.at[1])
            bufs[0:2] += recv[3:5]
            send(bufs.at[0], recv.at[0], rs_send.at[k], rsem.at[0], down)

        @pl.when(z == 2)
        def _():
            wait(recv.at[pl.ds(3, 2)], rsem.at[1])
            bufs[2:4] += recv[3:5]
            send(bufs.at[3], recv.at[0], rs_send.at[k], rsem.at[0], up)

    def z_final(k, bufs, recv, rsem):
        @pl.when(jnp.logical_not(mid))
        def _():
            wait(recv.at[0], rsem.at[0])
            bufs[z] += recv[0]

    def stage1(k):
        dslot = k % 5
        wait(dense.at[dslot, :, pl.ds(1, 3)], s0_recv.at[k % SLOTS])
        for d in range(2):
            def add(b, carry, d=d):
                row = pl.multiple_of(b * 2 * HALF, 16)
                tot = dense[dslot, d, 0, pl.ds(row, 2 * HALF)].astype(F32)
                for j in range(3):
                    off = pl.multiple_of(roff(k, d) + j * 8 * HALF + b * 2 * HALF, 16)
                    tot = tot + pb[(*rpiece(k, d), pl.ds(off, 2 * HALF))].astype(F32)
                for o in range(2):
                    pab[k, d, o, b] = tot[o * HALF:o * HALF + RAB]
                    pcd[k, d, b, o] = tot[o * HALF + RAB:(o + 1) * HALF]
                return carry
            lax.fori_loop(0, 4, add, 0)
        send(pab.at[k, 0, 1 - y], er.at[k, 0], rs_send.at[k], er_recv.at[k % SLOTS], ys)
        send(pab.at[k, 1, 1 - x], er.at[k, 1], rs_send.at[k], er_recv.at[k % SLOTS], xs)
        for d in range(2):
            z_first(k, pcd.at[k, d], cdr.at[k, d], cd_recv.at[k % SLOTS, d])

    def stage2(k):
        for d in range(2):
            z_second(k, pcd.at[k, d], cdr.at[k, d], cd_recv.at[k % SLOTS, d])
        wait(er.at[k], er_recv.at[k % SLOTS])
        for zz in range(4):
            abz[k, zz, 0] = pab[k, 0, y, zz] + er[k, 0, zz]
            abz[k, zz, 1] = pab[k, 1, x, zz] + er[k, 1, zz]
        z_first(k, abz.at[k], abr.at[k], ab_recv.at[k % SLOTS])

    def stage3(k):
        for d in range(2):
            z_third(k, pcd.at[k, d], cdr.at[k, d], cd_recv.at[k % SLOTS, d])
        z_second(k, abz.at[k], abr.at[k], ab_recv.at[k % SLOTS])

    def stage4(k):
        for d in range(2):
            z_final(k, pcd.at[k, d], cdr.at[k, d], cd_recv.at[k % SLOTS, d])
        send(pcd.at[k, 0, z, 1 - y], fr.at[k, 0], rs_send.at[k], f_recv.at[k % SLOTS], ys)
        send(pcd.at[k, 1, z, 1 - x], fr.at[k, 1], rs_send.at[k], f_recv.at[k % SLOTS], xs)
        z_third(k, abz.at[k], abr.at[k], ab_recv.at[k % SLOTS])

    def stage5(k):
        z_final(k, abz.at[k], abr.at[k], ab_recv.at[k % SLOTS])
        wait(fr.at[k], f_recv.at[k % SLOTS])
        base = pl.multiple_of(k * ROWS, 16)
        parts = (
            (0, RAB, abz[k, z, 0]),
            (RAB, RCD, pcd[k, 0, z, y] + fr[k, 0]),
            (HALF, RAB, abz[k, z, 1]),
            (HALF + RAB, RCD, pcd[k, 1, z, x] + fr[k, 1]),
        )
        acc = ssq[...]
        for off, num, val in parts:
            val = val * (1.0 / DP)
            gsum[pl.ds(base + off, num)] = val
            acc = acc + jnp.sum((val * val).reshape(num // 8, 8, 128), axis=0)
        ssq[...] = acc

    def rs_iter(i, carry):
        for s, fn in enumerate((stage0, stage1, stage2, stage3, stage4, stage5)):
            k = i - SKEW_RS * s

            @pl.when((k >= 0) & (k < CHUNKS))
            def _(fn=fn, k=k):
                fn(k)
        for j in range(6):
            @pl.when(i == 4 + 4 * j)
            def _(j=j):
                vec_step(j)
        return carry

    convert(0)
    await_neighbours()
    lax.fori_loop(0, CHUNKS + 5 * SKEW_RS, rs_iter, 0)

    for i, (src, dst) in enumerate(loads[1:]):
        pltpu.make_async_copy(src, dst, pmv_sem.at[i + 1]).wait()
    ns[...] = jnp.sum(ssq[...], axis=0, keepdims=True)
    nr[me] = ns[...]

    def tell(j, carry):
        send(ns, nr.at[me], norm_send, norm_recv, (me + j) % DP)
        return carry

    lax.fori_loop(1, DP, tell, 0)
    gvec = vs[5, 0:VEC] * (1.0 / DP)
    ssq[0:1] = jnp.sum(gvec * gvec, axis=0, keepdims=True)
    wait(nr.at[pl.ds(0, DP - 1)], norm_recv)
    norm_sq = jnp.full((8, 128), jnp.sum(jnp.sum(nr[...], axis=0) + ssq[0:1]))
    clip[...] = jnp.minimum(1.0, MAX_NORM / (jnp.sqrt(norm_sq) + NORM_EPS))

    rate = lrs[0, 0]

    def cut(k, off, num):
        return pl.ds(pl.multiple_of(k * AG_ROWS + off, 8), num)

    def rows_of(k):
        return (cut(k, 0, AG_AB), cut(k, AG_AB, AG_AB), cut(k, 2 * AG_AB, AG_CD), cut(k, 2 * AG_AB + AG_CD, AG_CD))

    full = slice(None)

    def region(zz, yy, xx, rows):
        return pb.at[zz, yy, xx, c, rows]

    def push(ref, k, rsem, to):
        send(ref, ref, ag_send.at[k], rsem, to)

    def sides(dist, fn):
        if dist == 0:
            fn(z, None)
            return

        @pl.when(z - dist >= 0)
        def _():
            fn(z - dist, 0)

        @pl.when(z + dist <= 3)
        def _():
            fn(z + dist, 1)

    def along_z(fn):
        @pl.when(nhigh)
        def _():
            fn(0, up)

        @pl.when(nlow)
        def _():
            fn(1, down)

    def onward_z(side, dist, fn):
        if dist == 0:
            along_z(fn)
        elif dist < 3 and side == 0:
            @pl.when(nhigh)
            def _():
                fn(0, up)
        elif dist < 3:
            @pl.when(nlow)
            def _():
                fn(1, down)

    def ab_arrived(k, dist):
        ra, rb = rows_of(k)[:2]
        ab = cut(k, 0, 2 * AG_AB)

        def fn(zz, side):
            if dist:
                wait(region(0, 0, 0, ab), ag_ab.at[k, zz])
            onward_z(side, dist, lambda way, to: push(region(zz, y, x, ab), k, ag_ab.at[k, zz], to))
            push(region(zz, y, x, ra), k, ag_h2.at[k, zz], ys)
            push(region(zz, y, x, rb), k, ag_h2.at[k, zz], xs)

        sides(dist, fn)

    def ab_second(k, dist):
        ra, rb = rows_of(k)[:2]

        def fn(zz, side):
            wait(region(0, 0, 0, cut(k, 0, 2 * AG_AB)), ag_h2.at[k, zz])
            push(region(zz, full, x, ra), k, ag_h3.at[k, zz], xs)
            push(region(zz, y, full, rb), k, ag_h3.at[k, zz], ys)

        sides(dist, fn)

    def cd_arrived(k, dist):
        rc, rd = rows_of(k)[2:]

        def fn(zz, side):
            if dist == 0:
                wait(region(0, 0, 0, cut(k, 0, 2 * AG_CD)), ag_cd1.at[k])
            else:
                wait(pb.at[0, 0, full, full, rc], ag_cd.at[k, zz])

            def on(way, to):
                push(region(zz, full, x, rc), k, ag_cd.at[k, zz], to)
                push(region(zz, y, full, rd), k, ag_cd.at[k, zz], to)

            onward_z(side, dist, on)
            push(region(zz, full, x, rc), k, ag_h3.at[k, zz], xs)
            push(region(zz, y, full, rd), k, ag_h3.at[k, zz], ys)

        sides(dist, fn)

    def ag0(k):
        def upd(b, carry):
            rows = pl.ds(pl.multiple_of(k * AG_ROWS + b * 48, 16), 48)
            new = adam_update(gsum[rows] * clip[0:1], po[rows], mo[rows], vo[rows], rate, WEIGHT_DECAY)
            po[rows], mo[rows], vo[rows] = new
            pb[z, y, x, c, rows] = new[0].astype(BF16)
            return carry
        lax.fori_loop(2 * AG_AB // 48, AG_ROWS // 48, upd, 0)
        rc, rd = rows_of(k)[2:]
        push(region(z, y, x, rc), k, ag_cd1.at[k], ys)
        push(region(z, y, x, rd), k, ag_cd1.at[k], xs)
        lax.fori_loop(0, 2 * AG_AB // 48, upd, 0)
        ab_arrived(k, 0)

    def middle(s):
        def fn(k):
            cd_arrived(k, s - 1)
            if s <= 3:
                ab_arrived(k, s)
            ab_second(k, s - 1)
        return fn

    def ag5(k):
        ra, rb, rc, rd = rows_of(k)

        def over(zz, xx, yy):
            push(region(zz, full, xx, ra), k, ag_d2d.at[k], partner)
            push(region(zz, yy, full, rb), k, ag_d2d.at[k], partner)
            push(region(zz, full, xx, rc), k, ag_d2d.at[k], partner)
            push(region(zz, yy, full, rd), k, ag_d2d.at[k], partner)

        def fn(zz, side):
            wait(pb.at[0, 0, 0, full, cut(k, 0, AG_ROWS)], ag_h3.at[k, zz])
            over(zz, 1 - x, 1 - y)

        over(full, x, y)
        for dist in range(4):
            sides(dist, fn)

    def ag_iter(i, carry):
        for s, fn in zip(AG_STAGES, (ag0, middle(1), middle(2), middle(3), middle(4), ag5)):
            k = i - s

            @pl.when((k >= 0) & (k < AG_CHUNKS))
            def _(fn=fn, k=k):
                fn(k)
        return carry

    lax.fori_loop(0, AG_CHUNKS + AG_STAGES[-1], ag_iter, 0)

    newv = adam_update(gvec * clip[0:1], pvo[...], mvo[...], vvo[...], rate, 0.0)
    pvo[...], mvo[...], vvo[...] = newv

    def drain_rs(k, carry):
        wait(gsum.at[pl.ds(0, 14 * HALF)], rs_send.at[k])
        return carry

    def drain_ag(k, carry):
        wait(pb.at[full, full, full, 0, cut(k, 0, AG_ROWS)], ag_d2d.at[k])
        base, along = 24 * AG_AB + 18 * AG_CD + 16 * AG_ROWS, 2 * AG_AB + 4 * AG_CD

        @pl.when(mid)
        def _():
            wait(pb.at[0, 0, full, full, pl.ds(0, (base + 5 * along) // 4)], ag_send.at[k])

        @pl.when(jnp.logical_not(mid))
        def _():
            wait(pb.at[0, 0, full, full, pl.ds(0, (base + along) // 4)], ag_send.at[k])

        return carry

    lax.fori_loop(0, CHUNKS, drain_rs, 0)
    lax.fori_loop(0, AG_CHUNKS, drain_ag, 0)
    for s in range(5):
        wait(dense.at[s, :, pl.ds(1, 3)], s0_send.at[s])
    for j in range(5):
        wait(vs.at[j], vec_send.at[j])
    wait(nr.at[pl.ds(0, DP - 1)], norm_send)


def finish(*refs):
    srcs, dsts, sem = refs[:7], refs[7:14], refs[14]
    copies = [
        pltpu.make_async_copy(srcs[6].at[i // 2, i % 2], dsts[6].at[i // 2, i % 2], sem.at[6 + i])
        for i in range(8)
    ]
    copies += [pltpu.make_async_copy(srcs[i], dsts[i], sem.at[i]) for i in range(6)]
    for copy in copies:
        copy.start()
    for copy in copies:
        copy.wait()


def solution(mesh):
    axis_name = mesh.axis_names[0]
    vm = pl.BlockSpec(memory_space=pltpu.VMEM)
    hbm = pl.BlockSpec(memory_space=pl.ANY)
    dma = pltpu.SemaphoreType.DMA
    K, G = CHUNKS, AG_CHUNKS

    call = pl.pallas_call(
        kernel,
        name="adam_step",
        out_shape=(
            [pltpu.VMEM((PIECE, 128), F32)] * 3
            + [pltpu.VMEM((VEC, 128), F32)] * 3
            + [pltpu.VMEM((4, 2, 2, 2, PIECE, 128), BF16)]
        ),
        in_specs=[hbm] * 9,
        out_specs=[vm] * 7,
        scratch_shapes=[
            pltpu.SMEM((1, 1), F32),
            pltpu.VMEM((1, VEC * 128), BF16),
            pltpu.VMEM((2, DP, 1, ROWS * 128), BF16),
            pltpu.VMEM((5, 2, 4, 8 * HALF, 128), BF16),
            pltpu.VMEM((K, 2, 2, 4, RAB, 128), F32),
            pltpu.VMEM((K, 2, 4, 2, RCD, 128), F32),
            pltpu.VMEM((K, 4, 2, RAB, 128), F32),
            pltpu.VMEM((K, 2, 4, RAB, 128), F32),
            pltpu.VMEM((K, 2, 5, 2, RCD, 128), F32),
            pltpu.VMEM((K, 5, 2, RAB, 128), F32),
            pltpu.VMEM((K, 2, RCD, 128), F32),
            pltpu.VMEM((PIECE, 128), F32),
            pltpu.VMEM((8, 128), F32),
            pltpu.VMEM((8, 128), F32),
            pltpu.VMEM((6, VPAD, 128), F32),
            pltpu.VMEM((5, VPAD, 128), F32),
            pltpu.VMEM((1, 128), F32),
            pltpu.VMEM((DP, 1, 128), F32),
            dma((2,)), dma((8,)), dma((5,)), dma((SLOTS,)), dma((K,)), dma((SLOTS,)), dma((SLOTS, 2, 2)), dma((SLOTS, 2)), dma((SLOTS,)),
            dma((5,)), dma((5,)), dma, dma,
            dma((G,)), dma((G, 4)), dma((G, 4)), dma((G,)), dma((G, 4)), dma((G, 4)), dma((G,)),
        ],
        compiler_params=pltpu.CompilerParams(
            collective_id=0, has_side_effects=True, vmem_limit_bytes=37 * 2 ** 20
        ),
    )

    shapes = [(PIECE, 128)] * 3 + [(VEC, 128)] * 3
    copy_out = pl.pallas_call(
        finish,
        name="copy_out",
        out_shape=[jax.ShapeDtypeStruct(s, F32) for s in shapes] + [jax.ShapeDtypeStruct((4, 2, 2, 2, PIECE, 128), BF16)],
        in_specs=[vm] * 7,
        out_specs=[hbm] * 7,
        scratch_shapes=[dma((14,))],
        compiler_params=pltpu.CompilerParams(vmem_limit_bytes=2 ** 20),
    )

    def local_step(g_mat, g_vec, p_mat, m_mat, v_mat, p_vec, m_vec, v_vec, learn_rate):
        outs = call(
            g_mat, g_vec,
            p_mat.reshape(PIECE, 128), m_mat.reshape(PIECE, 128), v_mat.reshape(PIECE, 128),
            p_vec.reshape(VEC, 128), m_vec.reshape(VEC, 128), v_vec.reshape(VEC, 128),
            learn_rate.reshape(1, 1),
        )
        return tuple(o.reshape(-1) for o in copy_out(*outs))

    return jax.shard_map(
        local_step,
        mesh=mesh,
        in_specs=(P(axis_name, None), P(axis_name, None), P(axis_name), P(axis_name), P(axis_name), P(), P(), P(), P()),
        out_specs=(P(axis_name), P(axis_name), P(axis_name), P(), P(), P(), P()),
        check_vma=False,
    )
```
